128 devices in a mesh: book: 8 (over y, core), path: 16 (over z, x).
Axes of the slice: x: 4, y: 4, z: 4, core: 2. Of those that a mesh axis runs over, the one named last changes fastest.
Arguments:
- states: float32 [10, 20, 262144], P(None, None, ('book', 'path')), parts along dimension 2, may hold values from -7.5 to 7.5
- itm_flags: int32 [10, 262144], P(None, ('book', 'path')), parts along dimension 1, may hold values 0 or 1
- terminal: float32 [262144], P(('book', 'path')), parts along dimension 0, may hold values from -3.5 to 5.5
- strike: float32 [8], P('book'), parts along dimension 0, may hold values from 0.025 to 0.035
- date_index: int32 [262144], P(('book', 'path')), parts along dimension 0, may hold values from 0 to 9
Outputs:
- cash_flow: float32 [262144], P(('book', 'path')), parts along dimension 0
- book_price: float32 [8], P('book'), parts along dimension 0
- coefficients: float32 [80, 231], P('book'), parts along dimension 0
The draws below stay inside these ranges and needn't reach their ends.
There are 8 independent parts, one for each index of `book`. The reference program is written for one: setup_inputs(seed, part) draws one part's arguments, and reference() takes and returns one part's arrays. A program takes and returns all parts, laid end to end along the dimension named above; each array names one. Nothing has to cross between parts.
All inputs are finite; a program needn't handle non-finite values. No bound on the sum of `itm_flags` on one device may be relied on, other than what follows from the above.
Results may differ from the reference program's by a relative error of at most 0.0003.
Values sent between devices are 32-bit elements; how exact they have to be, the bound alone decides.
A program may use at most 192 MiB of HBM per device.

```python
import jax
import jax.numpy as jnp
import numpy as np
from jax import lax

FACTORS = 20
DATES = 10
PATHS = 32768


def draw_states(key, part):
    position = (jnp.arange(PATHS, dtype=jnp.float32) + 0.5) / PATHS
    centre = 2.0 * position - 1.0
    spread = 0.5 * 3.0 ** position
    noise = jnp.clip(jax.random.normal(key, (DATES, FACTORS, PATHS), jnp.float32), -4.0, 4.0)
    offset = jnp.zeros((1, FACTORS, 1), jnp.float32)
    return centre + offset + spread * noise


def draw_terminal(key, part):
    position = (jnp.arange(PATHS, dtype=jnp.float32) + 0.5) / PATHS
    noise = jnp.clip(jax.random.normal(key, (PATHS,), jnp.float32), -4.0, 4.0)
    return 2.0 * position + 0.75 * noise


def set_ends(array, own_key, least, high):
    place = [jax.random.randint(jax.random.fold_in(own_key, axis), (), 0, length) for axis, length in enumerate(array.shape)]
    widest = array.shape.index(max(array.shape))
    beside = place[:widest] + [(place[widest] + 1) % array.shape[widest]] + place[widest + 1:]
    return array.at[tuple(place)].set(least).at[tuple(beside)].set(high)


def setup_inputs(seed: int = 0, part: int = 0) -> dict:
    key_list = jax.random.split(jax.random.key(seed), 6)
    part_splits = jax.random.split(jax.random.fold_in(key_list[5], part), 6)
    states = draw_states(jax.random.fold_in(jax.random.fold_in(key_list[5], part), 71), part)
    itm_flags = set_ends((jax.random.randint(part_splits[1], (DATES, PATHS), 0, 2) < 1).astype(jnp.int32), jax.random.fold_in(part_splits[1], 1), 0, 1)
    terminal = draw_terminal(jax.random.fold_in(jax.random.fold_in(key_list[5], part), 71), part)
    strike = jnp.clip(jax.random.uniform(part_splits[3], (1,), jnp.float32, 0.025, 0.035), 0.025, 0.035)
    date_index = set_ends(jax.random.randint(part_splits[4], (PATHS,), 0, DATES), jax.random.fold_in(part_splits[4], 1), 0, DATES - 1).astype(jnp.int32)
    return {"states": states, "itm_flags": itm_flags, "terminal": terminal, "strike": strike, "date_index": date_index}


ridge_weight = 0.05
temper_scale = 0.5
highest = lax.Precision.HIGHEST

def swap_terms(factors, strike_level):
    forwards = 0.03 * jnp.exp(0.25 * factors)
    discount = jnp.cumprod(1.0 / (1.0 + 0.25 * forwards), axis=0)
    annuity = 0.25 * lax.optimization_barrier(jnp.sum(discount, axis=0))
    swap_rate = (1.0 - discount[-1]) / annuity
    return (100.0 * annuity * (swap_rate - strike_level), discount[0])

def basis_of(scaled, pair_left, pair_right):
    ones_row = jnp.ones((1, scaled.shape[1]), scaled.dtype)
    return jnp.concatenate([ones_row, scaled, scaled[pair_left] * scaled[pair_right]], axis=0)

def solve_coefs(gram_sums, rhs_sums, path_count):
    system = gram_sums / path_count + ridge_weight * jnp.eye(gram_sums.shape[0], dtype=gram_sums.dtype)
    factor_chol = jnp.linalg.cholesky(system)
    return jax.scipy.linalg.cho_solve((factor_chol, True), rhs_sums / path_count)

def reference(states, itm_flags, terminal, strike, date_index):
    pair_left, pair_right = np.triu_indices(FACTORS)
    value_now = terminal
    coef_list = []
    for date_step in range(DATES - 1, -1, -1):
        factors = states[date_step]
        exercise, discount = swap_terms(factors, strike[0])
        value_now = value_now * discount
        money_flags = itm_flags[date_step].astype(jnp.float32)
        path_count = jnp.sum(money_flags)
        mean_vals = lax.optimization_barrier(jnp.sum(money_flags * factors, axis=1)) / path_count
        variance = lax.optimization_barrier(jnp.sum(money_flags * factors * factors, axis=1)) / path_count - mean_vals * mean_vals
        scale_vals = jnp.sqrt(variance + 1e-05)
        scaled = (factors - mean_vals[:, None]) / scale_vals[:, None]
        basis_rows = basis_of(scaled, pair_left, pair_right)
        weighted = basis_rows * money_flags
        gram_sums = lax.dot_general(weighted.astype(jnp.float32), basis_rows.astype(jnp.float32), (((1,), (1,)), ((), ())), precision=highest, preferred_element_type=jnp.float32)
        rhs_sums = jnp.dot(weighted.astype(jnp.float32), value_now.astype(jnp.float32), precision=highest, preferred_element_type=jnp.float32)
        coef_vector = solve_coefs(gram_sums, rhs_sums, path_count)
        continuation = jnp.dot(coef_vector.astype(jnp.float32), basis_rows.astype(jnp.float32), precision=highest, preferred_element_type=jnp.float32)
        open_date = (date_index <= date_step).astype(jnp.float32)
        weights = jax.nn.sigmoid((exercise - continuation) / temper_scale) * money_flags * open_date
        value_now = value_now + weights * (exercise - value_now)
        coef_list.append(coef_vector)
    book_price = jnp.reshape(jnp.sum(value_now) / PATHS, (1,))
    return (value_now, book_price, jnp.stack(coef_list[::-1], axis=0))
```

```python
import functools

import jax
import jax.numpy as jnp
import numpy as np
from jax import lax
from jax.experimental import pallas as pl
from jax.experimental.pallas import tpu as pltpu
from jax.sharding import PartitionSpec as P

RIDGE = 0.05
TEMPER = 0.5
HIGHEST = lax.Precision.HIGHEST
f32 = jnp.float32
bf16 = jnp.bfloat16
GROUP = 16
DATES = 10
FACTORS = 20
BASIS = 231
ROWS = 232
PACKED = 264
OWNER = (1, 2, 3, 4, 6, 9, 11, 12, 13, 14)
MESH_ID = pl.DeviceIdType.MESH


def selectors():
    left, right = np.triu_indices(FACTORS)
    pairs = [(FACTORS, FACTORS)] + [(j, FACTORS) for j in range(FACTORS)]
    pairs += list(zip(left.tolist(), right.tolist()))
    sel = np.zeros((2, 256, 96), np.float32)
    for row, (a, b) in enumerate(pairs):
        for part in range(3):
            sel[0, row, 32 * part + a] = 1.0
            sel[1, row, 32 * part + b] = 1.0
    return jnp.asarray(sel, bf16)


def greet(me):
    barrier = pltpu.get_barrier_semaphore()
    for k in range(1, GROUP):
        pl.semaphore_signal(
            barrier, inc=1, device_id={"path": lax.rem(me + k, GROUP)}, device_id_type=MESH_ID
        )
    return barrier


def vmem():
    return pl.BlockSpec(memory_space=pltpu.VMEM)


def three_parts(a):
    one = a.astype(bf16)
    rest = a - one.astype(f32)
    two = rest.astype(bf16)
    three = (rest - two.astype(f32)).astype(bf16)
    return one, two, three


def stats_kernel(states, flags, mean_out, inv_out, count_out, part, slots, send_sem, recv_sem):
    me = lax.axis_index("path")
    barrier = greet(me)
    paths = states.shape[2]
    zero = jnp.zeros((24, 128), f32)
    for d in range(DATES):
        first = jnp.zeros((FACTORS, 128), f32)
        second = jnp.zeros((FACTORS, 128), f32)
        count = jnp.zeros((1, 128), f32)
        for c in range(paths // 128):
            z = states[d, :, 128 * c : 128 * c + 128]
            m = flags[d : d + 1, 128 * c : 128 * c + 128].astype(f32)
            mz = m * z
            first = first + mz
            second = second + mz * z
            count = count + m
        base = 64 * d
        part[base : base + 24, :] = zero
        part[base : base + FACTORS, :] = first
        part[base + 24 : base + 48, :] = zero
        part[base + 24 : base + 24 + FACTORS, :] = second
        part[base + 48 : base + 64, :] = jnp.zeros((16, 128), f32)
        part[base + 48 : base + 49, :] = count
    mine = [
        jnp.sum(part[128 * t : 128 * t + 128, :].T, axis=0, keepdims=True) for t in range(5)
    ]
    slots[me] = jnp.concatenate(mine + [jnp.zeros((3, 128), f32)], axis=0)
    pl.semaphore_wait(barrier, GROUP - 1)
    copies = []
    for k in range(1, GROUP):
        copies.append(
            pltpu.make_async_remote_copy(
                src_ref=slots.at[me],
                dst_ref=slots.at[me],
                send_sem=send_sem.at[k],
                recv_sem=recv_sem.at[k],
                device_id={"path": lax.rem(me + k, GROUP)},
                device_id_type=MESH_ID,
            )
        )
        copies[-1].start()
    for copy in copies:
        copy.wait_recv()
    total = slots[0]
    for k in range(1, GROUP):
        total = total + slots[k]
    columns = jnp.concatenate([total, jnp.zeros((120, 128), f32)], axis=0).T
    for d in range(DATES):
        base = 64 * (d % 2)
        column = jnp.broadcast_to(columns[base : base + 64, d // 2 : d // 2 + 1], (64, 128))
        count = jnp.broadcast_to(column[48:49, :], (24, 128))
        mean = column[0:24, :] / count
        variance = column[24:48, :] / count - mean * mean
        mean_out[d] = mean
        inv_out[d] = 1.0 / jnp.sqrt(variance + 1e-05)
        count_out[d] = count[0:8, :]
    for copy in copies:
        copy.wait_send()


def stats_call(states, flags):
    return pl.pallas_call(
        stats_kernel,
        name="stats",
        out_shape=(
            jax.ShapeDtypeStruct((DATES, 24, 128), f32),
            jax.ShapeDtypeStruct((DATES, 24, 128), f32),
            jax.ShapeDtypeStruct((DATES, 8, 128), f32),
        ),
        in_specs=[vmem()] * 2,
        out_specs=(vmem(),) * 3,
        scratch_shapes=[
            pltpu.VMEM((640, 128), f32),
            pltpu.VMEM((GROUP, 8, 128), f32),
            pltpu.SemaphoreType.DMA((GROUP,)),
            pltpu.SemaphoreType.DMA((GROUP,)),
        ],
        compiler_params=pltpu.CompilerParams(collective_id=0, has_side_effects=True),
    )(states, flags)


def fill_factors(y, states_d, mean, inv):
    paths = y.shape[1]
    for c in range(paths // 128):
        cut = slice(128 * c, 128 * c + 128)
        y[0:FACTORS, cut] = (states_d(cut) - mean[0:FACTORS]) * inv[0:FACTORS]


def fill_rest(y):
    paths = y.shape[1]
    y[FACTORS : FACTORS + 1, :] = jnp.ones((1, paths), f32)
    y[FACTORS + 1 : 32, :] = jnp.zeros((31 - FACTORS, paths), f32)


def basis_chunk(y_chunk, sel):
    stacked = jnp.concatenate(three_parts(y_chunk), axis=0)
    left = jnp.dot(sel[0], stacked, preferred_element_type=f32)
    right = jnp.dot(sel[1], stacked, preferred_element_type=f32)
    return left * right


def fill_basis(phi, y, sel, scale=None):
    paths = y.shape[1]
    width = min(256, paths)

    def step(i, carry):
        cut = pl.ds(pl.multiple_of(i * width, width), width)
        rows = basis_chunk(y[:, cut], sel)
        if scale is not None:
            rows = rows * scale(cut)
        phi[:, cut] = rows
        return carry

    lax.fori_loop(0, paths // width, step, 0)


def pack(full):
    rows = lax.broadcasted_iota(jnp.int32, (128, 128), 0)
    lanes = lax.broadcasted_iota(jnp.int32, (128, 128), 1)
    first = full[0:128, 0:128]
    mixed = jnp.where(rows > lanes, first, full[128:256, 128:256])
    diagonal = jnp.sum(jnp.where(rows == lanes, first, 0.0), axis=0, keepdims=True)
    return full[0:128, 128:256], mixed, jnp.broadcast_to(diagonal, (8, 128))


def unpack(cross, mixed, diagonal):
    rows = lax.broadcasted_iota(jnp.int32, (128, 128), 0)
    lanes = lax.broadcasted_iota(jnp.int32, (128, 128), 1)
    turned = mixed.T
    diagonal = jnp.broadcast_to(diagonal, (128, 128))
    first = jnp.where(rows > lanes, mixed, jnp.where(rows < lanes, turned, diagonal))
    last = jnp.where(rows <= lanes, mixed, turned)
    return first, cross, cross.T, last


def gram_kernel(states, flags, mean, inv, sel, out, y, phi):
    d = pl.program_id(0)

    @pl.when(d == 0)
    def _():
        fill_rest(y)

    fill_factors(y, lambda cut: states[0, :, cut], mean[0], inv[0])
    fill_basis(phi, y, sel, lambda cut: flags[pl.ds(d, 1), cut].astype(f32))
    rows = phi[...]
    full = lax.dot_general(
        rows, rows, (((1,), (1,)), ((), ())), precision=HIGHEST, preferred_element_type=f32
    )
    cross, mixed, diagonal = pack(full)
    out[0, 0:128, :] = cross
    out[0, 128:256, :] = mixed
    out[0, 256:264, :] = diagonal


def gram_call(states, flags, mean, inv, sel):
    paths = states.shape[2]
    return pl.pallas_call(
        gram_kernel,
        name="gram",
        grid=(DATES,),
        out_shape=jax.ShapeDtypeStruct((DATES, PACKED, 128), f32),
        in_specs=[
            pl.BlockSpec((1, FACTORS, paths), lambda d: (d, 0, 0)),
            pl.BlockSpec((DATES, paths), lambda d: (0, 0)),
            pl.BlockSpec((1, 24, 128), lambda d: (d, 0, 0)),
            pl.BlockSpec((1, 24, 128), lambda d: (d, 0, 0)),
            pl.BlockSpec((2, 256, 96), lambda d: (0, 0, 0)),
        ],
        out_specs=pl.BlockSpec((1, PACKED, 128), lambda d: (d, 0, 0)),
        scratch_shapes=[pltpu.VMEM((32, paths), f32), pltpu.VMEM((256, paths), f32)],
    )(states, flags, mean, inv, sel)


def collect_kernel(gram, out, slots, send_sem, recv_sem):
    me = lax.axis_index("path")
    barrier = greet(me)
    pl.semaphore_wait(barrier, GROUP - 1)

    def copy_of(d):
        offset = lax.rem(me - OWNER[d] + GROUP, GROUP)
        return pltpu.make_async_remote_copy(
            src_ref=gram.at[d],
            dst_ref=slots.at[offset],
            send_sem=send_sem.at[d],
            recv_sem=recv_sem.at[offset],
            device_id={"path": OWNER[d]},
            device_id_type=MESH_ID,
        )

    for d in range(DATES):

        @pl.when(me != OWNER[d])
        def _(d=d):
            copy_of(d).start()

    out[...] = jnp.zeros_like(out)
    for d in range(DATES):

        @pl.when(me == OWNER[d])
        def _(d=d):
            for k in range(1, GROUP):
                pltpu.make_async_remote_copy(
                    src_ref=gram.at[d],
                    dst_ref=slots.at[k],
                    send_sem=send_sem.at[d],
                    recv_sem=recv_sem.at[k],
                    device_id={"path": lax.rem(me + k, GROUP)},
                    device_id_type=MESH_ID,
                ).wait_recv()
            total = gram[d]
            for k in range(1, GROUP):
                total = total + slots[k]
            out[...] = total

    for d in range(DATES):

        @pl.when(me != OWNER[d])
        def _(d=d):
            copy_of(d).wait_send()


def collect_call(gram):
    return pl.pallas_call(
        collect_kernel,
        name="collect",
        out_shape=jax.ShapeDtypeStruct((PACKED, 128), f32),
        in_specs=[vmem()],
        out_specs=vmem(),
        scratch_shapes=[
            pltpu.VMEM((GROUP, PACKED, 128), f32),
            pltpu.SemaphoreType.DMA((DATES,)),
            pltpu.SemaphoreType.DMA((GROUP,)),
        ],
        compiler_params=pltpu.CompilerParams(collective_id=1, has_side_effects=True),
    )(gram)


def sweep_block(panel, b, start):
    height = panel.shape[0]
    columns = [
        jnp.broadcast_to(panel[:, start + c : start + c + 1], (height, 128)) for c in range(8)
    ]
    pivot = [column[8 * b : 8 * b + 8, :] for column in columns]
    row_of = lax.broadcasted_iota(jnp.int32, (8, 128), 0)
    for p in range(8):
        across = [jnp.broadcast_to(column[p : p + 1, :], (8, 128)) for column in pivot]
        inverse = 1.0 / across[p]
        own = pivot[p]
        here = row_of == p
        for c in range(8):
            if c == p:
                continue
            ratio = across[c] * inverse
            pivot[c] = jnp.where(here, ratio, pivot[c] - own * ratio)
        pivot[p] = jnp.where(here, -inverse, own * inverse)
    rows = panel[8 * b : 8 * b + 8, :]
    lane = lax.broadcasted_iota(jnp.int32, (8, 256), 1)
    swept = jnp.zeros((8, 256), f32)
    wide = [jnp.concatenate([column, column], axis=1) for column in pivot]
    for c in range(8):
        swept = swept - wide[c] * jnp.broadcast_to(rows[c : c + 1, :], (8, 256))
    for c in range(8):
        swept = jnp.where(lane == start + c, wide[c], swept)
    lane = lax.broadcasted_iota(jnp.int32, (height, 256), 1)
    rest = jnp.where((lane >= start) & (lane < start + 8), 0.0, panel)
    for c in range(8):
        wide_c = jnp.concatenate([columns[c], columns[c]], axis=1)
        rest = rest - wide_c * jnp.broadcast_to(swept[c : c + 1, :], (height, 256))
    pieces = [rest[8 * q : 8 * q + 8, :] for q in range(height // 8)]
    pieces[b] = swept
    return jnp.concatenate(pieces, axis=0)


def inverse_kernel(gram, count, out, work):
    scale = 1.0 / count[0:1, :]
    rows = lax.broadcasted_iota(jnp.int32, (128, 128), 0)
    lanes = lax.broadcasted_iota(jnp.int32, (128, 128), 1)
    ridge = jnp.where(rows == lanes, RIDGE, 0.0).astype(f32)
    first, cross, turned, last = unpack(
        gram[0:128, :] * scale, gram[128:256, :] * scale, gram[256:257, :] * scale
    )
    work[0:128, 0:128] = first + ridge
    work[0:128, 128:256] = cross
    work[128:256, 0:128] = turned
    work[128:256, 128:256] = last + ridge
    for top in range(0, ROWS, 32):
        before = work[top : top + 32, :]
        panel = before
        for b in range(4):
            if top + 8 * b < ROWS:
                panel = sweep_block(panel, b, top + 8 * b)
        if top + 32 > ROWS:
            keep = ROWS - top
            before = before[0:keep, :]
            panel = panel[0:keep, :]
        deep = before.shape[0]
        lane = lax.broadcasted_iota(jnp.int32, (256, 256), 1)
        change = lax.dot_general(
            before, panel, (((0,), (0,)), ((), ())), precision=HIGHEST, preferred_element_type=f32
        )
        work[...] = jnp.where((lane >= top) & (lane < top + deep), 0.0, work[...]) - change
        work[top : top + deep, :] = panel
    cross, mixed, diagonal = pack(-work[...])
    out[0:128, :] = cross
    out[128:256, :] = mixed
    out[256:264, :] = diagonal


def inverse_call(gram, count):
    return pl.pallas_call(
        inverse_kernel,
        name="inverse",
        out_shape=jax.ShapeDtypeStruct((PACKED, 128), f32),
        in_specs=[vmem()] * 2,
        out_specs=vmem(),
        scratch_shapes=[pltpu.VMEM((256, 256), f32)],
    )(gram, count)


def chain_kernel(
    states, flags, terminal, strike, date_index, mean, inv, count, sel, mine,
    cash_out, price_out, coef_out,
    y, phi, exercise, discount, value, packed, solve, slots, slots_price, coefs,
    bulk_send, bulk_recv, send_sem, recv_sem, price_send, price_recv,
):
    me = lax.axis_index("path")
    barrier = greet(me)
    paths = states.shape[2]
    chunks = paths // 128

    def prepare(d, par):
        mean_d = mean[d]
        inv_d = inv[d]
        for c in range(chunks):
            cut = slice(128 * c, 128 * c + 128)
            z = states[d, :, cut]
            y[0:FACTORS, cut] = (z - mean_d[0:FACTORS]) * inv_d[0:FACTORS]
            step = 1.0 / (1.0 + 0.25 * (0.03 * jnp.exp(0.25 * z)))
            running = step[0:1, :]
            discount[par, :, cut] = running
            total = running
            for j in range(1, FACTORS):
                running = running * step[j : j + 1, :]
                total = total + running
            annuity = 0.25 * total
            rate = (1.0 - running) / annuity
            exercise[par, :, cut] = 100.0 * annuity * (rate - strike[0])
        fill_basis(phi.at[par], y, sel)

    def bulk(d, k):
        return pltpu.make_async_remote_copy(
            src_ref=mine,
            dst_ref=packed.at[d],
            send_sem=bulk_send.at[k],
            recv_sem=bulk_recv.at[d],
            device_id={"path": lax.rem(me + k, GROUP)},
            device_id_type=MESH_ID,
        )

    def rhs_copy(par, k):
        return pltpu.make_async_remote_copy(
            src_ref=slots.at[par, me],
            dst_ref=slots.at[par, me],
            send_sem=send_sem.at[par, k],
            recv_sem=recv_sem.at[par, k],
            device_id={"path": lax.rem(me + k, GROUP)},
            device_id_type=MESH_ID,
        )

    def price_copy(k):
        return pltpu.make_async_remote_copy(
            src_ref=slots_price.at[me],
            dst_ref=slots_price.at[me],
            send_sem=price_send.at[k],
            recv_sem=price_recv.at[k],
            device_id={"path": lax.rem(me + k, GROUP)},
            device_id_type=MESH_ID,
        )

    fill_rest(y)
    pl.semaphore_wait(barrier, GROUP - 1)
    for d in range(DATES):

        @pl.when(me == OWNER[d])
        def _(d=d):
            for k in range(1, GROUP):
                bulk(d, k).start()
            packed[d] = mine[...]

    prepare(DATES - 1, 0)
    value[...] = terminal[...]
    coefs[...] = jnp.zeros_like(coefs)
    for d in range(DATES):

        @pl.when(me != OWNER[d])
        def _(d=d):
            bulk(d, 1).wait_recv()

    for d in range(DATES):

        @pl.when(me == OWNER[d])
        def _(d=d):
            for k in range(1, GROUP):
                bulk(d, k).wait_send()

    def date_step(t, carry):
        d = DATES - 1 - t
        par = lax.rem(t, 2)
        now = phi.at[par]
        held = value[...] * discount[par]
        money = flags[pl.ds(d, 1), :].astype(f32)
        weighted = money * held
        sums = jnp.zeros((ROWS, 128), f32)
        for c in range(chunks):
            cut = slice(128 * c, 128 * c + 128)
            sums = sums + now[0:ROWS, cut] * weighted[:, cut]
        low = jnp.sum(sums[0:128, :].T, axis=0, keepdims=True)
        high = jnp.concatenate([sums[128:ROWS, :], jnp.zeros((256 - ROWS, 128), f32)], axis=0)
        high = jnp.sum(high.T, axis=0, keepdims=True)
        slots[par, me] = jnp.concatenate([low, high], axis=0)
        for k in range(1, GROUP):
            rhs_copy(par, k).start()

        first, cross, turned, last = unpack(
            packed[d, 0:128, :], packed[d, 128:256, :], packed[d, 256:257, :]
        )
        solve[0:128, 0:128] = first
        solve[0:128, 128:256] = cross
        solve[128:256, 0:128] = turned
        solve[128:256, 128:256] = last
        prepare(jnp.maximum(d - 1, 0), 1 - par)

        for k in range(1, GROUP):
            rhs_copy(par, k).wait_recv()
        rhs = slots[par, 0]
        for k in range(1, GROUP):
            rhs = rhs + slots[par, k]
        rhs = rhs / count[d, 0:2, :]
        product = solve[0:ROWS, 0:128] * rhs[0:1, :] + solve[0:ROWS, 128:256] * rhs[1:2, :]
        coef = jnp.sum(product, axis=1, keepdims=True)
        coef = jnp.broadcast_to(coef, (ROWS, 128))
        lane = lax.broadcasted_iota(jnp.int32, (ROWS, 128), 1)
        coefs[0:ROWS, :] = jnp.where(lane == d, coef, coefs[0:ROWS, :])
        for c in range(chunks):
            cut = slice(128 * c, 128 * c + 128)
            continuation = jnp.sum(coef * now[0:ROWS, cut], axis=0, keepdims=True)
            gain = exercise[par, :, cut]
            open_date = (date_index[:, cut] <= d).astype(f32)
            weight = jax.nn.sigmoid((gain - continuation) / TEMPER) * money[:, cut] * open_date
            old = held[:, cut]
            value[:, cut] = old + weight * (gain - old)
        for k in range(1, GROUP):
            rhs_copy(par, k).wait_send()
        return carry

    lax.fori_loop(0, DATES, date_step, 0)

    total = jnp.zeros((1, 128), f32)
    for c in range(chunks):
        total = total + value[:, 128 * c : 128 * c + 128]
    slots_price[me] = total
    for k in range(1, GROUP):
        price_copy(k).start()
    cash_out[...] = value[...]
    turned = jnp.concatenate([coefs[0:128, :].T[0:16, :], coefs[128:256, :].T[0:16, :]], axis=1)
    coef_out[...] = turned[0:DATES, 0:BASIS]
    for k in range(1, GROUP):
        price_copy(k).wait_recv()
    total = slots_price[0]
    for k in range(1, GROUP):
        total = total + slots_price[k]
    price = jnp.sum(total, axis=1, keepdims=True) / (paths * GROUP)
    price_out[...] = jnp.broadcast_to(price, (1, 128))
    for k in range(1, GROUP):
        price_copy(k).wait_send()


def chain_call(states, flags, terminal, strike, date_index, mean, inv, count, sel, mine):
    paths = states.shape[2]
    return pl.pallas_call(
        chain_kernel,
        name="chain",
        out_shape=(
            jax.ShapeDtypeStruct((1, paths), f32),
            jax.ShapeDtypeStruct((1, 128), f32),
            jax.ShapeDtypeStruct((DATES, BASIS), f32),
        ),
        in_specs=[vmem()] * 3 + [pl.BlockSpec(memory_space=pltpu.SMEM)] + [vmem()] * 6,
        out_specs=(vmem(),) * 3,
        scratch_shapes=[
            pltpu.VMEM((32, paths), f32),
            pltpu.VMEM((2, 256, paths), f32),
            pltpu.VMEM((2, 1, paths), f32),
            pltpu.VMEM((2, 1, paths), f32),
            pltpu.VMEM((1, paths), f32),
            pltpu.VMEM((DATES, PACKED, 128), f32),
            pltpu.VMEM((256, 256), f32),
            pltpu.VMEM((2, GROUP, 2, 128), f32),
            pltpu.VMEM((GROUP, 1, 128), f32),
            pltpu.VMEM((256, 128), f32),
            pltpu.SemaphoreType.DMA((GROUP,)),
            pltpu.SemaphoreType.DMA((DATES,)),
            pltpu.SemaphoreType.DMA((2, GROUP)),
            pltpu.SemaphoreType.DMA((2, GROUP)),
            pltpu.SemaphoreType.DMA((GROUP,)),
            pltpu.SemaphoreType.DMA((GROUP,)),
        ],
        compiler_params=pltpu.CompilerParams(collective_id=2, has_side_effects=True),
    )(states, flags, terminal, strike, date_index, mean, inv, count, sel, mine)


def shards(states, flags, terminal, strike, date_index):
    paths = states.shape[2]
    sel = selectors()
    mean, inv, count = stats_call(states, flags)
    gram = gram_call(states, flags, mean, inv, sel)
    mine = collect_call(gram)
    me = lax.axis_index("path")
    own_count = count[0]
    for d in range(1, DATES):
        own_count = jnp.where(me == OWNER[d], count[d], own_count)
    packed = inverse_call(mine, own_count)
    cash, price, coefs = chain_call(
        states, flags, terminal.reshape(1, paths), strike, date_index.reshape(1, paths),
        mean, inv, count, sel, packed,
    )
    return cash.reshape(paths), price[0, 0:1], coefs


def solution(mesh):
    both = ("book", "path")
    return jax.shard_map(
        shards,
        mesh=mesh,
        in_specs=(P(None, None, both), P(None, both), P(both), P("book"), P(both)),
        out_specs=(P(both), P("book"), P("book", None)),
        check_vma=False,
    )
```

```python
import functools

import jax
import jax.numpy as jnp
import numpy as np
from jax import lax
from jax.experimental import pallas as pl
from jax.experimental.pallas import tpu as pltpu
from jax.sharding import PartitionSpec as P

RIDGE = 0.05
TEMPER = 0.5
HIGHEST = lax.Precision.HIGHEST
f32 = jnp.float32
bf16 = jnp.bfloat16
GROUP = 16
DATES = 10
FACTORS = 20
BASIS = 231
ROWS = 232
PACKED = 264
HALF = 136
SIDE = 4
LAG = 2
MESH_ID = pl.DeviceIdType.MESH


def selectors():
    left, right = np.triu_indices(FACTORS)
    pairs = [(FACTORS, FACTORS)] + [(j, FACTORS) for j in range(FACTORS)]
    pairs += list(zip(left.tolist(), right.tolist()))
    sel = np.zeros((2, 256, 96), np.float32)
    for row, (a, b) in enumerate(pairs):
        for part in range(3):
            sel[0, row, 32 * part + a] = 1.0
            sel[1, row, 32 * part + b] = 1.0
    return jnp.asarray(sel, bf16)


def owner_x(d):
    return d % SIDE


def owner_z(d):
    return (d % SIDE + d // SIDE) % SIDE


def greet(me):
    barrier = pltpu.get_barrier_semaphore()
    for k in range(1, GROUP):
        pl.semaphore_signal(
            barrier, inc=1, device_id={"path": lax.rem(me + k, GROUP)}, device_id_type=MESH_ID
        )
    return barrier


def vmem():
    return pl.BlockSpec(memory_space=pltpu.VMEM)


def three_parts(a):
    one = a.astype(bf16)
    rest = a - one.astype(f32)
    two = rest.astype(bf16)
    three = (rest - two.astype(f32)).astype(bf16)
    return one, two, three


def fill_factors(y, states_d, mean, inv):
    paths = y.shape[1]
    for c in range(paths // 128):
        cut = slice(128 * c, 128 * c + 128)
        y[0:FACTORS, cut] = (states_d(cut) - mean[0:FACTORS]) * inv[0:FACTORS]


def fill_rest(y):
    paths = y.shape[1]
    y[FACTORS : FACTORS + 1, :] = jnp.ones((1, paths), f32)
    y[FACTORS + 1 : 32, :] = jnp.zeros((31 - FACTORS, paths), f32)


def basis_chunk(y_chunk, sel):
    stacked = jnp.concatenate(three_parts(y_chunk), axis=0)
    left = jnp.dot(sel[0], stacked, preferred_element_type=f32)
    right = jnp.dot(sel[1], stacked, preferred_element_type=f32)
    return left * right


def over_chunks(paths, body):
    width = min(256, paths)

    def step(i, carry):
        body(pl.ds(pl.multiple_of(i * width, width), width))
        return carry

    lax.fori_loop(0, paths // width, step, 0)


def fill_basis(phi, y, sel):
    def body(cut):
        phi[:, cut] = basis_chunk(y[:, cut], sel)

    over_chunks(y.shape[1], body)


def triangle():
    rows = lax.broadcasted_iota(jnp.int32, (128, 128), 0)
    lanes = lax.broadcasted_iota(jnp.int32, (128, 128), 1)
    return rows, lanes


def pack(first, last):
    rows, lanes = triangle()
    mixed = jnp.where(rows > lanes, first, last)
    diagonal = jnp.sum(jnp.where(rows == lanes, first, 0.0), axis=0, keepdims=True)
    return mixed, jnp.broadcast_to(diagonal, (8, 128))


def unpack(cross, mixed, diagonal):
    rows, lanes = triangle()
    turned = mixed.T
    diagonal = jnp.broadcast_to(diagonal, (128, 128))
    first = jnp.where(rows > lanes, mixed, jnp.where(rows < lanes, turned, diagonal))
    last = jnp.where(rows <= lanes, mixed, turned)
    return first, cross, cross.T, last


def wait_all(copies):
    for copy in copies:
        copy.wait_recv()


def front_kernel(
    states, flags, sel, mean_out, inv_out, count_out, system_out,
    part, slots, y, parts, gram, slot_a, slot_b, sum_a, sum_b, last_a, last_b,
    send_sem, recv_sem, send_a, send_b, recv_a, recv_b,
    send_last_a, send_last_b, recv_last_a, recv_last_b,
):
    me = lax.axis_index("path")
    barrier = greet(me)
    paths = states.shape[2]
    zero = jnp.zeros((24, 128), f32)
    for d in range(DATES):
        first = jnp.zeros((FACTORS, 128), f32)
        second = jnp.zeros((FACTORS, 128), f32)
        count = jnp.zeros((1, 128), f32)
        for c in range(paths // 128):
            z = states[d, :, 128 * c : 128 * c + 128]
            m = flags[d : d + 1, 128 * c : 128 * c + 128].astype(f32)
            mz = m * z
            first = first + mz
            second = second + mz * z
            count = count + m
        base = 64 * d
        part[base : base + 24, :] = zero
        part[base : base + FACTORS, :] = first
        part[base + 24 : base + 48, :] = zero
        part[base + 24 : base + 24 + FACTORS, :] = second
        part[base + 48 : base + 64, :] = jnp.zeros((16, 128), f32)
        part[base + 48 : base + 49, :] = count
    mine = [
        jnp.sum(part[128 * t : 128 * t + 128, :].T, axis=0, keepdims=True) for t in range(5)
    ]
    slots[me] = jnp.concatenate(mine + [jnp.zeros((3, 128), f32)], axis=0)
    pl.semaphore_wait(barrier, GROUP - 1)
    copies = []
    for k in range(1, GROUP):
        copies.append(
            pltpu.make_async_remote_copy(
                src_ref=slots.at[me],
                dst_ref=slots.at[me],
                send_sem=send_sem.at[k],
                recv_sem=recv_sem.at[k],
                device_id={"path": lax.rem(me + k, GROUP)},
                device_id_type=MESH_ID,
            )
        )
        copies[-1].start()
    fill_rest(y)
    wait_all(copies)
    total = slots[0]
    for k in range(1, GROUP):
        total = total + slots[k]
    columns = jnp.concatenate([total, jnp.zeros((120, 128), f32)], axis=0).T
    for d in range(DATES):
        base = 64 * (d % 2)
        column = jnp.broadcast_to(columns[base : base + 64, d // 2 : d // 2 + 1], (64, 128))
        count = jnp.broadcast_to(column[48:49, :], (24, 128))
        mean = column[0:24, :] / count
        variance = column[24:48, :] / count - mean * mean
        mean_out[d] = mean
        inv_out[d] = 1.0 / jnp.sqrt(variance + 1e-05)
        count_out[d] = count[0:8, :]

    my_z, my_x = me // SIDE, lax.rem(me, SIDE)

    def copy_a(d, k):
        return pltpu.make_async_remote_copy(
            src_ref=gram.at[d, 0:HALF],
            dst_ref=slot_a.at[d // SIDE, k],
            send_sem=send_a.at[d],
            recv_sem=recv_a.at[d // SIDE, k],
            device_id={"path": my_z * SIDE + owner_x(d)},
            device_id_type=MESH_ID,
        )

    def copy_b(d, k):
        return pltpu.make_async_remote_copy(
            src_ref=gram.at[d, HALF:PACKED],
            dst_ref=slot_b.at[d // SIDE, k],
            send_sem=send_b.at[d],
            recv_sem=recv_b.at[d // SIDE, k],
            device_id={"path": owner_z(d) * SIDE + my_x},
            device_id_type=MESH_ID,
        )

    def last_copy_a(d, k):
        return pltpu.make_async_remote_copy(
            src_ref=sum_a.at[d // SIDE],
            dst_ref=last_a.at[k],
            send_sem=send_last_a.at[d // SIDE],
            recv_sem=recv_last_a.at[k],
            device_id={"path": owner_z(d) * SIDE + my_x},
            device_id_type=MESH_ID,
        )

    def last_copy_b(d, k):
        return pltpu.make_async_remote_copy(
            src_ref=sum_b.at[d // SIDE],
            dst_ref=last_b.at[k],
            send_sem=send_last_b.at[d // SIDE],
            recv_sem=recv_last_b.at[k],
            device_id={"path": my_z * SIDE + owner_x(d)},
            device_id_type=MESH_ID,
        )

    def compute(d):
        fill_factors(y, lambda cut: states[d, :, cut], mean_out[d], inv_out[d])

        def body(cut):
            rows = basis_chunk(y[:, cut], sel) * flags[pl.ds(d, 1), cut].astype(f32)
            one, two, three = three_parts(rows)
            parts[0:256, cut] = one
            parts[256:512, cut] = two
            parts[512:768, cut] = three

        over_chunks(paths, body)
        lanes = (((1,), (1,)), ((), ()))
        wide = lax.dot_general(parts[0:256, :], parts[...], lanes, preferred_element_type=f32)
        small = lax.dot_general(
            parts[256:512, :], parts[256:512, :], lanes, preferred_element_type=f32
        )
        main = wide[:, 0:256] + small
        side = wide[:, 256:512] + wide[:, 512:768]
        low, high = slice(0, 128), slice(128, 256)
        gram[d, 0:128, :] = main[low, high] + (side[low, high] + side[high, low].T)
        mixed, diagonal = pack(
            main[low, low] + (side[low, low] + side[low, low].T),
            main[high, high] + (side[high, high] + side[high, high].T),
        )
        gram[d, 128:256, :] = mixed
        gram[d, 256:264, :] = diagonal

    def send(d):
        k_x = lax.rem(my_x - owner_x(d) + SIDE, SIDE)
        k_z = lax.rem(my_z - owner_z(d) + SIDE, SIDE)

        @pl.when(k_x != 0)
        def _():
            copy_a(d, k_x).start()

        @pl.when(k_z != 0)
        def _():
            copy_b(d, k_z).start()

    def collect(d):
        q = d // SIDE
        k_x = lax.rem(my_x - owner_x(d) + SIDE, SIDE)
        k_z = lax.rem(my_z - owner_z(d) + SIDE, SIDE)

        @pl.when(k_x == 0)
        def _():
            for k in range(1, SIDE):
                copy_a(d, k).wait_recv()
            sum_a[q] = (gram[d, 0:HALF] + slot_a[q, 1]) + (slot_a[q, 2] + slot_a[q, 3])

            @pl.when(k_z != 0)
            def _():
                last_copy_a(d, k_z).start()

        @pl.when(k_z == 0)
        def _():
            for k in range(1, SIDE):
                copy_b(d, k).wait_recv()
            sum_b[q] = (gram[d, HALF:PACKED] + slot_b[q, 1]) + (slot_b[q, 2] + slot_b[q, 3])

            @pl.when(k_x != 0)
            def _():
                last_copy_b(d, k_x).start()

    def date_step(d, carry):
        compute(d)
        send(d)

        @pl.when(d >= LAG)
        def _():
            collect(d - LAG)

        return carry

    lax.fori_loop(0, DATES, date_step, 0)
    lax.fori_loop(DATES - LAG, DATES, lambda d, carry: (collect(d), carry)[1], 0)

    own_q = lax.rem(my_z - my_x + SIDE, SIDE)
    own = own_q * SIDE + my_x
    system_out[...] = jnp.zeros_like(system_out)

    @pl.when(own < DATES)
    def _():
        for k in range(1, SIDE):
            last_copy_a(own, k).wait_recv()
            last_copy_b(own, k).wait_recv()
        scale = 1.0 / count_out[own, 0:1, :]
        system_out[0:HALF] = ((sum_a[own_q] + last_a[1]) + (last_a[2] + last_a[3])) * scale
        system_out[HALF:PACKED] = ((sum_b[own_q] + last_b[1]) + (last_b[2] + last_b[3])) * scale

    def finish(d, carry):
        k_x = lax.rem(my_x - owner_x(d) + SIDE, SIDE)
        k_z = lax.rem(my_z - owner_z(d) + SIDE, SIDE)

        @pl.when(k_x != 0)
        def _():
            copy_a(d, k_x).wait_send()

        @pl.when(k_z != 0)
        def _():
            copy_b(d, k_z).wait_send()

        @pl.when((k_x == 0) & (k_z != 0))
        def _():
            last_copy_a(d, k_z).wait_send()

        @pl.when((k_z == 0) & (k_x != 0))
        def _():
            last_copy_b(d, k_x).wait_send()

        return carry

    lax.fori_loop(0, DATES, finish, 0)
    for copy in copies:
        copy.wait_send()


def front_call(states, flags, sel):
    paths = states.shape[2]
    columns = DATES // SIDE + 1
    dma = pltpu.SemaphoreType.DMA
    return pl.pallas_call(
        front_kernel,
        name="front",
        out_shape=(
            jax.ShapeDtypeStruct((DATES, 24, 128), f32),
            jax.ShapeDtypeStruct((DATES, 24, 128), f32),
            jax.ShapeDtypeStruct((DATES, 8, 128), f32),
            jax.ShapeDtypeStruct((PACKED, 128), f32),
        ),
        in_specs=[vmem()] * 3,
        out_specs=(vmem(),) * 4,
        scratch_shapes=[
            pltpu.VMEM((640, 128), f32),
            pltpu.VMEM((GROUP, 8, 128), f32),
            pltpu.VMEM((32, paths), f32),
            pltpu.VMEM((768, paths), bf16),
            pltpu.VMEM((DATES, PACKED, 128), f32),
            pltpu.VMEM((columns, SIDE, HALF, 128), f32),
            pltpu.VMEM((columns, SIDE, PACKED - HALF, 128), f32),
            pltpu.VMEM((columns, HALF, 128), f32),
            pltpu.VMEM((columns, PACKED - HALF, 128), f32),
            pltpu.VMEM((SIDE, HALF, 128), f32),
            pltpu.VMEM((SIDE, PACKED - HALF, 128), f32),
            dma((GROUP,)),
            dma((GROUP,)),
            dma((DATES,)),
            dma((DATES,)),
            dma((columns, SIDE)),
            dma((columns, SIDE)),
            dma((columns,)),
            dma((columns,)),
            dma((SIDE,)),
            dma((SIDE,)),
        ],
        compiler_params=pltpu.CompilerParams(collective_id=0, has_side_effects=True),
    )(states, flags, sel)


def sweep_block(panel, b, start):
    height = panel.shape[0]
    columns = [
        jnp.broadcast_to(panel[:, start + c : start + c + 1], (height, 128)) for c in range(8)
    ]
    pivot = [column[8 * b : 8 * b + 8, :] for column in columns]
    row_of = lax.broadcasted_iota(jnp.int32, (8, 128), 0)
    for p in range(8):
        across = [jnp.broadcast_to(column[p : p + 1, :], (8, 128)) for column in pivot]
        inverse = 1.0 / across[p]
        own = pivot[p]
        here = row_of == p
        for c in range(8):
            if c == p:
                continue
            ratio = across[c] * inverse
            pivot[c] = jnp.where(here, ratio, pivot[c] - own * ratio)
        pivot[p] = jnp.where(here, -inverse, own * inverse)
    rows = panel[8 * b : 8 * b + 8, :]
    lane = lax.broadcasted_iota(jnp.int32, (8, 256), 1)
    swept = jnp.zeros((8, 256), f32)
    wide = [jnp.concatenate([column, column], axis=1) for column in pivot]
    for c in range(8):
        swept = swept - wide[c] * jnp.broadcast_to(rows[c : c + 1, :], (8, 256))
    for c in range(8):
        swept = jnp.where(lane == start + c, wide[c], swept)
    lane = lax.broadcasted_iota(jnp.int32, (height, 256), 1)
    rest = jnp.where((lane >= start) & (lane < start + 8), 0.0, panel)
    for c in range(8):
        wide_c = jnp.concatenate([columns[c], columns[c]], axis=1)
        rest = rest - wide_c * jnp.broadcast_to(swept[c : c + 1, :], (height, 256))
    pieces = [rest[8 * q : 8 * q + 8, :] for q in range(height // 8)]
    pieces[b] = swept
    return jnp.concatenate(pieces, axis=0)


def inverse_kernel(gram, out, work):
    rows, lanes = triangle()
    ridge = jnp.where(rows == lanes, RIDGE, 0.0).astype(f32)
    first, cross, turned, last = unpack(gram[0:128, :], gram[128:256, :], gram[256:257, :])
    work[0:128, 0:128] = first + ridge
    work[0:128, 128:256] = cross
    work[128:256, 0:128] = turned
    work[128:256, 128:256] = last + ridge
    for top in range(0, ROWS, 32):
        before = work[top : top + 32, :]
        panel = before
        for b in range(4):
            if top + 8 * b < ROWS:
                panel = sweep_block(panel, b, top + 8 * b)
        if top + 32 > ROWS:
            keep = ROWS - top
            before = before[0:keep, :]
            panel = panel[0:keep, :]
        deep = before.shape[0]
        lane = lax.broadcasted_iota(jnp.int32, (256, 256), 1)
        change = lax.dot_general(
            before, panel, (((0,), (0,)), ((), ())), precision=HIGHEST, preferred_element_type=f32
        )
        work[...] = jnp.where((lane >= top) & (lane < top + deep), 0.0, work[...]) - change
        work[top : top + deep, :] = panel
    mixed, diagonal = pack(-work[0:128, 0:128], -work[128:256, 128:256])
    out[0:128, :] = -work[0:128, 128:256]
    out[128:256, :] = mixed
    out[256:264, :] = diagonal


def inverse_call(gram):
    return pl.pallas_call(
        inverse_kernel,
        name="inverse",
        out_shape=jax.ShapeDtypeStruct((PACKED, 128), f32),
        in_specs=[vmem()],
        out_specs=vmem(),
        scratch_shapes=[pltpu.VMEM((256, 256), f32)],
    )(gram)


def chain_kernel(
    states, flags, terminal, strike, date_index, mean, inv, count, sel, mine,
    cash_out, price_out, coef_out,
    y, phi, exercise, discount, value, packed, solve, slots, slots_price, coefs,
    spread_send, spread_recv, send_sem, recv_sem, price_send, price_recv,
):
    me = lax.axis_index("path")
    barrier = greet(me)
    paths = states.shape[2]
    chunks = paths // 128

    def prepare(d, par):
        mean_d = mean[d]
        inv_d = inv[d]
        for c in range(chunks):
            cut = slice(128 * c, 128 * c + 128)
            z = states[d, :, cut]
            y[0:FACTORS, cut] = (z - mean_d[0:FACTORS]) * inv_d[0:FACTORS]
            step = 1.0 / (1.0 + 0.25 * (0.03 * jnp.exp(0.25 * z)))
            running = step[0:1, :]
            discount[par, :, cut] = running
            total = running
            for j in range(1, FACTORS):
                running = running * step[j : j + 1, :]
                total = total + running
            annuity = 0.25 * total
            rate = (1.0 - running) / annuity
            exercise[par, :, cut] = 100.0 * annuity * (rate - strike[0])
        fill_basis(phi.at[par], y, sel)

    my_z, my_x = me // SIDE, lax.rem(me, SIDE)
    spans = (slice(0, HALF), slice(HALF, PACKED))

    def along(axis, k):
        if axis == 0:
            return {"path": my_z * SIDE + lax.rem(my_x + k, SIDE)}
        return {"path": lax.rem(my_z + k, SIDE) * SIDE + my_x}

    def spread(source, d, half, axis, k, stage):
        return pltpu.make_async_remote_copy(
            src_ref=source,
            dst_ref=packed.at[d, spans[half]],
            send_sem=spread_send.at[stage, half, d // SIDE, k],
            recv_sem=spread_recv.at[half, d],
            device_id=along(axis, k),
            device_id_type=MESH_ID,
        )

    def relay(d, half):
        apart = my_z != owner_z(d) if half == 0 else my_x != owner_x(d)
        return jnp.logical_not(apart)

    def is_owner(d):
        return (my_x == owner_x(d)) & (my_z == owner_z(d))

    def rhs_copy(par, k):
        return pltpu.make_async_remote_copy(
            src_ref=slots.at[par, me],
            dst_ref=slots.at[par, me],
            send_sem=send_sem.at[par, k],
            recv_sem=recv_sem.at[par, k],
            device_id={"path": lax.rem(me + k, GROUP)},
            device_id_type=MESH_ID,
        )

    def price_copy(k):
        return pltpu.make_async_remote_copy(
            src_ref=slots_price.at[me],
            dst_ref=slots_price.at[me],
            send_sem=price_send.at[k],
            recv_sem=price_recv.at[k],
            device_id={"path": lax.rem(me + k, GROUP)},
            device_id_type=MESH_ID,
        )

    fill_rest(y)
    pl.semaphore_wait(barrier, GROUP - 1)
    own_q = lax.rem(my_z - my_x + SIDE, SIDE)
    own = own_q * SIDE + my_x

    @pl.when(own < DATES)
    def _():
        for k in range(1, SIDE):
            for half in range(2):
                spread(mine.at[spans[half]], own, half, half, k, 0).start()
        for k in range(1, SIDE):
            for half in range(2):
                spread(mine.at[spans[half]], own, half, 1 - half, k, 1).start()
        packed[own] = mine[...]

    prepare(DATES - 1, 0)
    value[...] = terminal[...]
    coefs[...] = jnp.zeros_like(coefs)
    def relay_step(t, carry):
        d = DATES - 1 - t
        for half in range(2):

            @pl.when(relay(d, half) & jnp.logical_not(is_owner(d)))
            def _(half=half):
                source = packed.at[d, spans[half]]
                spread(source, d, half, half, 1, 0).wait_recv()
                for k in range(1, SIDE):
                    spread(source, d, half, 1 - half, k, 1).start()

        return carry

    lax.fori_loop(0, DATES, relay_step, 0)

    def date_step(t, carry):
        d = DATES - 1 - t
        par = lax.rem(t, 2)
        now = phi.at[par]
        held = value[...] * discount[par]
        money = flags[pl.ds(d, 1), :].astype(f32)
        weighted = money * held
        sums = jnp.zeros((ROWS, 128), f32)
        for c in range(chunks):
            cut = slice(128 * c, 128 * c + 128)
            sums = sums + now[0:ROWS, cut] * weighted[:, cut]
        low = jnp.sum(sums[0:128, :].T, axis=0, keepdims=True)
        high = jnp.concatenate([sums[128:ROWS, :], jnp.zeros((256 - ROWS, 128), f32)], axis=0)
        high = jnp.sum(high.T, axis=0, keepdims=True)
        slots[par, me] = jnp.concatenate([low, high], axis=0)
        for k in range(1, GROUP):
            rhs_copy(par, k).start()

        for half in range(2):

            @pl.when(jnp.logical_not(relay(d, half)))
            def _(half=half):
                spread(packed.at[d, spans[half]], d, half, half, 1, 0).wait_recv()

        first, cross, turned, last = unpack(
            packed[d, 0:128, :], packed[d, 128:256, :], packed[d, 256:257, :]
        )
        solve[0:128, 0:128] = first
        solve[0:128, 128:256] = cross
        solve[128:256, 0:128] = turned
        solve[128:256, 128:256] = last
        prepare(jnp.maximum(d - 1, 0), 1 - par)

        for k in range(1, GROUP):
            rhs_copy(par, k).wait_recv()
        rhs = slots[par, 0]
        for k in range(1, GROUP):
            rhs = rhs + slots[par, k]
        rhs = rhs / count[d, 0:2, :]
        product = solve[0:ROWS, 0:128] * rhs[0:1, :] + solve[0:ROWS, 128:256] * rhs[1:2, :]
        coef = jnp.sum(product, axis=1, keepdims=True)
        coef = jnp.broadcast_to(coef, (ROWS, 128))
        lane = lax.broadcasted_iota(jnp.int32, (ROWS, 128), 1)
        coefs[0:ROWS, :] = jnp.where(lane == d, coef, coefs[0:ROWS, :])
        for c in range(chunks):
            cut = slice(128 * c, 128 * c + 128)
            continuation = jnp.sum(coef * now[0:ROWS, cut], axis=0, keepdims=True)
            gain = exercise[par, :, cut]
            open_date = (date_index[:, cut] <= d).astype(f32)
            weight = jax.nn.sigmoid((gain - continuation) / TEMPER) * money[:, cut] * open_date
            old = held[:, cut]
            value[:, cut] = old + weight * (gain - old)
        for k in range(1, GROUP):
            rhs_copy(par, k).wait_send()
        return carry

    lax.fori_loop(0, DATES, date_step, 0)

    total = jnp.zeros((1, 128), f32)
    for c in range(chunks):
        total = total + value[:, 128 * c : 128 * c + 128]
    slots_price[me] = total
    for k in range(1, GROUP):
        price_copy(k).start()
    cash_out[...] = value[...]
    turned = jnp.concatenate([coefs[0:128, :].T[0:16, :], coefs[128:256, :].T[0:16, :]], axis=1)
    coef_out[...] = turned[0:DATES, 0:BASIS]
    for k in range(1, GROUP):
        price_copy(k).wait_recv()
    total = slots_price[0]
    for k in range(1, GROUP):
        total = total + slots_price[k]
    price = jnp.sum(total, axis=1, keepdims=True) / (paths * GROUP)
    price_out[...] = jnp.broadcast_to(price, (1, 128))
    for k in range(1, GROUP):
        price_copy(k).wait_send()

    @pl.when(own < DATES)
    def _():
        for k in range(1, SIDE):
            for half in range(2):
                spread(mine.at[spans[half]], own, half, half, k, 0).wait_send()
                spread(mine.at[spans[half]], own, half, 1 - half, k, 1).wait_send()

    def relay_done(d, carry):
        for half in range(2):

            @pl.when(relay(d, half) & jnp.logical_not(is_owner(d)))
            def _(half=half):
                for k in range(1, SIDE):
                    spread(packed.at[d, spans[half]], d, half, 1 - half, k, 1).wait_send()

        return carry

    lax.fori_loop(0, DATES, relay_done, 0)


def chain_call(states, flags, terminal, strike, date_index, mean, inv, count, sel, mine):
    paths = states.shape[2]
    return pl.pallas_call(
        chain_kernel,
        name="chain",
        out_shape=(
            jax.ShapeDtypeStruct((1, paths), f32),
            jax.ShapeDtypeStruct((1, 128), f32),
            jax.ShapeDtypeStruct((DATES, BASIS), f32),
        ),
        in_specs=[vmem()] * 3 + [pl.BlockSpec(memory_space=pltpu.SMEM)] + [vmem()] * 6,
        out_specs=(vmem(),) * 3,
        scratch_shapes=[
            pltpu.VMEM((32, paths), f32),
            pltpu.VMEM((2, 256, paths), f32),
            pltpu.VMEM((2, 1, paths), f32),
            pltpu.VMEM((2, 1, paths), f32),
            pltpu.VMEM((1, paths), f32),
            pltpu.VMEM((DATES, PACKED, 128), f32),
            pltpu.VMEM((256, 256), f32),
            pltpu.VMEM((2, GROUP, 2, 128), f32),
            pltpu.VMEM((GROUP, 1, 128), f32),
            pltpu.VMEM((256, 128), f32),
            pltpu.SemaphoreType.DMA((2, 2, DATES // SIDE + 1, SIDE)),
            pltpu.SemaphoreType.DMA((2, DATES)),
            pltpu.SemaphoreType.DMA((2, GROUP)),
            pltpu.SemaphoreType.DMA((2, GROUP)),
            pltpu.SemaphoreType.DMA((GROUP,)),
            pltpu.SemaphoreType.DMA((GROUP,)),
        ],
        compiler_params=pltpu.CompilerParams(collective_id=2, has_side_effects=True),
    )(states, flags, terminal, strike, date_index, mean, inv, count, sel, mine)


def shards(states, flags, terminal, strike, date_index):
    paths = states.shape[2]
    sel = selectors()
    mean, inv, count, system = front_call(states, flags, sel)
    packed = inverse_call(system)
    cash, price, coefs = chain_call(
        states, flags, terminal.reshape(1, paths), strike, date_index.reshape(1, paths),
        mean, inv, count, sel, packed,
    )
    return cash.reshape(paths), price[0, 0:1], coefs


def solution(mesh):
    both = ("book", "path")
    return jax.shard_map(
        shards,
        mesh=mesh,
        in_specs=(P(None, None, both), P(None, both), P(both), P("book"), P(both)),
        out_specs=(P(both), P("book"), P("book", None)),
        check_vma=False,
    )
```

```python
import functools

import jax
import jax.numpy as jnp
import numpy as np
from jax import lax
from jax.experimental import pallas as pl
from jax.experimental.pallas import tpu as pltpu
from jax.sharding import PartitionSpec as P

RIDGE = 0.05
TEMPER = 0.5
HIGHEST = lax.Precision.HIGHEST
f32 = jnp.float32
bf16 = jnp.bfloat16
GROUP = 16
DATES = 10
FACTORS = 20
BASIS = 231
ROWS = 232
PACKED = 264
HALF = 136
SIDE = 4
LAG = 2
MESH_ID = pl.DeviceIdType.MESH


def basis_pairs():
    pairs = []
    for base in (0, 8):
        for s in range(4):
            pairs += [(base + i, base + (i + s) % 8) for i in range(8)]
    pairs += [(i, i + 4) for i in range(4)] + [(8 + i, 8 + (i + 4) % 8) for i in range(4, 8)]
    for s in range(8):
        pairs += [(i, 8 + (i + s) % 8) for i in range(8)]
    for base in (0, 8):
        for k in range(5):
            pairs += [(base + i, 16 + k) for i in range(8)]
    pairs += [(16 + i, 16 + i) for i in range(5)] + [(16 + i, 18 + i) for i in range(3)]
    pairs += [(16 + i, 17 + i) for i in range(4)] + [(16, 19), (17, 20), (16, 20)]
    return [tuple(sorted(pair)) for pair in pairs]


def reference_order():
    left, right = np.triu_indices(FACTORS)
    wanted = [(FACTORS, FACTORS)] + [(j, FACTORS) for j in range(FACTORS)]
    wanted += list(zip(left.tolist(), right.tolist()))
    held = basis_pairs()
    move = np.zeros((256, 256), np.float32)
    for column, pair in enumerate(wanted):
        move[held.index(pair), column] = 1.0
    return jnp.asarray(move, bf16)


def owner_x(d):
    return d % SIDE


def owner_z(d):
    return (d % SIDE + d // SIDE) % SIDE


def greet(me):
    barrier = pltpu.get_barrier_semaphore()
    for k in range(1, GROUP):
        pl.semaphore_signal(
            barrier, inc=1, device_id={"path": lax.rem(me + k, GROUP)}, device_id_type=MESH_ID
        )
    return barrier


def vmem():
    return pl.BlockSpec(memory_space=pltpu.VMEM)


def three_parts(a):
    one = a.astype(bf16)
    rest = a - one.astype(f32)
    two = rest.astype(bf16)
    three = (rest - two.astype(f32)).astype(bf16)
    return one, two, three


def fill_factors(y, states_d, mean, inv):
    paths = y.shape[1]
    for c in range(paths // 128):
        cut = slice(128 * c, 128 * c + 128)
        y[0:FACTORS, cut] = (states_d(cut) - mean[0:FACTORS]) * inv[0:FACTORS]


def fill_rest(y):
    paths = y.shape[1]
    y[FACTORS : FACTORS + 1, :] = jnp.ones((1, paths), f32)
    y[FACTORS + 1 : 24, :] = jnp.zeros((23 - FACTORS, paths), f32)


def turn(rows, s):
    return rows if s == 0 else pltpu.roll(rows, 8 - s, 0)


def products(y_chunk, money=None):
    groups = [y_chunk[8 * g : 8 * g + 8, :] for g in range(3)]
    scaled = groups if money is None else [group * money for group in groups]
    turned = [turn(groups[1], s) for s in range(8)]
    pieces = [scaled[0] * turn(groups[0], s) for s in range(4)]
    pieces += [scaled[1] * turned[s] for s in range(4)]
    row = lax.broadcasted_iota(jnp.int32, groups[0].shape, 0)
    left = jnp.where(row < 4, scaled[0], scaled[1])
    pieces.append(left * jnp.where(row < 4, turn(groups[0], 4), turned[4]))
    pieces += [scaled[0] * turned[s] for s in range(8)]
    single = [jnp.broadcast_to(groups[2][k : k + 1, :], groups[0].shape) for k in range(5)]
    for g in range(2):
        pieces += [scaled[g] * single[k] for k in range(5)]
    apart = [scaled[2] * turn(groups[2], s) for s in range(5)]
    pieces.append(apart[0] + pltpu.roll(apart[2], 5, 0))
    ends = jnp.where(row < 4, apart[4], 0.0)
    pieces.append(apart[1] + pltpu.roll(apart[3], 4, 0) + pltpu.roll(ends, 6, 0))
    return pieces


def fill_basis(phi, y):
    paths = y.shape[1]

    def step(i, carry):
        cut = pl.ds(pl.multiple_of(i * 128, 128), 128)
        for q, piece in enumerate(products(y[:, cut])):
            phi[8 * q : 8 * q + 8, cut] = piece
        return carry

    lax.fori_loop(0, paths // 128, step, 0)


def triangle():
    rows = lax.broadcasted_iota(jnp.int32, (128, 128), 0)
    lanes = lax.broadcasted_iota(jnp.int32, (128, 128), 1)
    return rows, lanes


def pack(first, last):
    rows, lanes = triangle()
    mixed = jnp.where(rows > lanes, first, last)
    diagonal = jnp.sum(jnp.where(rows == lanes, first, 0.0), axis=0, keepdims=True)
    return mixed, jnp.broadcast_to(diagonal, (8, 128))


def unpack(cross, mixed, diagonal):
    rows, lanes = triangle()
    turned = mixed.T
    diagonal = jnp.broadcast_to(diagonal, (128, 128))
    first = jnp.where(rows > lanes, mixed, jnp.where(rows < lanes, turned, diagonal))
    last = jnp.where(rows <= lanes, mixed, turned)
    return first, cross, cross.T, last


def wait_all(copies):
    for copy in copies:
        copy.wait_recv()


def front_kernel(
    states, flags, mean_out, inv_out, count_out, system_out,
    part, slots, money_of, y, parts_0, parts_1, gram, slot_a, slot_b, sum_a, sum_b, last_a, last_b,
    send_sem, recv_sem, send_a, send_b, recv_a, recv_b,
    send_last_a, send_last_b, recv_last_a, recv_last_b,
):
    me = lax.axis_index("path")
    barrier = greet(me)
    paths = states.shape[2]
    zero = jnp.zeros((24, 128), f32)
    for d in range(DATES):
        first = jnp.zeros((FACTORS, 128), f32)
        second = jnp.zeros((FACTORS, 128), f32)
        count = jnp.zeros((1, 128), f32)
        for c in range(paths // 128):
            z = states[d, :, 128 * c : 128 * c + 128]
            m = flags[d : d + 1, 128 * c : 128 * c + 128].astype(f32)
            money_of[d, :, 128 * c : 128 * c + 128] = m
            mz = m * z
            first = first + mz
            second = second + mz * z
            count = count + m
        base = 64 * d
        part[base : base + 24, :] = zero
        part[base : base + FACTORS, :] = first
        part[base + 24 : base + 48, :] = zero
        part[base + 24 : base + 24 + FACTORS, :] = second
        part[base + 48 : base + 64, :] = jnp.zeros((16, 128), f32)
        part[base + 48 : base + 49, :] = count
    mine = [
        jnp.sum(part[128 * t : 128 * t + 128, :].T, axis=0, keepdims=True) for t in range(5)
    ]
    slots[me] = jnp.concatenate(mine + [jnp.zeros((3, 128), f32)], axis=0)
    pl.semaphore_wait(barrier, GROUP - 1)
    copies = []
    for k in range(1, GROUP):
        copies.append(
            pltpu.make_async_remote_copy(
                src_ref=slots.at[me],
                dst_ref=slots.at[me],
                send_sem=send_sem.at[k],
                recv_sem=recv_sem.at[k],
                device_id={"path": lax.rem(me + k, GROUP)},
                device_id_type=MESH_ID,
            )
        )
        copies[-1].start()
    fill_rest(y)
    wait_all(copies)
    total = slots[0]
    for k in range(1, GROUP):
        total = total + slots[k]
    columns = jnp.concatenate([total, jnp.zeros((120, 128), f32)], axis=0).T
    for d in range(DATES):
        base = 64 * (d % 2)
        column = jnp.broadcast_to(columns[base : base + 64, d // 2 : d // 2 + 1], (64, 128))
        count = jnp.broadcast_to(column[48:49, :], (24, 128))
        mean = column[0:24, :] / count
        variance = column[24:48, :] / count - mean * mean
        mean_out[d] = mean
        inv_out[d] = 1.0 / jnp.sqrt(variance + 1e-05)
        count_out[d] = count[0:8, :]

    my_z, my_x = me // SIDE, lax.rem(me, SIDE)

    def copy_a(d, k):
        return pltpu.make_async_remote_copy(
            src_ref=gram.at[d, 0:HALF],
            dst_ref=slot_a.at[d // SIDE, k],
            send_sem=send_a.at[d],
            recv_sem=recv_a.at[d // SIDE, k],
            device_id={"path": my_z * SIDE + owner_x(d)},
            device_id_type=MESH_ID,
        )

    def copy_b(d, k):
        return pltpu.make_async_remote_copy(
            src_ref=gram.at[d, HALF:PACKED],
            dst_ref=slot_b.at[d // SIDE, k],
            send_sem=send_b.at[d],
            recv_sem=recv_b.at[d // SIDE, k],
            device_id={"path": owner_z(d) * SIDE + my_x},
            device_id_type=MESH_ID,
        )

    def last_copy_a(d, k):
        return pltpu.make_async_remote_copy(
            src_ref=sum_a.at[d // SIDE],
            dst_ref=last_a.at[k],
            send_sem=send_last_a.at[d // SIDE],
            recv_sem=recv_last_a.at[k],
            device_id={"path": owner_z(d) * SIDE + my_x},
            device_id_type=MESH_ID,
        )

    def last_copy_b(d, k):
        return pltpu.make_async_remote_copy(
            src_ref=sum_b.at[d // SIDE],
            dst_ref=last_b.at[k],
            send_sem=send_last_b.at[d // SIDE],
            recv_sem=recv_last_b.at[k],
            device_id={"path": my_z * SIDE + owner_x(d)},
            device_id_type=MESH_ID,
        )

    def split(d, parts):
        fill_factors(y, lambda cut: states[d, :, cut], mean_out[d], inv_out[d])
        for c in range(paths // 128):
            cut = slice(128 * c, 128 * c + 128)
            money = money_of[d, :, cut]
            pieces = products(y[:, cut], money)
            pieces.append(jnp.zeros((8, 128), f32))
            for q in range(0, 30, 2):
                rows = jnp.concatenate(pieces[q : q + 2], axis=0)
                for i, piece in enumerate(three_parts(rows)):
                    parts[c, 256 * i + 8 * q : 256 * i + 8 * q + 16, :] = piece

    def compute(d, parts, other):
        lanes = (((1,), (1,)), ((), ()))
        whole = [
            jnp.concatenate(
                [parts[c, 256 * i : 256 * i + 256, :] for c in range(paths // 128)], axis=1
            )
            for i in range(3)
        ]
        main = lax.dot_general(whole[0], whole[0], lanes, preferred_element_type=f32)
        main = main + lax.dot_general(whole[1], whole[1], lanes, preferred_element_type=f32)
        side = lax.dot_general(whole[0], whole[1], lanes, preferred_element_type=f32)
        side = side + lax.dot_general(whole[0], whole[2], lanes, preferred_element_type=f32)
        split(jnp.minimum(d + 1, DATES - 1), other)
        low, high = slice(0, 128), slice(128, 256)
        gram[d, 0:128, :] = main[low, high] + (side[low, high] + side[high, low].T)
        mixed, diagonal = pack(
            main[low, low] + (side[low, low] + side[low, low].T),
            main[high, high] + (side[high, high] + side[high, high].T),
        )
        gram[d, 128:256, :] = mixed
        gram[d, 256:264, :] = diagonal

    def send(d):
        k_x = lax.rem(my_x - owner_x(d) + SIDE, SIDE)
        k_z = lax.rem(my_z - owner_z(d) + SIDE, SIDE)

        @pl.when(k_x != 0)
        def _():
            copy_a(d, k_x).start()

        @pl.when(k_z != 0)
        def _():
            copy_b(d, k_z).start()

    def collect(d):
        q = d // SIDE
        k_x = lax.rem(my_x - owner_x(d) + SIDE, SIDE)
        k_z = lax.rem(my_z - owner_z(d) + SIDE, SIDE)

        @pl.when(k_x == 0)
        def _():
            for k in range(1, SIDE):
                copy_a(d, k).wait_recv()
            sum_a[q] = (gram[d, 0:HALF] + slot_a[q, 1]) + (slot_a[q, 2] + slot_a[q, 3])

            @pl.when(k_z != 0)
            def _():
                last_copy_a(d, k_z).start()

        @pl.when(k_z == 0)
        def _():
            for k in range(1, SIDE):
                copy_b(d, k).wait_recv()
            sum_b[q] = (gram[d, HALF:PACKED] + slot_b[q, 1]) + (slot_b[q, 2] + slot_b[q, 3])

            @pl.when(k_x != 0)
            def _():
                last_copy_b(d, k_x).start()

    def two_dates(i, carry):
        for half, parts, other in ((0, parts_0, parts_1), (1, parts_1, parts_0)):
            d = 2 * i + half
            compute(d, parts, other)
            send(d)

            @pl.when(d >= LAG)
            def _(d=d):
                collect(d - LAG)

        return carry

    for parts in (parts_0, parts_1):
        for i in range(3):
            parts[:, 256 * i + 240 : 256 * i + 256, :] = jnp.zeros((paths // 128, 16, 128), bf16)
    split(0, parts_0)
    lax.fori_loop(0, DATES // 2, two_dates, 0)
    lax.fori_loop(DATES - LAG, DATES, lambda d, carry: (collect(d), carry)[1], 0)

    own_q = lax.rem(my_z - my_x + SIDE, SIDE)
    own = own_q * SIDE + my_x
    system_out[...] = jnp.zeros_like(system_out)

    @pl.when(own < DATES)
    def _():
        for k in range(1, SIDE):
            last_copy_a(own, k).wait_recv()
            last_copy_b(own, k).wait_recv()
        scale = 1.0 / count_out[own, 0:1, :]
        system_out[0:HALF] = ((sum_a[own_q] + last_a[1]) + (last_a[2] + last_a[3])) * scale
        system_out[HALF:PACKED] = ((sum_b[own_q] + last_b[1]) + (last_b[2] + last_b[3])) * scale

    def finish(d, carry):
        k_x = lax.rem(my_x - owner_x(d) + SIDE, SIDE)
        k_z = lax.rem(my_z - owner_z(d) + SIDE, SIDE)

        @pl.when(k_x != 0)
        def _():
            copy_a(d, k_x).wait_send()

        @pl.when(k_z != 0)
        def _():
            copy_b(d, k_z).wait_send()

        @pl.when((k_x == 0) & (k_z != 0))
        def _():
            last_copy_a(d, k_z).wait_send()

        @pl.when((k_z == 0) & (k_x != 0))
        def _():
            last_copy_b(d, k_x).wait_send()

        return carry

    lax.fori_loop(0, DATES, finish, 0)
    for copy in copies:
        copy.wait_send()


def front_call(states, flags):
    paths = states.shape[2]
    columns = DATES // SIDE + 1
    dma = pltpu.SemaphoreType.DMA
    return pl.pallas_call(
        front_kernel,
        name="front",
        out_shape=(
            jax.ShapeDtypeStruct((DATES, 24, 128), f32),
            jax.ShapeDtypeStruct((DATES, 24, 128), f32),
            jax.ShapeDtypeStruct((DATES, 8, 128), f32),
            jax.ShapeDtypeStruct((PACKED, 128), f32),
        ),
        in_specs=[vmem()] * 2,
        out_specs=(vmem(),) * 4,
        scratch_shapes=[
            pltpu.VMEM((640, 128), f32),
            pltpu.VMEM((GROUP, 8, 128), f32),
            pltpu.VMEM((DATES, 1, paths), f32),
            pltpu.VMEM((24, paths), f32),
            pltpu.VMEM((paths // 128, 768, 128), bf16),
            pltpu.VMEM((paths // 128, 768, 128), bf16),
            pltpu.VMEM((DATES, PACKED, 128), f32),
            pltpu.VMEM((columns, SIDE, HALF, 128), f32),
            pltpu.VMEM((columns, SIDE, PACKED - HALF, 128), f32),
            pltpu.VMEM((columns, HALF, 128), f32),
            pltpu.VMEM((columns, PACKED - HALF, 128), f32),
            pltpu.VMEM((SIDE, HALF, 128), f32),
            pltpu.VMEM((SIDE, PACKED - HALF, 128), f32),
            dma((GROUP,)),
            dma((GROUP,)),
            dma((DATES,)),
            dma((DATES,)),
            dma((columns, SIDE)),
            dma((columns, SIDE)),
            dma((columns,)),
            dma((columns,)),
            dma((SIDE,)),
            dma((SIDE,)),
        ],
        compiler_params=pltpu.CompilerParams(collective_id=0, has_side_effects=True),
    )(states, flags)


def sweep_block(panel, b, start):
    height = panel.shape[0]
    columns = [
        jnp.broadcast_to(panel[:, start + c : start + c + 1], (height, 128)) for c in range(8)
    ]
    pivot = [column[8 * b : 8 * b + 8, :] for column in columns]
    row_of = lax.broadcasted_iota(jnp.int32, (8, 128), 0)
    for p in range(8):
        across = [jnp.broadcast_to(column[p : p + 1, :], (8, 128)) for column in pivot]
        inverse = 1.0 / across[p]
        own = pivot[p]
        here = row_of == p
        for c in range(8):
            if c == p:
                continue
            ratio = across[c] * inverse
            pivot[c] = jnp.where(here, ratio, pivot[c] - own * ratio)
        pivot[p] = jnp.where(here, -inverse, own * inverse)
    rows = panel[8 * b : 8 * b + 8, :]
    lane = lax.broadcasted_iota(jnp.int32, (8, 256), 1)
    swept = jnp.zeros((8, 256), f32)
    wide = [jnp.concatenate([column, column], axis=1) for column in pivot]
    for c in range(8):
        swept = swept - wide[c] * jnp.broadcast_to(rows[c : c + 1, :], (8, 256))
    for c in range(8):
        swept = jnp.where(lane == start + c, wide[c], swept)
    lane = lax.broadcasted_iota(jnp.int32, (height, 256), 1)
    rest = jnp.where((lane >= start) & (lane < start + 8), 0.0, panel)
    for c in range(8):
        wide_c = jnp.concatenate([columns[c], columns[c]], axis=1)
        rest = rest - wide_c * jnp.broadcast_to(swept[c : c + 1, :], (height, 256))
    pieces = [rest[8 * q : 8 * q + 8, :] for q in range(height // 8)]
    pieces[b] = swept
    return jnp.concatenate(pieces, axis=0)


def inverse_kernel(gram, out, work):
    rows, lanes = triangle()
    ridge = jnp.where(rows == lanes, RIDGE, 0.0).astype(f32)
    first, cross, turned, last = unpack(gram[0:128, :], gram[128:256, :], gram[256:257, :])
    work[0:128, 0:128] = first + ridge
    work[0:128, 128:256] = cross
    work[128:256, 0:128] = turned
    work[128:256, 128:256] = last + ridge
    for top in range(0, ROWS, 32):
        before = work[top : top + 32, :]
        panel = before
        for b in range(4):
            if top + 8 * b < ROWS:
                panel = sweep_block(panel, b, top + 8 * b)
        if top + 32 > ROWS:
            keep = ROWS - top
            before = before[0:keep, :]
            panel = panel[0:keep, :]
        deep = before.shape[0]
        lane = lax.broadcasted_iota(jnp.int32, (256, 256), 1)
        change = lax.dot_general(
            before, panel, (((0,), (0,)), ((), ())), precision=HIGHEST, preferred_element_type=f32
        )
        work[...] = jnp.where((lane >= top) & (lane < top + deep), 0.0, work[...]) - change
        work[top : top + deep, :] = panel
    mixed, diagonal = pack(-work[0:128, 0:128], -work[128:256, 128:256])
    out[0:128, :] = -work[0:128, 128:256]
    out[128:256, :] = mixed
    out[256:264, :] = diagonal


def inverse_call(gram):
    return pl.pallas_call(
        inverse_kernel,
        name="inverse",
        out_shape=jax.ShapeDtypeStruct((PACKED, 128), f32),
        in_specs=[vmem()],
        out_specs=vmem(),
        scratch_shapes=[pltpu.VMEM((256, 256), f32)],
    )(gram)


def chain_kernel(
    states, flags, terminal, strike, date_index, mean, inv, count, mine, move,
    cash_out, price_out, coef_out,
    y, phi, exercise, discount, value, packed, solve, slots, slots_price, coefs,
    spread_send, spread_recv, send_sem, recv_sem, price_send, price_recv,
):
    me = lax.axis_index("path")
    barrier = greet(me)
    paths = states.shape[2]
    chunks = paths // 128

    def prepare(d, par):
        mean_d = mean[d]
        inv_d = inv[d]
        for c in range(chunks):
            cut = slice(128 * c, 128 * c + 128)
            z = states[d, :, cut]
            y[0:FACTORS, cut] = (z - mean_d[0:FACTORS]) * inv_d[0:FACTORS]
            step = 1.0 / (1.0 + 0.25 * (0.03 * jnp.exp(0.25 * z)))
            running = step[0:1, :]
            discount[par, :, cut] = running
            total = running
            for j in range(1, FACTORS):
                running = running * step[j : j + 1, :]
                total = total + running
            annuity = 0.25 * total
            rate = (1.0 - running) / annuity
            exercise[par, :, cut] = 100.0 * annuity * (rate - strike[0])
        fill_basis(phi.at[par], y)

    my_z, my_x = me // SIDE, lax.rem(me, SIDE)
    spans = (slice(0, HALF), slice(HALF, PACKED))

    def along(axis, k):
        if axis == 0:
            return {"path": my_z * SIDE + lax.rem(my_x + k, SIDE)}
        return {"path": lax.rem(my_z + k, SIDE) * SIDE + my_x}

    def spread(source, d, half, axis, k, stage):
        return pltpu.make_async_remote_copy(
            src_ref=source,
            dst_ref=packed.at[d, spans[half]],
            send_sem=spread_send.at[stage, half, d // SIDE, k],
            recv_sem=spread_recv.at[half, d],
            device_id=along(axis, k),
            device_id_type=MESH_ID,
        )

    def relay(d, half):
        apart = my_z != owner_z(d) if half == 0 else my_x != owner_x(d)
        return jnp.logical_not(apart)

    def is_owner(d):
        return (my_x == owner_x(d)) & (my_z == owner_z(d))

    def rhs_copy(par, k):
        return pltpu.make_async_remote_copy(
            src_ref=slots.at[par, me],
            dst_ref=slots.at[par, me],
            send_sem=send_sem.at[par, k],
            recv_sem=recv_sem.at[par, k],
            device_id={"path": lax.rem(me + k, GROUP)},
            device_id_type=MESH_ID,
        )

    def price_copy(k):
        return pltpu.make_async_remote_copy(
            src_ref=slots_price.at[me],
            dst_ref=slots_price.at[me],
            send_sem=price_send.at[k],
            recv_sem=price_recv.at[k],
            device_id={"path": lax.rem(me + k, GROUP)},
            device_id_type=MESH_ID,
        )

    fill_rest(y)
    pl.semaphore_wait(barrier, GROUP - 1)
    own_q = lax.rem(my_z - my_x + SIDE, SIDE)
    own = own_q * SIDE + my_x

    @pl.when(own < DATES)
    def _():
        for k in range(1, SIDE):
            for half in range(2):
                spread(mine.at[spans[half]], own, half, half, k, 0).start()
        for k in range(1, SIDE):
            for half in range(2):
                spread(mine.at[spans[half]], own, half, 1 - half, k, 1).start()
        packed[own] = mine[...]

    prepare(DATES - 1, 0)
    value[...] = terminal[...]
    coefs[...] = jnp.zeros_like(coefs)
    def relay_step(t, carry):
        d = DATES - 1 - t
        for half in range(2):

            @pl.when(relay(d, half) & jnp.logical_not(is_owner(d)))
            def _(half=half):
                source = packed.at[d, spans[half]]
                spread(source, d, half, half, 1, 0).wait_recv()
                for k in range(1, SIDE):
                    spread(source, d, half, 1 - half, k, 1).start()

        return carry

    lax.fori_loop(0, DATES, relay_step, 0)

    def date_step(t, carry):
        d = DATES - 1 - t
        par = lax.rem(t, 2)
        now = phi.at[par]
        held = value[...] * discount[par]
        money = flags[pl.ds(d, 1), :].astype(f32)
        weighted = money * held
        sums = jnp.zeros((ROWS, 128), f32)
        for c in range(chunks):
            cut = slice(128 * c, 128 * c + 128)
            sums = sums + now[0:ROWS, cut] * weighted[:, cut]
        low = jnp.sum(sums[0:128, :].T, axis=0, keepdims=True)
        high = jnp.concatenate([sums[128:ROWS, :], jnp.zeros((256 - ROWS, 128), f32)], axis=0)
        high = jnp.sum(high.T, axis=0, keepdims=True)
        slots[par, me] = jnp.concatenate([low, high], axis=0)
        for k in range(1, GROUP):
            rhs_copy(par, k).start()

        for half in range(2):

            @pl.when(jnp.logical_not(relay(d, half)))
            def _(half=half):
                spread(packed.at[d, spans[half]], d, half, half, 1, 0).wait_recv()

        first, cross, turned, last = unpack(
            packed[d, 0:128, :], packed[d, 128:256, :], packed[d, 256:257, :]
        )
        solve[0:128, 0:128] = first
        solve[0:128, 128:256] = cross
        solve[128:256, 0:128] = turned
        solve[128:256, 128:256] = last
        prepare(jnp.maximum(d - 1, 0), 1 - par)

        for k in range(1, GROUP):
            rhs_copy(par, k).wait_recv()
        rhs = slots[par, 0]
        for k in range(1, GROUP):
            rhs = rhs + slots[par, k]
        rhs = rhs / count[d, 0:2, :]
        product = solve[0:ROWS, 0:128] * rhs[0:1, :] + solve[0:ROWS, 128:256] * rhs[1:2, :]
        coef = jnp.sum(product, axis=1, keepdims=True)
        coef = jnp.broadcast_to(coef, (ROWS, 128))
        lane = lax.broadcasted_iota(jnp.int32, (ROWS, 128), 1)
        coefs[0:ROWS, :] = jnp.where(lane == d, coef, coefs[0:ROWS, :])
        for c in range(chunks):
            cut = slice(128 * c, 128 * c + 128)
            continuation = jnp.sum(coef * now[0:ROWS, cut], axis=0, keepdims=True)
            gain = exercise[par, :, cut]
            open_date = (date_index[:, cut] <= d).astype(f32)
            weight = jax.nn.sigmoid((gain - continuation) / TEMPER) * money[:, cut] * open_date
            old = held[:, cut]
            value[:, cut] = old + weight * (gain - old)
        for k in range(1, GROUP):
            rhs_copy(par, k).wait_send()
        return carry

    lax.fori_loop(0, DATES, date_step, 0)

    total = jnp.zeros((1, 128), f32)
    for c in range(chunks):
        total = total + value[:, 128 * c : 128 * c + 128]
    slots_price[me] = total
    for k in range(1, GROUP):
        price_copy(k).start()
    cash_out[...] = value[...]
    turned = jnp.concatenate([coefs[0:128, :].T[0:16, :], coefs[128:256, :].T[0:16, :]], axis=1)
    ordered = jnp.zeros((16, 256), f32)
    for piece in three_parts(turned)[::-1]:
        ordered = ordered + jnp.dot(piece, move[...], preferred_element_type=f32)
    coef_out[...] = ordered[0:DATES, 0:BASIS]
    for k in range(1, GROUP):
        price_copy(k).wait_recv()
    total = slots_price[0]
    for k in range(1, GROUP):
        total = total + slots_price[k]
    price = jnp.sum(total, axis=1, keepdims=True) / (paths * GROUP)
    price_out[...] = jnp.broadcast_to(price, (1, 128))
    for k in range(1, GROUP):
        price_copy(k).wait_send()

    @pl.when(own < DATES)
    def _():
        for k in range(1, SIDE):
            for half in range(2):
                spread(mine.at[spans[half]], own, half, half, k, 0).wait_send()
                spread(mine.at[spans[half]], own, half, 1 - half, k, 1).wait_send()

    def relay_done(d, carry):
        for half in range(2):

            @pl.when(relay(d, half) & jnp.logical_not(is_owner(d)))
            def _(half=half):
                for k in range(1, SIDE):
                    spread(packed.at[d, spans[half]], d, half, 1 - half, k, 1).wait_send()

        return carry

    lax.fori_loop(0, DATES, relay_done, 0)


def chain_call(states, flags, terminal, strike, date_index, mean, inv, count, mine, move):
    paths = states.shape[2]
    return pl.pallas_call(
        chain_kernel,
        name="chain",
        out_shape=(
            jax.ShapeDtypeStruct((1, paths), f32),
            jax.ShapeDtypeStruct((1, 128), f32),
            jax.ShapeDtypeStruct((DATES, BASIS), f32),
        ),
        in_specs=[vmem()] * 3 + [pl.BlockSpec(memory_space=pltpu.SMEM)] + [vmem()] * 6,
        out_specs=(vmem(),) * 3,
        scratch_shapes=[
            pltpu.VMEM((24, paths), f32),
            pltpu.VMEM((2, ROWS, paths), f32),
            pltpu.VMEM((2, 1, paths), f32),
            pltpu.VMEM((2, 1, paths), f32),
            pltpu.VMEM((1, paths), f32),
            pltpu.VMEM((DATES, PACKED, 128), f32),
            pltpu.VMEM((256, 256), f32),
            pltpu.VMEM((2, GROUP, 2, 128), f32),
            pltpu.VMEM((GROUP, 1, 128), f32),
            pltpu.VMEM((256, 128), f32),
            pltpu.SemaphoreType.DMA((2, 2, DATES // SIDE + 1, SIDE)),
            pltpu.SemaphoreType.DMA((2, DATES)),
            pltpu.SemaphoreType.DMA((2, GROUP)),
            pltpu.SemaphoreType.DMA((2, GROUP)),
            pltpu.SemaphoreType.DMA((GROUP,)),
            pltpu.SemaphoreType.DMA((GROUP,)),
        ],
        compiler_params=pltpu.CompilerParams(collective_id=2, has_side_effects=True),
    )(states, flags, terminal, strike, date_index, mean, inv, count, mine, move)


def shards(states, flags, terminal, strike, date_index):
    paths = states.shape[2]
    mean, inv, count, system = front_call(states, flags)
    packed = inverse_call(system)
    cash, price, coefs = chain_call(
        states, flags, terminal.reshape(1, paths), strike, date_index.reshape(1, paths),
        mean, inv, count, packed, reference_order(),
    )
    return cash.reshape(paths), price[0, 0:1], coefs


def solution(mesh):
    both = ("book", "path")
    return jax.shard_map(
        shards,
        mesh=mesh,
        in_specs=(P(None, None, both), P(None, both), P(both), P("book"), P(both)),
        out_specs=(P(both), P("book"), P("book", None)),
        check_vma=False,
    )
```

```python
import functools

import jax
import jax.numpy as jnp
import numpy as np
from jax import lax
from jax.experimental import pallas as pl
from jax.experimental.pallas import tpu as pltpu
from jax.sharding import PartitionSpec as P

RIDGE = 0.05
TEMPER = 0.5
HIGHEST = lax.Precision.HIGHEST
f32 = jnp.float32
bf16 = jnp.bfloat16
GROUP = 16
DATES = 10
FACTORS = 20
BASIS = 231
ROWS = 232
PACKED = 264
HALF = 136
SIDE = 4
LAG = 2
CHUNKS = 8
MESH_ID = pl.DeviceIdType.MESH


def basis_pairs():
    pairs = []
    for base in (0, 8):
        for s in range(4):
            pairs += [(base + i, base + (i + s) % 8) for i in range(8)]
    pairs += [(i, i + 4) for i in range(4)] + [(8 + i, 8 + (i + 4) % 8) for i in range(4, 8)]
    for s in range(8):
        pairs += [(i, 8 + (i + s) % 8) for i in range(8)]
    for base in (0, 8):
        for k in range(5):
            pairs += [(base + i, 16 + k) for i in range(8)]
    pairs += [(16 + i, 16 + i) for i in range(5)] + [(16 + i, 18 + i) for i in range(3)]
    pairs += [(16 + i, 17 + i) for i in range(4)] + [(16, 19), (17, 20), (16, 20)]
    return [tuple(sorted(pair)) for pair in pairs]


def reference_order():
    left, right = np.triu_indices(FACTORS)
    wanted = [(FACTORS, FACTORS)] + [(j, FACTORS) for j in range(FACTORS)]
    wanted += list(zip(left.tolist(), right.tolist()))
    held = basis_pairs()
    move = np.zeros((256, 256), np.float32)
    for column, pair in enumerate(wanted):
        move[held.index(pair), column] = 1.0
    return jnp.asarray(move, bf16)


def owner_x(d):
    return d % SIDE


def owner_z(d):
    return (d % SIDE + d // SIDE) % SIDE


def greet(me):
    barrier = pltpu.get_barrier_semaphore()
    for k in range(1, GROUP):
        pl.semaphore_signal(
            barrier, inc=1, device_id={"path": lax.rem(me + k, GROUP)}, device_id_type=MESH_ID
        )
    return barrier


def vmem():
    return pl.BlockSpec(memory_space=pltpu.VMEM)


def three_parts(a):
    one = a.astype(bf16)
    rest = a - one.astype(f32)
    two = rest.astype(bf16)
    three = (rest - two.astype(f32)).astype(bf16)
    return one, two, three


def fill_factors(y, states_d, mean, inv):
    paths = y.shape[1]
    for c in range(paths // 128):
        cut = slice(128 * c, 128 * c + 128)
        y[0:FACTORS, cut] = (states_d(cut) - mean[0:FACTORS]) * inv[0:FACTORS]


def fill_rest(y):
    paths = y.shape[1]
    y[FACTORS : FACTORS + 1, :] = jnp.ones((1, paths), f32)
    y[FACTORS + 1 : 24, :] = jnp.zeros((23 - FACTORS, paths), f32)


def turn(rows, s):
    return rows if s == 0 else pltpu.roll(rows, 8 - s, 0)


def products(y_chunk, money=None):
    groups = [y_chunk[8 * g : 8 * g + 8, :] for g in range(3)]
    scaled = groups if money is None else [group * money for group in groups]
    turned = [turn(groups[1], s) for s in range(8)]
    pieces = [scaled[0] * turn(groups[0], s) for s in range(4)]
    pieces += [scaled[1] * turned[s] for s in range(4)]
    row = lax.broadcasted_iota(jnp.int32, groups[0].shape, 0)
    left = jnp.where(row < 4, scaled[0], scaled[1])
    pieces.append(left * jnp.where(row < 4, turn(groups[0], 4), turned[4]))
    pieces += [scaled[0] * turned[s] for s in range(8)]
    single = [jnp.broadcast_to(groups[2][k : k + 1, :], groups[0].shape) for k in range(5)]
    for g in range(2):
        pieces += [scaled[g] * single[k] for k in range(5)]
    apart = [scaled[2] * turn(groups[2], s) for s in range(5)]
    pieces.append(apart[0] + pltpu.roll(apart[2], 5, 0))
    ends = jnp.where(row < 4, apart[4], 0.0)
    pieces.append(apart[1] + pltpu.roll(apart[3], 4, 0) + pltpu.roll(ends, 6, 0))
    return pieces


def fill_basis(phi, y):
    paths = y.shape[1]

    def step(i, carry):
        cut = pl.ds(pl.multiple_of(i * 128, 128), 128)
        for q, piece in enumerate(products(y[:, cut])):
            phi[8 * q : 8 * q + 8, cut] = piece
        return carry

    lax.fori_loop(0, paths // 128, step, 0)


def triangle():
    rows = lax.broadcasted_iota(jnp.int32, (128, 128), 0)
    lanes = lax.broadcasted_iota(jnp.int32, (128, 128), 1)
    return rows, lanes


def pack(first, last):
    rows, lanes = triangle()
    mixed = jnp.where(rows > lanes, first, last)
    diagonal = jnp.sum(jnp.where(rows == lanes, first, 0.0), axis=0, keepdims=True)
    return mixed, jnp.broadcast_to(diagonal, (8, 128))


def unpack(cross, mixed, diagonal):
    rows, lanes = triangle()
    turned = mixed.T
    diagonal = jnp.broadcast_to(diagonal, (128, 128))
    first = jnp.where(rows > lanes, mixed, jnp.where(rows < lanes, turned, diagonal))
    last = jnp.where(rows <= lanes, mixed, turned)
    return first, cross, cross.T, last


def wait_all(copies):
    for copy in copies:
        copy.wait_recv()


def front_kernel(
    states, flags, mean_out, inv_out, count_out, system_out,
    part, slots, money_of, y, parts, gram, slot_a, slot_b, sum_a, sum_b, last_a, last_b,
    send_sem, recv_sem, send_a, send_b, recv_a, recv_b,
    send_last_a, send_last_b, recv_last_a, recv_last_b,
):
    me = lax.axis_index("path")
    barrier = greet(me)
    paths = states.shape[2]
    zero = jnp.zeros((24, 128), f32)
    for d in range(DATES):
        first = jnp.zeros((FACTORS, 128), f32)
        second = jnp.zeros((FACTORS, 128), f32)
        count = jnp.zeros((1, 128), f32)
        for c in range(paths // 128):
            z = states[d, :, 128 * c : 128 * c + 128]
            m = flags[d : d + 1, 128 * c : 128 * c + 128].astype(f32)
            money_of[d, :, 128 * c : 128 * c + 128] = m
            mz = m * z
            first = first + mz
            second = second + mz * z
            count = count + m
        base = 64 * d
        part[base : base + 24, :] = zero
        part[base : base + FACTORS, :] = first
        part[base + 24 : base + 48, :] = zero
        part[base + 24 : base + 24 + FACTORS, :] = second
        part[base + 48 : base + 64, :] = jnp.zeros((16, 128), f32)
        part[base + 48 : base + 49, :] = count
    mine = [
        jnp.sum(part[128 * t : 128 * t + 128, :].T, axis=0, keepdims=True) for t in range(5)
    ]
    slots[me] = jnp.concatenate(mine + [jnp.zeros((3, 128), f32)], axis=0)
    pl.semaphore_wait(barrier, GROUP - 1)
    copies = []
    for k in range(1, GROUP):
        copies.append(
            pltpu.make_async_remote_copy(
                src_ref=slots.at[me],
                dst_ref=slots.at[me],
                send_sem=send_sem.at[k],
                recv_sem=recv_sem.at[k],
                device_id={"path": lax.rem(me + k, GROUP)},
                device_id_type=MESH_ID,
            )
        )
        copies[-1].start()
    fill_rest(y)
    wait_all(copies)
    total = slots[0]
    for k in range(1, GROUP):
        total = total + slots[k]
    columns = jnp.concatenate([total, jnp.zeros((120, 128), f32)], axis=0).T
    for d in range(DATES):
        base = 64 * (d % 2)
        column = jnp.broadcast_to(columns[base : base + 64, d // 2 : d // 2 + 1], (64, 128))
        count = jnp.broadcast_to(column[48:49, :], (24, 128))
        mean = column[0:24, :] / count
        variance = column[24:48, :] / count - mean * mean
        mean_out[d] = mean
        inv_out[d] = 1.0 / jnp.sqrt(variance + 1e-05)
        count_out[d] = count[0:8, :]

    my_z, my_x = me // SIDE, lax.rem(me, SIDE)

    def copy_a(d, k):
        return pltpu.make_async_remote_copy(
            src_ref=gram.at[d, 0:HALF],
            dst_ref=slot_a.at[d // SIDE, k],
            send_sem=send_a.at[d],
            recv_sem=recv_a.at[d // SIDE, k],
            device_id={"path": my_z * SIDE + owner_x(d)},
            device_id_type=MESH_ID,
        )

    def copy_b(d, k):
        return pltpu.make_async_remote_copy(
            src_ref=gram.at[d, HALF:PACKED],
            dst_ref=slot_b.at[d // SIDE, k],
            send_sem=send_b.at[d],
            recv_sem=recv_b.at[d // SIDE, k],
            device_id={"path": owner_z(d) * SIDE + my_x},
            device_id_type=MESH_ID,
        )

    def last_copy_a(d, k):
        return pltpu.make_async_remote_copy(
            src_ref=sum_a.at[d // SIDE],
            dst_ref=last_a.at[k],
            send_sem=send_last_a.at[d // SIDE],
            recv_sem=recv_last_a.at[k],
            device_id={"path": owner_z(d) * SIDE + my_x},
            device_id_type=MESH_ID,
        )

    def last_copy_b(d, k):
        return pltpu.make_async_remote_copy(
            src_ref=sum_b.at[d // SIDE],
            dst_ref=last_b.at[k],
            send_sem=send_last_b.at[d // SIDE],
            recv_sem=recv_last_b.at[k],
            device_id={"path": my_z * SIDE + owner_x(d)},
            device_id_type=MESH_ID,
        )

    def split(d, parts, slabs):
        for c in slabs:
            cut = slice(128 * c, 128 * c + 128)
            y[0:FACTORS, cut] = (states[d, :, cut] - mean_out[d, 0:FACTORS]) * inv_out[d, 0:FACTORS]
            money = money_of[d, :, cut]
            pieces = products(y[:, cut], money)
            pieces.append(jnp.zeros((8, 128), f32))
            for q in range(0, 30, 2):
                rows = jnp.concatenate(pieces[q : q + 2], axis=0)
                for i, piece in enumerate(three_parts(rows)):
                    parts[c, 256 * i + 8 * q : 256 * i + 8 * q + 16, :] = piece

    def compute(d, parts):
        lanes = (((1,), (1,)), ((), ()))
        total = paths // 128
        step = max(total // CHUNKS, 1)
        main = jnp.zeros((256, 256), f32)
        side = jnp.zeros((256, 256), f32)
        for start in range(0, total, step):
            slabs = range(start, start + step)
            split(d, parts, slabs)
            whole = [
                jnp.concatenate(
                    [parts[c, 256 * i : 256 * i + 256, :] for c in slabs], axis=1
                )
                for i in range(3)
            ]
            for i, k in ((0, 0), (1, 1)):
                main = main + lax.dot_general(
                    whole[i], whole[k], lanes, preferred_element_type=f32
                )
            for i, k in ((0, 1), (0, 2)):
                side = side + lax.dot_general(
                    whole[i], whole[k], lanes, preferred_element_type=f32
                )
        low, high = slice(0, 128), slice(128, 256)
        gram[d, 0:128, :] = main[low, high] + (side[low, high] + side[high, low].T)
        mixed, diagonal = pack(
            main[low, low] + (side[low, low] + side[low, low].T),
            main[high, high] + (side[high, high] + side[high, high].T),
        )
        gram[d, 128:256, :] = mixed
        gram[d, 256:264, :] = diagonal

    def send(d):
        k_x = lax.rem(my_x - owner_x(d) + SIDE, SIDE)
        k_z = lax.rem(my_z - owner_z(d) + SIDE, SIDE)

        @pl.when(k_x != 0)
        def _():
            copy_a(d, k_x).start()

        @pl.when(k_z != 0)
        def _():
            copy_b(d, k_z).start()

    def collect(d):
        q = d // SIDE
        k_x = lax.rem(my_x - owner_x(d) + SIDE, SIDE)
        k_z = lax.rem(my_z - owner_z(d) + SIDE, SIDE)

        @pl.when(k_x == 0)
        def _():
            for k in range(1, SIDE):
                copy_a(d, k).wait_recv()
            sum_a[q] = (gram[d, 0:HALF] + slot_a[q, 1]) + (slot_a[q, 2] + slot_a[q, 3])

            @pl.when(k_z != 0)
            def _():
                last_copy_a(d, k_z).start()

        @pl.when(k_z == 0)
        def _():
            for k in range(1, SIDE):
                copy_b(d, k).wait_recv()
            sum_b[q] = (gram[d, HALF:PACKED] + slot_b[q, 1]) + (slot_b[q, 2] + slot_b[q, 3])

            @pl.when(k_x != 0)
            def _():
                last_copy_b(d, k_x).start()

    def date_step(d, carry):
        compute(d, parts)
        send(d)

        @pl.when(d >= LAG)
        def _():
            collect(d - LAG)

        return carry

    for i in range(3):
        parts[:, 256 * i + 240 : 256 * i + 256, :] = jnp.zeros((paths // 128, 16, 128), bf16)
    lax.fori_loop(0, DATES, date_step, 0)
    lax.fori_loop(DATES - LAG, DATES, lambda d, carry: (collect(d), carry)[1], 0)

    own_q = lax.rem(my_z - my_x + SIDE, SIDE)
    own = own_q * SIDE + my_x
    system_out[...] = jnp.zeros_like(system_out)

    @pl.when(own < DATES)
    def _():
        for k in range(1, SIDE):
            last_copy_a(own, k).wait_recv()
            last_copy_b(own, k).wait_recv()
        scale = 1.0 / count_out[own, 0:1, :]
        system_out[0:HALF] = ((sum_a[own_q] + last_a[1]) + (last_a[2] + last_a[3])) * scale
        system_out[HALF:PACKED] = ((sum_b[own_q] + last_b[1]) + (last_b[2] + last_b[3])) * scale

    def finish(d, carry):
        k_x = lax.rem(my_x - owner_x(d) + SIDE, SIDE)
        k_z = lax.rem(my_z - owner_z(d) + SIDE, SIDE)

        @pl.when(k_x != 0)
        def _():
            copy_a(d, k_x).wait_send()

        @pl.when(k_z != 0)
        def _():
            copy_b(d, k_z).wait_send()

        @pl.when((k_x == 0) & (k_z != 0))
        def _():
            last_copy_a(d, k_z).wait_send()

        @pl.when((k_z == 0) & (k_x != 0))
        def _():
            last_copy_b(d, k_x).wait_send()

        return carry

    lax.fori_loop(0, DATES, finish, 0)
    for copy in copies:
        copy.wait_send()


def front_call(states, flags):
    paths = states.shape[2]
    columns = DATES // SIDE + 1
    dma = pltpu.SemaphoreType.DMA
    return pl.pallas_call(
        front_kernel,
        name="front",
        out_shape=(
            jax.ShapeDtypeStruct((DATES, 24, 128), f32),
            jax.ShapeDtypeStruct((DATES, 24, 128), f32),
            jax.ShapeDtypeStruct((DATES, 8, 128), f32),
            jax.ShapeDtypeStruct((PACKED, 128), f32),
        ),
        in_specs=[vmem()] * 2,
        out_specs=(vmem(),) * 4,
        scratch_shapes=[
            pltpu.VMEM((640, 128), f32),
            pltpu.VMEM((GROUP, 8, 128), f32),
            pltpu.VMEM((DATES, 1, paths), f32),
            pltpu.VMEM((24, paths), f32),
            pltpu.VMEM((paths // 128, 768, 128), bf16),
            pltpu.VMEM((DATES, PACKED, 128), f32),
            pltpu.VMEM((columns, SIDE, HALF, 128), f32),
            pltpu.VMEM((columns, SIDE, PACKED - HALF, 128), f32),
            pltpu.VMEM((columns, HALF, 128), f32),
            pltpu.VMEM((columns, PACKED - HALF, 128), f32),
            pltpu.VMEM((SIDE, HALF, 128), f32),
            pltpu.VMEM((SIDE, PACKED - HALF, 128), f32),
            dma((GROUP,)),
            dma((GROUP,)),
            dma((DATES,)),
            dma((DATES,)),
            dma((columns, SIDE)),
            dma((columns, SIDE)),
            dma((columns,)),
            dma((columns,)),
            dma((SIDE,)),
            dma((SIDE,)),
        ],
        compiler_params=pltpu.CompilerParams(collective_id=0, has_side_effects=True),
    )(states, flags)


def sweep_block(panel, b, start):
    height = panel.shape[0]
    columns = [
        jnp.broadcast_to(panel[:, start + c : start + c + 1], (height, 128)) for c in range(8)
    ]
    pivot = [column[8 * b : 8 * b + 8, :] for column in columns]
    row_of = lax.broadcasted_iota(jnp.int32, (8, 128), 0)
    for p in range(8):
        across = [jnp.broadcast_to(column[p : p + 1, :], (8, 128)) for column in pivot]
        inverse = 1.0 / across[p]
        own = pivot[p]
        here = row_of == p
        for c in range(8):
            if c == p:
                continue
            ratio = across[c] * inverse
            pivot[c] = jnp.where(here, ratio, pivot[c] - own * ratio)
        pivot[p] = jnp.where(here, -inverse, own * inverse)
    rows = panel[8 * b : 8 * b + 8, :]
    lane = lax.broadcasted_iota(jnp.int32, (8, 256), 1)
    swept = jnp.zeros((8, 256), f32)
    wide = [jnp.concatenate([column, column], axis=1) for column in pivot]
    for c in range(8):
        swept = swept - wide[c] * jnp.broadcast_to(rows[c : c + 1, :], (8, 256))
    for c in range(8):
        swept = jnp.where(lane == start + c, wide[c], swept)
    lane = lax.broadcasted_iota(jnp.int32, (height, 256), 1)
    rest = jnp.where((lane >= start) & (lane < start + 8), 0.0, panel)
    for c in range(8):
        wide_c = jnp.concatenate([columns[c], columns[c]], axis=1)
        rest = rest - wide_c * jnp.broadcast_to(swept[c : c + 1, :], (height, 256))
    pieces = [rest[8 * q : 8 * q + 8, :] for q in range(height // 8)]
    pieces[b] = swept
    return jnp.concatenate(pieces, axis=0)


def stacked(before, panel):
    one, two, three = three_parts(before)
    uno, due, tre = three_parts(panel)
    left = jnp.concatenate([three, two, one, two, one, one], axis=0)
    right = jnp.concatenate([uno, due, tre, uno, due, uno], axis=0)
    return left, right


def transposed_product(left, right):
    return lax.dot_general(
        left, right, (((0,), (0,)), ((), ())), preferred_element_type=f32
    )


def inverse_kernel(gram, out, work):
    rows, lanes = triangle()
    ridge = jnp.where(rows == lanes, RIDGE, 0.0).astype(f32)
    first, cross, turned, last = unpack(gram[0:128, :], gram[128:256, :], gram[256:257, :])
    work[0:128, 0:128] = first + ridge
    work[0:128, 128:256] = cross
    work[128:256, 0:128] = turned
    work[128:256, 128:256] = last + ridge
    lane = lax.broadcasted_iota(jnp.int32, (256, 256), 1)
    current = work[0:32, :]
    for top in range(0, ROWS, 32):
        before = current
        panel = before
        for b in range(4):
            if top + 8 * b < ROWS:
                panel = sweep_block(panel, b, top + 8 * b)
        deep = min(32, ROWS - top)
        if deep < 32:
            row = lax.broadcasted_iota(jnp.int32, (32, 256), 0)
            before = jnp.where(row < deep, before, 0.0)
        kept = (lane < top) | (lane >= top + deep)
        after = top + 32
        left, right = stacked(before, panel)
        if after < ROWS:
            change = transposed_product(left[:, after : after + 32], right)
            current = jnp.where(kept[0:32, :], work[after : after + 32, :], 0.0) - change
        work[...] = jnp.where(kept, work[...], 0.0) - transposed_product(left, right)
        work[top : top + deep, :] = panel[0:deep, :]
    mixed, diagonal = pack(-work[0:128, 0:128], -work[128:256, 128:256])
    out[0:128, :] = -work[0:128, 128:256]
    out[128:256, :] = mixed
    out[256:264, :] = diagonal


def inverse_call(gram):
    return pl.pallas_call(
        inverse_kernel,
        name="inverse",
        out_shape=jax.ShapeDtypeStruct((PACKED, 128), f32),
        in_specs=[vmem()],
        out_specs=vmem(),
        scratch_shapes=[pltpu.VMEM((256, 256), f32)],
    )(gram)


def chain_kernel(
    states, flags, terminal, strike, date_index, mean, inv, count, mine, move,
    cash_out, price_out, coef_out,
    y, phi, exercise, discount, value, packed, solve, slots, slots_price, coefs,
    spread_send, spread_recv, send_sem, recv_sem, price_send, price_recv,
):
    me = lax.axis_index("path")
    barrier = greet(me)
    paths = states.shape[2]
    chunks = paths // 128

    def prepare(d, par):
        mean_d = mean[d]
        inv_d = inv[d]
        for c in range(chunks):
            cut = slice(128 * c, 128 * c + 128)
            z = states[d, :, cut]
            y[0:FACTORS, cut] = (z - mean_d[0:FACTORS]) * inv_d[0:FACTORS]
            step = 1.0 / (1.0 + 0.25 * (0.03 * jnp.exp(0.25 * z)))
            running = step[0:1, :]
            discount[par, :, cut] = running
            total = running
            for j in range(1, FACTORS):
                running = running * step[j : j + 1, :]
                total = total + running
            annuity = 0.25 * total
            rate = (1.0 - running) / annuity
            exercise[par, :, cut] = 100.0 * annuity * (rate - strike[0])
        fill_basis(phi.at[par], y)

    my_z, my_x = me // SIDE, lax.rem(me, SIDE)
    spans = (slice(0, HALF), slice(HALF, PACKED))

    def along(axis, k):
        if axis == 0:
            return {"path": my_z * SIDE + lax.rem(my_x + k, SIDE)}
        return {"path": lax.rem(my_z + k, SIDE) * SIDE + my_x}

    def spread(source, d, half, axis, k, stage):
        return pltpu.make_async_remote_copy(
            src_ref=source,
            dst_ref=packed.at[d, spans[half]],
            send_sem=spread_send.at[stage, half, d // SIDE, k],
            recv_sem=spread_recv.at[half, d],
            device_id=along(axis, k),
            device_id_type=MESH_ID,
        )

    def relay(d, half):
        apart = my_z != owner_z(d) if half == 0 else my_x != owner_x(d)
        return jnp.logical_not(apart)

    def is_owner(d):
        return (my_x == owner_x(d)) & (my_z == owner_z(d))

    def rhs_copy(par, k):
        return pltpu.make_async_remote_copy(
            src_ref=slots.at[par, me],
            dst_ref=slots.at[par, me],
            send_sem=send_sem.at[par, k],
            recv_sem=recv_sem.at[par, k],
            device_id={"path": lax.rem(me + k, GROUP)},
            device_id_type=MESH_ID,
        )

    def price_copy(k):
        return pltpu.make_async_remote_copy(
            src_ref=slots_price.at[me],
            dst_ref=slots_price.at[me],
            send_sem=price_send.at[k],
            recv_sem=price_recv.at[k],
            device_id={"path": lax.rem(me + k, GROUP)},
            device_id_type=MESH_ID,
        )

    fill_rest(y)
    pl.semaphore_wait(barrier, GROUP - 1)
    own_q = lax.rem(my_z - my_x + SIDE, SIDE)
    own = own_q * SIDE + my_x

    @pl.when(own < DATES)
    def _():
        for k in range(1, SIDE):
            for half in range(2):
                spread(mine.at[spans[half]], own, half, half, k, 0).start()
        for k in range(1, SIDE):
            for half in range(2):
                spread(mine.at[spans[half]], own, half, 1 - half, k, 1).start()
        packed[own] = mine[...]

    prepare(DATES - 1, 0)
    value[...] = terminal[...]
    coefs[...] = jnp.zeros_like(coefs)
    def relay_step(t, carry):
        d = DATES - 1 - t
        for half in range(2):

            @pl.when(relay(d, half) & jnp.logical_not(is_owner(d)))
            def _(half=half):
                source = packed.at[d, spans[half]]
                spread(source, d, half, half, 1, 0).wait_recv()
                for k in range(1, SIDE):
                    spread(source, d, half, 1 - half, k, 1).start()

        return carry

    lax.fori_loop(0, DATES, relay_step, 0)

    def date_step(t, carry):
        d = DATES - 1 - t
        par = lax.rem(t, 2)
        now = phi.at[par]
        held = value[...] * discount[par]
        money = flags[pl.ds(d, 1), :].astype(f32)
        weighted = money * held
        sums = jnp.zeros((ROWS, 128), f32)
        for c in range(chunks):
            cut = slice(128 * c, 128 * c + 128)
            sums = sums + now[0:ROWS, cut] * weighted[:, cut]
        low = jnp.sum(sums[0:128, :].T, axis=0, keepdims=True)
        high = jnp.concatenate([sums[128:ROWS, :], jnp.zeros((256 - ROWS, 128), f32)], axis=0)
        high = jnp.sum(high.T, axis=0, keepdims=True)
        slots[par, me] = jnp.concatenate([low, high], axis=0)
        for k in range(1, GROUP):
            rhs_copy(par, k).start()

        for half in range(2):

            @pl.when(jnp.logical_not(relay(d, half)))
            def _(half=half):
                spread(packed.at[d, spans[half]], d, half, half, 1, 0).wait_recv()

        first, cross, turned, last = unpack(
            packed[d, 0:128, :], packed[d, 128:256, :], packed[d, 256:257, :]
        )
        solve[0:128, 0:128] = first
        solve[0:128, 128:256] = cross
        solve[128:256, 0:128] = turned
        solve[128:256, 128:256] = last
        prepare(jnp.maximum(d - 1, 0), 1 - par)

        for k in range(1, GROUP):
            rhs_copy(par, k).wait_recv()
        rhs = slots[par, 0]
        for k in range(1, GROUP):
            rhs = rhs + slots[par, k]
        rhs = rhs / count[d, 0:2, :]
        product = solve[0:ROWS, 0:128] * rhs[0:1, :] + solve[0:ROWS, 128:256] * rhs[1:2, :]
        coef = jnp.sum(product, axis=1, keepdims=True)
        coef = jnp.broadcast_to(coef, (ROWS, 128))
        lane = lax.broadcasted_iota(jnp.int32, (ROWS, 128), 1)
        coefs[0:ROWS, :] = jnp.where(lane == d, coef, coefs[0:ROWS, :])
        for c in range(chunks):
            cut = slice(128 * c, 128 * c + 128)
            continuation = jnp.sum(coef * now[0:ROWS, cut], axis=0, keepdims=True)
            gain = exercise[par, :, cut]
            open_date = (date_index[:, cut] <= d).astype(f32)
            weight = jax.nn.sigmoid((gain - continuation) / TEMPER) * money[:, cut] * open_date
            old = held[:, cut]
            value[:, cut] = old + weight * (gain - old)
        for k in range(1, GROUP):
            rhs_copy(par, k).wait_send()
        return carry

    lax.fori_loop(0, DATES, date_step, 0)

    total = jnp.zeros((1, 128), f32)
    for c in range(chunks):
        total = total + value[:, 128 * c : 128 * c + 128]
    slots_price[me] = total
    for k in range(1, GROUP):
        price_copy(k).start()
    cash_out[...] = value[...]
    turned = jnp.concatenate([coefs[0:128, :].T[0:16, :], coefs[128:256, :].T[0:16, :]], axis=1)
    ordered = jnp.zeros((16, 256), f32)
    for piece in three_parts(turned)[::-1]:
        ordered = ordered + jnp.dot(piece, move[...], preferred_element_type=f32)
    coef_out[...] = ordered[0:DATES, 0:BASIS]
    for k in range(1, GROUP):
        price_copy(k).wait_recv()
    total = slots_price[0]
    for k in range(1, GROUP):
        total = total + slots_price[k]
    price = jnp.sum(total, axis=1, keepdims=True) / (paths * GROUP)
    price_out[...] = jnp.broadcast_to(price, (1, 128))
    for k in range(1, GROUP):
        price_copy(k).wait_send()

    @pl.when(own < DATES)
    def _():
        for k in range(1, SIDE):
            for half in range(2):
                spread(mine.at[spans[half]], own, half, half, k, 0).wait_send()
                spread(mine.at[spans[half]], own, half, 1 - half, k, 1).wait_send()

    def relay_done(d, carry):
        for half in range(2):

            @pl.when(relay(d, half) & jnp.logical_not(is_owner(d)))
            def _(half=half):
                for k in range(1, SIDE):
                    spread(packed.at[d, spans[half]], d, half, 1 - half, k, 1).wait_send()

        return carry

    lax.fori_loop(0, DATES, relay_done, 0)


def chain_call(states, flags, terminal, strike, date_index, mean, inv, count, mine, move):
    paths = states.shape[2]
    return pl.pallas_call(
        chain_kernel,
        name="chain",
        out_shape=(
            jax.ShapeDtypeStruct((1, paths), f32),
            jax.ShapeDtypeStruct((1, 128), f32),
            jax.ShapeDtypeStruct((DATES, BASIS), f32),
        ),
        in_specs=[vmem()] * 3 + [pl.BlockSpec(memory_space=pltpu.SMEM)] + [vmem()] * 6,
        out_specs=(vmem(),) * 3,
        scratch_shapes=[
            pltpu.VMEM((24, paths), f32),
            pltpu.VMEM((2, ROWS, paths), f32),
            pltpu.VMEM((2, 1, paths), f32),
            pltpu.VMEM((2, 1, paths), f32),
            pltpu.VMEM((1, paths), f32),
            pltpu.VMEM((DATES, PACKED, 128), f32),
            pltpu.VMEM((256, 256), f32),
            pltpu.VMEM((2, GROUP, 2, 128), f32),
            pltpu.VMEM((GROUP, 1, 128), f32),
            pltpu.VMEM((256, 128), f32),
            pltpu.SemaphoreType.DMA((2, 2, DATES // SIDE + 1, SIDE)),
            pltpu.SemaphoreType.DMA((2, DATES)),
            pltpu.SemaphoreType.DMA((2, GROUP)),
            pltpu.SemaphoreType.DMA((2, GROUP)),
            pltpu.SemaphoreType.DMA((GROUP,)),
            pltpu.SemaphoreType.DMA((GROUP,)),
        ],
        compiler_params=pltpu.CompilerParams(collective_id=2, has_side_effects=True),
    )(states, flags, terminal, strike, date_index, mean, inv, count, mine, move)


def shards(states, flags, terminal, strike, date_index):
    paths = states.shape[2]
    mean, inv, count, system = front_call(states, flags)
    packed = inverse_call(system)
    cash, price, coefs = chain_call(
        states, flags, terminal.reshape(1, paths), strike, date_index.reshape(1, paths),
        mean, inv, count, packed, reference_order(),
    )
    return cash.reshape(paths), price[0, 0:1], coefs


def solution(mesh):
    both = ("book", "path")
    return jax.shard_map(
        shards,
        mesh=mesh,
        in_specs=(P(None, None, both), P(None, both), P(both), P("book"), P(both)),
        out_specs=(P(both), P("book"), P("book", None)),
        check_vma=False,
    )
```

```python
import functools

import jax
import jax.numpy as jnp
import numpy as np
from jax import lax
from jax.experimental import pallas as pl
from jax.experimental.pallas import tpu as pltpu
from jax.sharding import PartitionSpec as P

RIDGE = 0.05
TEMPER = 0.5
HIGHEST = lax.Precision.HIGHEST
f32 = jnp.float32
bf16 = jnp.bfloat16
GROUP = 16
DATES = 10
FACTORS = 20
BASIS = 231
ROWS = 232
PACKED = 264
HALF = 136
SIDE = 4
LAG = 2
CHUNKS = 8
MESH_ID = pl.DeviceIdType.MESH


def basis_pairs():
    pairs = []
    for base in (0, 8):
        for s in range(4):
            pairs += [(base + i, base + (i + s) % 8) for i in range(8)]
    pairs += [(i, i + 4) for i in range(4)] + [(8 + i, 8 + (i + 4) % 8) for i in range(4, 8)]
    for s in range(8):
        pairs += [(i, 8 + (i + s) % 8) for i in range(8)]
    for base in (0, 8):
        for k in range(5):
            pairs += [(base + i, 16 + k) for i in range(8)]
    pairs += [(16 + i, 16 + i) for i in range(5)] + [(16 + i, 18 + i) for i in range(3)]
    pairs += [(16 + i, 17 + i) for i in range(4)] + [(16, 19), (17, 20), (16, 20)]
    return [tuple(sorted(pair)) for pair in pairs]


def reference_order():
    left, right = np.triu_indices(FACTORS)
    wanted = [(FACTORS, FACTORS)] + [(j, FACTORS) for j in range(FACTORS)]
    wanted += list(zip(left.tolist(), right.tolist()))
    held = basis_pairs()
    move = np.zeros((256, 256), np.float32)
    for column, pair in enumerate(wanted):
        move[held.index(pair), column] = 1.0
    return jnp.asarray(move, bf16)


def owner_x(d):
    return d % SIDE


def owner_z(d):
    return (d % SIDE + d // SIDE) % SIDE


def greet(me):
    barrier = pltpu.get_barrier_semaphore()
    for k in range(1, GROUP):
        pl.semaphore_signal(
            barrier, inc=1, device_id={"path": lax.rem(me + k, GROUP)}, device_id_type=MESH_ID
        )
    return barrier


def vmem():
    return pl.BlockSpec(memory_space=pltpu.VMEM)


def three_parts(a):
    one = a.astype(bf16)
    rest = a - one.astype(f32)
    two = rest.astype(bf16)
    three = (rest - two.astype(f32)).astype(bf16)
    return one, two, three


def fill_factors(y, states_d, mean, inv):
    paths = y.shape[1]
    for c in range(paths // 128):
        cut = slice(128 * c, 128 * c + 128)
        y[0:FACTORS, cut] = (states_d(cut) - mean[0:FACTORS]) * inv[0:FACTORS]


def fill_rest(y):
    paths = y.shape[1]
    y[FACTORS : FACTORS + 1, :] = jnp.ones((1, paths), f32)
    y[FACTORS + 1 : 24, :] = jnp.zeros((23 - FACTORS, paths), f32)


def turn(rows, s):
    return rows if s == 0 else pltpu.roll(rows, 8 - s, 0)


def products(y_chunk, money=None):
    groups = [y_chunk[8 * g : 8 * g + 8, :] for g in range(3)]
    scaled = groups if money is None else [group * money for group in groups]
    turned = [turn(groups[1], s) for s in range(8)]
    pieces = [scaled[0] * turn(groups[0], s) for s in range(4)]
    pieces += [scaled[1] * turned[s] for s in range(4)]
    row = lax.broadcasted_iota(jnp.int32, groups[0].shape, 0)
    left = jnp.where(row < 4, scaled[0], scaled[1])
    pieces.append(left * jnp.where(row < 4, turn(groups[0], 4), turned[4]))
    pieces += [scaled[0] * turned[s] for s in range(8)]
    single = [jnp.broadcast_to(groups[2][k : k + 1, :], groups[0].shape) for k in range(5)]
    for g in range(2):
        pieces += [scaled[g] * single[k] for k in range(5)]
    apart = [scaled[2] * turn(groups[2], s) for s in range(5)]
    pieces.append(apart[0] + pltpu.roll(apart[2], 5, 0))
    ends = jnp.where(row < 4, apart[4], 0.0)
    pieces.append(apart[1] + pltpu.roll(apart[3], 4, 0) + pltpu.roll(ends, 6, 0))
    return pieces


def fill_basis(phi, y):
    paths = y.shape[1]

    def step(i, carry):
        cut = pl.ds(pl.multiple_of(i * 128, 128), 128)
        for q, piece in enumerate(products(y[:, cut])):
            phi[8 * q : 8 * q + 8, cut] = piece
        return carry

    lax.fori_loop(0, paths // 128, step, 0)


def triangle():
    rows = lax.broadcasted_iota(jnp.int32, (128, 128), 0)
    lanes = lax.broadcasted_iota(jnp.int32, (128, 128), 1)
    return rows, lanes


def pack(first, last):
    rows, lanes = triangle()
    mixed = jnp.where(rows > lanes, first, last)
    diagonal = jnp.sum(jnp.where(rows == lanes, first, 0.0), axis=0, keepdims=True)
    return mixed, jnp.broadcast_to(diagonal, (8, 128))


def unpack(cross, mixed, diagonal):
    rows, lanes = triangle()
    turned = mixed.T
    diagonal = jnp.broadcast_to(diagonal, (128, 128))
    first = jnp.where(rows > lanes, mixed, jnp.where(rows < lanes, turned, diagonal))
    last = jnp.where(rows <= lanes, mixed, turned)
    return first, cross, cross.T, last


def wait_all(copies):
    for copy in copies:
        copy.wait_recv()


def front(
    states, flags, mean_out, inv_out, count_out, system_out,
    part, slots, money_of, y, parts, gram, slot_a, slot_b, sum_a, sum_b, last_a, last_b,
    send_sem, recv_sem, send_a, send_b, recv_a, recv_b,
    send_last_a, send_last_b, recv_last_a, recv_last_b,
):
    me = lax.axis_index("path")
    barrier = greet(me)
    paths = states.shape[2]
    zero = jnp.zeros((24, 128), f32)
    for d in range(DATES):
        first = jnp.zeros((FACTORS, 128), f32)
        second = jnp.zeros((FACTORS, 128), f32)
        count = jnp.zeros((1, 128), f32)
        for c in range(paths // 128):
            z = states[d, :, 128 * c : 128 * c + 128]
            m = flags[d : d + 1, 128 * c : 128 * c + 128].astype(f32)
            money_of[d, :, 128 * c : 128 * c + 128] = m
            mz = m * z
            first = first + mz
            second = second + mz * z
            count = count + m
        base = 64 * d
        part[base : base + 24, :] = zero
        part[base : base + FACTORS, :] = first
        part[base + 24 : base + 48, :] = zero
        part[base + 24 : base + 24 + FACTORS, :] = second
        part[base + 48 : base + 64, :] = jnp.zeros((16, 128), f32)
        part[base + 48 : base + 49, :] = count
    mine = [
        jnp.sum(part[128 * t : 128 * t + 128, :].T, axis=0, keepdims=True) for t in range(5)
    ]
    slots[me] = jnp.concatenate(mine + [jnp.zeros((3, 128), f32)], axis=0)
    pl.semaphore_wait(barrier, GROUP - 1)
    copies = []
    for k in range(1, GROUP):
        copies.append(
            pltpu.make_async_remote_copy(
                src_ref=slots.at[me],
                dst_ref=slots.at[me],
                send_sem=send_sem.at[k],
                recv_sem=recv_sem.at[k],
                device_id={"path": lax.rem(me + k, GROUP)},
                device_id_type=MESH_ID,
            )
        )
        copies[-1].start()
    fill_rest(y)
    wait_all(copies)
    total = slots[0]
    for k in range(1, GROUP):
        total = total + slots[k]
    columns = jnp.concatenate([total, jnp.zeros((120, 128), f32)], axis=0).T
    for d in range(DATES):
        base = 64 * (d % 2)
        column = jnp.broadcast_to(columns[base : base + 64, d // 2 : d // 2 + 1], (64, 128))
        count = jnp.broadcast_to(column[48:49, :], (24, 128))
        mean = column[0:24, :] / count
        variance = column[24:48, :] / count - mean * mean
        mean_out[d] = mean
        inv_out[d] = 1.0 / jnp.sqrt(variance + 1e-05)
        count_out[d] = count[0:8, :]

    my_z, my_x = me // SIDE, lax.rem(me, SIDE)

    def copy_a(d, k):
        return pltpu.make_async_remote_copy(
            src_ref=gram.at[d, 0:HALF],
            dst_ref=slot_a.at[d // SIDE, k],
            send_sem=send_a.at[d],
            recv_sem=recv_a.at[d // SIDE, k],
            device_id={"path": my_z * SIDE + owner_x(d)},
            device_id_type=MESH_ID,
        )

    def copy_b(d, k):
        return pltpu.make_async_remote_copy(
            src_ref=gram.at[d, HALF:PACKED],
            dst_ref=slot_b.at[d // SIDE, k],
            send_sem=send_b.at[d],
            recv_sem=recv_b.at[d // SIDE, k],
            device_id={"path": owner_z(d) * SIDE + my_x},
            device_id_type=MESH_ID,
        )

    def last_copy_a(d, k):
        return pltpu.make_async_remote_copy(
            src_ref=sum_a.at[d // SIDE],
            dst_ref=last_a.at[k],
            send_sem=send_last_a.at[d // SIDE],
            recv_sem=recv_last_a.at[k],
            device_id={"path": owner_z(d) * SIDE + my_x},
            device_id_type=MESH_ID,
        )

    def last_copy_b(d, k):
        return pltpu.make_async_remote_copy(
            src_ref=sum_b.at[d // SIDE],
            dst_ref=last_b.at[k],
            send_sem=send_last_b.at[d // SIDE],
            recv_sem=recv_last_b.at[k],
            device_id={"path": my_z * SIDE + owner_x(d)},
            device_id_type=MESH_ID,
        )

    def split(d, parts, slabs):
        for c in slabs:
            cut = slice(128 * c, 128 * c + 128)
            y[0:FACTORS, cut] = (states[d, :, cut] - mean_out[d, 0:FACTORS]) * inv_out[d, 0:FACTORS]
            money = money_of[d, :, cut]
            pieces = products(y[:, cut], money)
            pieces.append(jnp.zeros((8, 128), f32))
            for q in range(0, 30, 2):
                rows = jnp.concatenate(pieces[q : q + 2], axis=0)
                for i, piece in enumerate(three_parts(rows)):
                    parts[c, 256 * i + 8 * q : 256 * i + 8 * q + 16, :] = piece

    def compute(d, parts):
        lanes = (((1,), (1,)), ((), ()))
        total = paths // 128
        step = max(total // CHUNKS, 1)
        main = jnp.zeros((256, 256), f32)
        side = jnp.zeros((256, 256), f32)
        for start in range(0, total, step):
            slabs = range(start, start + step)
            split(d, parts, slabs)
            whole = [
                jnp.concatenate(
                    [parts[c, 256 * i : 256 * i + 256, :] for c in slabs], axis=1
                )
                for i in range(3)
            ]
            for i, k in ((0, 0), (1, 1)):
                main = main + lax.dot_general(
                    whole[i], whole[k], lanes, preferred_element_type=f32
                )
            for i, k in ((0, 1), (0, 2)):
                side = side + lax.dot_general(
                    whole[i], whole[k], lanes, preferred_element_type=f32
                )
        low, high = slice(0, 128), slice(128, 256)
        gram[d, 0:128, :] = main[low, high] + (side[low, high] + side[high, low].T)
        mixed, diagonal = pack(
            main[low, low] + (side[low, low] + side[low, low].T),
            main[high, high] + (side[high, high] + side[high, high].T),
        )
        gram[d, 128:256, :] = mixed
        gram[d, 256:264, :] = diagonal

    def send(d):
        k_x = lax.rem(my_x - owner_x(d) + SIDE, SIDE)
        k_z = lax.rem(my_z - owner_z(d) + SIDE, SIDE)

        @pl.when(k_x != 0)
        def _():
            copy_a(d, k_x).start()

        @pl.when(k_z != 0)
        def _():
            copy_b(d, k_z).start()

    def collect(d):
        q = d // SIDE
        k_x = lax.rem(my_x - owner_x(d) + SIDE, SIDE)
        k_z = lax.rem(my_z - owner_z(d) + SIDE, SIDE)

        @pl.when(k_x == 0)
        def _():
            for k in range(1, SIDE):
                copy_a(d, k).wait_recv()
            sum_a[q] = (gram[d, 0:HALF] + slot_a[q, 1]) + (slot_a[q, 2] + slot_a[q, 3])

            @pl.when(k_z != 0)
            def _():
                last_copy_a(d, k_z).start()

        @pl.when(k_z == 0)
        def _():
            for k in range(1, SIDE):
                copy_b(d, k).wait_recv()
            sum_b[q] = (gram[d, HALF:PACKED] + slot_b[q, 1]) + (slot_b[q, 2] + slot_b[q, 3])

            @pl.when(k_x != 0)
            def _():
                last_copy_b(d, k_x).start()

    def date_step(d, carry):
        compute(d, parts)
        send(d)

        @pl.when(d >= LAG)
        def _():
            collect(d - LAG)

        return carry

    for i in range(3):
        parts[:, 256 * i + 240 : 256 * i + 256, :] = jnp.zeros((paths // 128, 16, 128), bf16)
    lax.fori_loop(0, DATES, date_step, 0)
    lax.fori_loop(DATES - LAG, DATES, lambda d, carry: (collect(d), carry)[1], 0)

    own_q = lax.rem(my_z - my_x + SIDE, SIDE)
    own = own_q * SIDE + my_x
    system_out[...] = jnp.zeros_like(system_out)

    @pl.when(own < DATES)
    def _():
        for k in range(1, SIDE):
            last_copy_a(own, k).wait_recv()
            last_copy_b(own, k).wait_recv()
        scale = 1.0 / count_out[own, 0:1, :]
        system_out[0:HALF] = ((sum_a[own_q] + last_a[1]) + (last_a[2] + last_a[3])) * scale
        system_out[HALF:PACKED] = ((sum_b[own_q] + last_b[1]) + (last_b[2] + last_b[3])) * scale

    def finish(d, carry):
        k_x = lax.rem(my_x - owner_x(d) + SIDE, SIDE)
        k_z = lax.rem(my_z - owner_z(d) + SIDE, SIDE)

        @pl.when(k_x != 0)
        def _():
            copy_a(d, k_x).wait_send()

        @pl.when(k_z != 0)
        def _():
            copy_b(d, k_z).wait_send()

        @pl.when((k_x == 0) & (k_z != 0))
        def _():
            last_copy_a(d, k_z).wait_send()

        @pl.when((k_z == 0) & (k_x != 0))
        def _():
            last_copy_b(d, k_x).wait_send()

        return carry

    lax.fori_loop(0, DATES, finish, 0)
    for copy in copies:
        copy.wait_send()


def sweep_block(panel, b, start):
    height = panel.shape[0]
    columns = [
        jnp.broadcast_to(panel[:, start + c : start + c + 1], (height, 128)) for c in range(8)
    ]
    pivot = [column[8 * b : 8 * b + 8, :] for column in columns]
    row_of = lax.broadcasted_iota(jnp.int32, (8, 128), 0)
    for p in range(8):
        across = [jnp.broadcast_to(column[p : p + 1, :], (8, 128)) for column in pivot]
        inverse = 1.0 / across[p]
        own = pivot[p]
        here = row_of == p
        for c in range(8):
            if c == p:
                continue
            ratio = across[c] * inverse
            pivot[c] = jnp.where(here, ratio, pivot[c] - own * ratio)
        pivot[p] = jnp.where(here, -inverse, own * inverse)
    rows = panel[8 * b : 8 * b + 8, :]
    lane = lax.broadcasted_iota(jnp.int32, (8, 256), 1)
    swept = jnp.zeros((8, 256), f32)
    wide = [jnp.concatenate([column, column], axis=1) for column in pivot]
    for c in range(8):
        swept = swept - wide[c] * jnp.broadcast_to(rows[c : c + 1, :], (8, 256))
    for c in range(8):
        swept = jnp.where(lane == start + c, wide[c], swept)
    lane = lax.broadcasted_iota(jnp.int32, (height, 256), 1)
    rest = jnp.where((lane >= start) & (lane < start + 8), 0.0, panel)
    for c in range(8):
        wide_c = jnp.concatenate([columns[c], columns[c]], axis=1)
        rest = rest - wide_c * jnp.broadcast_to(swept[c : c + 1, :], (height, 256))
    pieces = [rest[8 * q : 8 * q + 8, :] for q in range(height // 8)]
    pieces[b] = swept
    return jnp.concatenate(pieces, axis=0)


def stacked(before, panel):
    one, two, three = three_parts(before)
    uno, due, tre = three_parts(panel)
    left = jnp.concatenate([three, two, one, two, one, one], axis=0)
    right = jnp.concatenate([uno, due, tre, uno, due, uno], axis=0)
    return left, right


def transposed_product(left, right):
    return lax.dot_general(
        left, right, (((0,), (0,)), ((), ())), preferred_element_type=f32
    )


def invert(gram, out, work):
    rows, lanes = triangle()
    ridge = jnp.where(rows == lanes, RIDGE, 0.0).astype(f32)
    first, cross, turned, last = unpack(gram[0:128, :], gram[128:256, :], gram[256:257, :])
    work[0:128, 0:128] = first + ridge
    work[0:128, 128:256] = cross
    work[128:256, 0:128] = turned
    work[128:256, 128:256] = last + ridge
    lane = lax.broadcasted_iota(jnp.int32, (256, 256), 1)
    current = work[0:32, :]
    for top in range(0, ROWS, 32):
        before = current
        panel = before
        for b in range(4):
            if top + 8 * b < ROWS:
                panel = sweep_block(panel, b, top + 8 * b)
        deep = min(32, ROWS - top)
        if deep < 32:
            row = lax.broadcasted_iota(jnp.int32, (32, 256), 0)
            before = jnp.where(row < deep, before, 0.0)
        kept = (lane < top) | (lane >= top + deep)
        after = top + 32
        left, right = stacked(before, panel)
        if after < ROWS:
            change = transposed_product(left[:, after : after + 32], right)
            current = jnp.where(kept[0:32, :], work[after : after + 32, :], 0.0) - change
        work[...] = jnp.where(kept, work[...], 0.0) - transposed_product(left, right)
        work[top : top + deep, :] = panel[0:deep, :]
    mixed, diagonal = pack(-work[0:128, 0:128], -work[128:256, 128:256])
    out[0:128, :] = -work[0:128, 128:256]
    out[128:256, :] = mixed
    out[256:264, :] = diagonal


def chain(
    states, money_of, terminal, strike, date_index, mean, inv, count, mine, move,
    cash_out, price_out, coef_out,
    y, phi, exercise, discount, value, packed, solve, slots, slots_price, coefs,
    spread_send, spread_recv, send_sem, recv_sem, price_send, price_recv,
):
    me = lax.axis_index("path")
    paths = states.shape[2]
    chunks = paths // 128

    def prepare(d, par):
        mean_d = mean[d]
        inv_d = inv[d]
        for c in range(chunks):
            cut = slice(128 * c, 128 * c + 128)
            z = states[d, :, cut]
            y[0:FACTORS, cut] = (z - mean_d[0:FACTORS]) * inv_d[0:FACTORS]
            step = 1.0 / (1.0 + 0.25 * (0.03 * jnp.exp(0.25 * z)))
            running = step[0:1, :]
            discount[par, :, cut] = running
            total = running
            for j in range(1, FACTORS):
                running = running * step[j : j + 1, :]
                total = total + running
            annuity = 0.25 * total
            rate = (1.0 - running) / annuity
            exercise[par, :, cut] = 100.0 * annuity * (rate - strike[0])
        fill_basis(phi.at[par], y)

    my_z, my_x = me // SIDE, lax.rem(me, SIDE)
    spans = (slice(0, HALF), slice(HALF, PACKED))

    def along(axis, k):
        if axis == 0:
            return {"path": my_z * SIDE + lax.rem(my_x + k, SIDE)}
        return {"path": lax.rem(my_z + k, SIDE) * SIDE + my_x}

    def spread(source, d, half, axis, k, stage):
        return pltpu.make_async_remote_copy(
            src_ref=source,
            dst_ref=packed.at[d, spans[half]],
            send_sem=spread_send.at[stage, half, d // SIDE, k],
            recv_sem=spread_recv.at[half, d],
            device_id=along(axis, k),
            device_id_type=MESH_ID,
        )

    def relay(d, half):
        apart = my_z != owner_z(d) if half == 0 else my_x != owner_x(d)
        return jnp.logical_not(apart)

    def is_owner(d):
        return (my_x == owner_x(d)) & (my_z == owner_z(d))

    def rhs_copy(par, k):
        return pltpu.make_async_remote_copy(
            src_ref=slots.at[par, me],
            dst_ref=slots.at[par, me],
            send_sem=send_sem.at[par, k],
            recv_sem=recv_sem.at[par, k],
            device_id={"path": lax.rem(me + k, GROUP)},
            device_id_type=MESH_ID,
        )

    def price_copy(k):
        return pltpu.make_async_remote_copy(
            src_ref=slots_price.at[me],
            dst_ref=slots_price.at[me],
            send_sem=price_send.at[k],
            recv_sem=price_recv.at[k],
            device_id={"path": lax.rem(me + k, GROUP)},
            device_id_type=MESH_ID,
        )

    own_q = lax.rem(my_z - my_x + SIDE, SIDE)
    own = own_q * SIDE + my_x

    @pl.when(own < DATES)
    def _():
        for k in range(1, SIDE):
            for half in range(2):
                spread(mine.at[spans[half]], own, half, half, k, 0).start()
        for k in range(1, SIDE):
            for half in range(2):
                spread(mine.at[spans[half]], own, half, 1 - half, k, 1).start()
        packed[own] = mine[...]

    prepare(DATES - 1, 0)
    value[...] = terminal[...]
    coefs[...] = jnp.zeros_like(coefs)
    def relay_step(t, carry):
        d = DATES - 1 - t
        for half in range(2):

            @pl.when(relay(d, half) & jnp.logical_not(is_owner(d)))
            def _(half=half):
                source = packed.at[d, spans[half]]
                spread(source, d, half, half, 1, 0).wait_recv()
                for k in range(1, SIDE):
                    spread(source, d, half, 1 - half, k, 1).start()

        return carry

    lax.fori_loop(0, DATES, relay_step, 0)

    def date_step(t, carry):
        d = DATES - 1 - t
        par = lax.rem(t, 2)
        now = phi.at[par]
        held = value[...] * discount[par]
        money = money_of[d]
        weighted = money * held
        sums = jnp.zeros((ROWS, 128), f32)
        for c in range(chunks):
            cut = slice(128 * c, 128 * c + 128)
            sums = sums + now[0:ROWS, cut] * weighted[:, cut]
        low = jnp.sum(sums[0:128, :].T, axis=0, keepdims=True)
        high = jnp.concatenate([sums[128:ROWS, :], jnp.zeros((256 - ROWS, 128), f32)], axis=0)
        high = jnp.sum(high.T, axis=0, keepdims=True)
        slots[par, me] = jnp.concatenate([low, high], axis=0)
        for k in range(1, GROUP):
            rhs_copy(par, k).start()

        for half in range(2):

            @pl.when(jnp.logical_not(relay(d, half)))
            def _(half=half):
                spread(packed.at[d, spans[half]], d, half, half, 1, 0).wait_recv()

        first, cross, turned, last = unpack(
            packed[d, 0:128, :], packed[d, 128:256, :], packed[d, 256:257, :]
        )
        solve[0:128, 0:128] = first
        solve[0:128, 128:256] = cross
        solve[128:256, 0:128] = turned
        solve[128:256, 128:256] = last
        prepare(jnp.maximum(d - 1, 0), 1 - par)

        for k in range(1, GROUP):
            rhs_copy(par, k).wait_recv()
        rhs = slots[par, 0]
        for k in range(1, GROUP):
            rhs = rhs + slots[par, k]
        rhs = rhs / count[d, 0:2, :]
        product = solve[0:ROWS, 0:128] * rhs[0:1, :] + solve[0:ROWS, 128:256] * rhs[1:2, :]
        coef = jnp.sum(product, axis=1, keepdims=True)
        coef = jnp.broadcast_to(coef, (ROWS, 128))
        lane = lax.broadcasted_iota(jnp.int32, (ROWS, 128), 1)
        coefs[0:ROWS, :] = jnp.where(lane == d, coef, coefs[0:ROWS, :])
        for c in range(chunks):
            cut = slice(128 * c, 128 * c + 128)
            continuation = jnp.sum(coef * now[0:ROWS, cut], axis=0, keepdims=True)
            gain = exercise[par, :, cut]
            open_date = (date_index[:, cut] <= d).astype(f32)
            weight = jax.nn.sigmoid((gain - continuation) / TEMPER) * money[:, cut] * open_date
            old = held[:, cut]
            value[:, cut] = old + weight * (gain - old)
        for k in range(1, GROUP):
            rhs_copy(par, k).wait_send()
        return carry

    lax.fori_loop(0, DATES, date_step, 0)

    total = jnp.zeros((1, 128), f32)
    for c in range(chunks):
        total = total + value[:, 128 * c : 128 * c + 128]
    slots_price[me] = total
    for k in range(1, GROUP):
        price_copy(k).start()
    cash_out[...] = value[...]
    turned = jnp.concatenate([coefs[0:128, :].T[0:16, :], coefs[128:256, :].T[0:16, :]], axis=1)
    ordered = jnp.zeros((16, 256), f32)
    for piece in three_parts(turned)[::-1]:
        ordered = ordered + jnp.dot(piece, move[...], preferred_element_type=f32)
    coef_out[...] = ordered[0:DATES, 0:BASIS]
    for k in range(1, GROUP):
        price_copy(k).wait_recv()
    total = slots_price[0]
    for k in range(1, GROUP):
        total = total + slots_price[k]
    price = jnp.sum(total, axis=1, keepdims=True) / (paths * GROUP)
    price_out[...] = jnp.broadcast_to(price, (1, 128))
    for k in range(1, GROUP):
        price_copy(k).wait_send()

    @pl.when(own < DATES)
    def _():
        for k in range(1, SIDE):
            for half in range(2):
                spread(mine.at[spans[half]], own, half, half, k, 0).wait_send()
                spread(mine.at[spans[half]], own, half, 1 - half, k, 1).wait_send()

    def relay_done(d, carry):
        for half in range(2):

            @pl.when(relay(d, half) & jnp.logical_not(is_owner(d)))
            def _(half=half):
                for k in range(1, SIDE):
                    spread(packed.at[d, spans[half]], d, half, 1 - half, k, 1).wait_send()

        return carry

    lax.fori_loop(0, DATES, relay_done, 0)


FRONT_SCRATCH = 22


def whole_kernel(states, flags, terminal, strike, date_index, move, cash, price, coefs, *scratch):
    mean, inv, count, system, mine, work = scratch[:6]
    front_scratch = scratch[6 : 6 + FRONT_SCRATCH]
    money_of, y = front_scratch[2:4]
    me = lax.axis_index("path")
    front(states, flags, mean, inv, count, system, *front_scratch)
    own = lax.rem(me // SIDE - lax.rem(me, SIDE) + SIDE, SIDE) * SIDE + lax.rem(me, SIDE)

    @pl.when(own < DATES)
    def _():
        invert(system, mine, work)

    chain(
        states, money_of, terminal, strike, date_index, mean, inv, count, mine, move,
        cash, price, coefs, y, *scratch[6 + FRONT_SCRATCH :],
    )


def whole_call(states, flags, terminal, strike, date_index, move):
    paths = states.shape[2]
    columns = DATES // SIDE + 1
    dma = pltpu.SemaphoreType.DMA

    def space(*shape):
        return pltpu.VMEM(shape, f32)

    front_scratch = [
        space(640, 128),
        space(GROUP, 8, 128),
        space(DATES, 1, paths),
        space(24, paths),
        pltpu.VMEM((paths // 128, 768, 128), bf16),
        space(DATES, PACKED, 128),
        space(columns, SIDE, HALF, 128),
        space(columns, SIDE, PACKED - HALF, 128),
        space(columns, HALF, 128),
        space(columns, PACKED - HALF, 128),
        space(SIDE, HALF, 128),
        space(SIDE, PACKED - HALF, 128),
        dma((GROUP,)),
        dma((GROUP,)),
        dma((DATES,)),
        dma((DATES,)),
        dma((columns, SIDE)),
        dma((columns, SIDE)),
        dma((columns,)),
        dma((columns,)),
        dma((SIDE,)),
        dma((SIDE,)),
    ]
    assert len(front_scratch) == FRONT_SCRATCH
    return pl.pallas_call(
        whole_kernel,
        name="whole",
        out_shape=(
            jax.ShapeDtypeStruct((1, paths), f32),
            jax.ShapeDtypeStruct((1, 128), f32),
            jax.ShapeDtypeStruct((DATES, BASIS), f32),
        ),
        in_specs=[vmem()] * 3 + [pl.BlockSpec(memory_space=pltpu.SMEM)] + [vmem()] * 2,
        out_specs=(vmem(),) * 3,
        scratch_shapes=[
            space(DATES, 24, 128),
            space(DATES, 24, 128),
            space(DATES, 8, 128),
            space(PACKED, 128),
            space(PACKED, 128),
            space(256, 256),
            *front_scratch,
            space(2, ROWS, paths),
            space(2, 1, paths),
            space(2, 1, paths),
            space(1, paths),
            space(DATES, PACKED, 128),
            space(256, 256),
            space(2, GROUP, 2, 128),
            space(GROUP, 1, 128),
            space(256, 128),
            dma((2, 2, columns, SIDE)),
            dma((2, DATES)),
            dma((2, GROUP)),
            dma((2, GROUP)),
            dma((GROUP,)),
            dma((GROUP,)),
        ],
        compiler_params=pltpu.CompilerParams(collective_id=0, has_side_effects=True),
    )(states, flags, terminal, strike, date_index, move)


def shards(states, flags, terminal, strike, date_index):
    paths = states.shape[2]
    cash, price, coefs = whole_call(
        states, flags, terminal.reshape(1, paths), strike, date_index.reshape(1, paths),
        reference_order(),
    )
    return cash.reshape(paths), price[0, 0:1], coefs


def solution(mesh):
    both = ("book", "path")
    return jax.shard_map(
        shards,
        mesh=mesh,
        in_specs=(P(None, None, both), P(None, both), P(both), P("book"), P(both)),
        out_specs=(P(both), P("book"), P("book", None)),
        check_vma=False,
    )
```

```python
import functools

import jax
import jax.numpy as jnp
import numpy as np
from jax import lax
from jax.experimental import pallas as pl
from jax.experimental.pallas import tpu as pltpu
from jax.sharding import PartitionSpec as P

RIDGE = 0.05
TEMPER = 0.5
HIGHEST = lax.Precision.HIGHEST
f32 = jnp.float32
bf16 = jnp.bfloat16
GROUP = 16
DATES = 10
FACTORS = 20
BASIS = 231
ROWS = 232
PACKED = 264
HALF = 136
SIDE = 4
LAG = 2
CHUNKS = 8
MESH_ID = pl.DeviceIdType.MESH


def basis_pairs():
    pairs = []
    for base in (0, 8):
        for s in range(4):
            pairs += [(base + i, base + (i + s) % 8) for i in range(8)]
    pairs += [(i, i + 4) for i in range(4)] + [(8 + i, 8 + (i + 4) % 8) for i in range(4, 8)]
    for s in range(8):
        pairs += [(i, 8 + (i + s) % 8) for i in range(8)]
    for base in (0, 8):
        for k in range(5):
            pairs += [(base + i, 16 + k) for i in range(8)]
    pairs += [(16 + i, 16 + i) for i in range(5)] + [(16 + i, 18 + i) for i in range(3)]
    pairs += [(16 + i, 17 + i) for i in range(4)] + [(16, 19), (17, 20), (16, 20)]
    return [tuple(sorted(pair)) for pair in pairs]


def reference_order():
    left, right = np.triu_indices(FACTORS)
    wanted = [(FACTORS, FACTORS)] + [(j, FACTORS) for j in range(FACTORS)]
    wanted += list(zip(left.tolist(), right.tolist()))
    held = basis_pairs()
    move = np.zeros((256, 256), np.float32)
    for column, pair in enumerate(wanted):
        move[held.index(pair), column] = 1.0
    return jnp.asarray(move, bf16)


def owner_x(d):
    return d % SIDE


def owner_z(d):
    return (d % SIDE + d // SIDE) % SIDE


def greet(me):
    barrier = pltpu.get_barrier_semaphore()
    for k in range(1, GROUP):
        pl.semaphore_signal(
            barrier, inc=1, device_id={"path": lax.rem(me + k, GROUP)}, device_id_type=MESH_ID
        )
    return barrier


def vmem():
    return pl.BlockSpec(memory_space=pltpu.VMEM)


def three_parts(a):
    one = a.astype(bf16)
    rest = a - one.astype(f32)
    two = rest.astype(bf16)
    three = (rest - two.astype(f32)).astype(bf16)
    return one, two, three


def fill_factors(y, states_d, mean, inv):
    paths = y.shape[1]
    for c in range(paths // 128):
        cut = slice(128 * c, 128 * c + 128)
        y[0:FACTORS, cut] = (states_d(cut) - mean[0:FACTORS]) * inv[0:FACTORS]


def fill_rest(y):
    paths = y.shape[1]
    y[FACTORS : FACTORS + 1, :] = jnp.ones((1, paths), f32)
    y[FACTORS + 1 : 24, :] = jnp.zeros((23 - FACTORS, paths), f32)


def turn(rows, s):
    return rows if s == 0 else pltpu.roll(rows, 8 - s, 0)


def products(y_chunk, money=None):
    groups = [y_chunk[8 * g : 8 * g + 8, :] for g in range(3)]
    scaled = groups if money is None else [group * money for group in groups]
    turned = [turn(groups[1], s) for s in range(8)]
    pieces = [scaled[0] * turn(groups[0], s) for s in range(4)]
    pieces += [scaled[1] * turned[s] for s in range(4)]
    row = lax.broadcasted_iota(jnp.int32, groups[0].shape, 0)
    left = jnp.where(row < 4, scaled[0], scaled[1])
    pieces.append(left * jnp.where(row < 4, turn(groups[0], 4), turned[4]))
    pieces += [scaled[0] * turned[s] for s in range(8)]
    single = [jnp.broadcast_to(groups[2][k : k + 1, :], groups[0].shape) for k in range(5)]
    for g in range(2):
        pieces += [scaled[g] * single[k] for k in range(5)]
    apart = [scaled[2] * turn(groups[2], s) for s in range(5)]
    pieces.append(apart[0] + pltpu.roll(apart[2], 5, 0))
    ends = jnp.where(row < 4, apart[4], 0.0)
    pieces.append(apart[1] + pltpu.roll(apart[3], 4, 0) + pltpu.roll(ends, 6, 0))
    return pieces


def fill_basis(phi, y):
    paths = y.shape[1]

    def step(i, carry):
        cut = pl.ds(pl.multiple_of(i * 128, 128), 128)
        for q, piece in enumerate(products(y[:, cut])):
            phi[8 * q : 8 * q + 8, cut] = piece
        return carry

    lax.fori_loop(0, paths // 128, step, 0)


def triangle():
    rows = lax.broadcasted_iota(jnp.int32, (128, 128), 0)
    lanes = lax.broadcasted_iota(jnp.int32, (128, 128), 1)
    return rows, lanes


def pack(first, last):
    rows, lanes = triangle()
    mixed = jnp.where(rows > lanes, first, last)
    diagonal = jnp.sum(jnp.where(rows == lanes, first, 0.0), axis=0, keepdims=True)
    return mixed, jnp.broadcast_to(diagonal, (8, 128))


def unpack(cross, mixed, diagonal):
    rows, lanes = triangle()
    turned = mixed.T
    diagonal = jnp.broadcast_to(diagonal, (128, 128))
    first = jnp.where(rows > lanes, mixed, jnp.where(rows < lanes, turned, diagonal))
    last = jnp.where(rows <= lanes, mixed, turned)
    return first, cross, cross.T, last


def wait_all(copies):
    for copy in copies:
        copy.wait_recv()


def front(
    meanwhile, states, flags, mean_out, inv_out, count_out, system_out,
    part, slots, money_of, y, parts, gram, slot_a, slot_b, sum_a, sum_b, last_a, last_b,
    send_sem, recv_sem, send_a, send_b, recv_a, recv_b,
    send_last_a, send_last_b, recv_last_a, recv_last_b,
):
    me = lax.axis_index("path")
    barrier = greet(me)
    paths = states.shape[2]
    zero = jnp.zeros((24, 128), f32)
    for d in range(DATES):
        first = jnp.zeros((FACTORS, 128), f32)
        second = jnp.zeros((FACTORS, 128), f32)
        count = jnp.zeros((1, 128), f32)
        for c in range(paths // 128):
            z = states[d, :, 128 * c : 128 * c + 128]
            m = flags[d : d + 1, 128 * c : 128 * c + 128].astype(f32)
            money_of[d, :, 128 * c : 128 * c + 128] = m
            mz = m * z
            first = first + mz
            second = second + mz * z
            count = count + m
        base = 64 * d
        part[base : base + 24, :] = zero
        part[base : base + FACTORS, :] = first
        part[base + 24 : base + 48, :] = zero
        part[base + 24 : base + 24 + FACTORS, :] = second
        part[base + 48 : base + 64, :] = jnp.zeros((16, 128), f32)
        part[base + 48 : base + 49, :] = count
    mine = [
        jnp.sum(part[128 * t : 128 * t + 128, :].T, axis=0, keepdims=True) for t in range(5)
    ]
    slots[me] = jnp.concatenate(mine + [jnp.zeros((3, 128), f32)], axis=0)
    pl.semaphore_wait(barrier, GROUP - 1)
    copies = []
    for k in range(1, GROUP):
        copies.append(
            pltpu.make_async_remote_copy(
                src_ref=slots.at[me],
                dst_ref=slots.at[me],
                send_sem=send_sem.at[k],
                recv_sem=recv_sem.at[k],
                device_id={"path": lax.rem(me + k, GROUP)},
                device_id_type=MESH_ID,
            )
        )
        copies[-1].start()
    fill_rest(y)
    wait_all(copies)
    total = slots[0]
    for k in range(1, GROUP):
        total = total + slots[k]
    columns = jnp.concatenate([total, jnp.zeros((120, 128), f32)], axis=0).T
    for d in range(DATES):
        base = 64 * (d % 2)
        column = jnp.broadcast_to(columns[base : base + 64, d // 2 : d // 2 + 1], (64, 128))
        count = jnp.broadcast_to(column[48:49, :], (24, 128))
        mean = column[0:24, :] / count
        variance = column[24:48, :] / count - mean * mean
        mean_out[d] = mean
        inv_out[d] = 1.0 / jnp.sqrt(variance + 1e-05)
        count_out[d] = count[0:8, :]

    my_z, my_x = me // SIDE, lax.rem(me, SIDE)

    def copy_a(d, k):
        return pltpu.make_async_remote_copy(
            src_ref=gram.at[d, 0:HALF],
            dst_ref=slot_a.at[d // SIDE, k],
            send_sem=send_a.at[d],
            recv_sem=recv_a.at[d // SIDE, k],
            device_id={"path": my_z * SIDE + owner_x(d)},
            device_id_type=MESH_ID,
        )

    def copy_b(d, k):
        return pltpu.make_async_remote_copy(
            src_ref=gram.at[d, HALF:PACKED],
            dst_ref=slot_b.at[d // SIDE, k],
            send_sem=send_b.at[d],
            recv_sem=recv_b.at[d // SIDE, k],
            device_id={"path": owner_z(d) * SIDE + my_x},
            device_id_type=MESH_ID,
        )

    def last_copy_a(d, k):
        return pltpu.make_async_remote_copy(
            src_ref=sum_a.at[d // SIDE],
            dst_ref=last_a.at[k],
            send_sem=send_last_a.at[d // SIDE],
            recv_sem=recv_last_a.at[k],
            device_id={"path": owner_z(d) * SIDE + my_x},
            device_id_type=MESH_ID,
        )

    def last_copy_b(d, k):
        return pltpu.make_async_remote_copy(
            src_ref=sum_b.at[d // SIDE],
            dst_ref=last_b.at[k],
            send_sem=send_last_b.at[d // SIDE],
            recv_sem=recv_last_b.at[k],
            device_id={"path": my_z * SIDE + owner_x(d)},
            device_id_type=MESH_ID,
        )

    def split(d, parts, slabs):
        for c in slabs:
            cut = slice(128 * c, 128 * c + 128)
            y[0:FACTORS, cut] = (states[d, :, cut] - mean_out[d, 0:FACTORS]) * inv_out[d, 0:FACTORS]
            money = money_of[d, :, cut]
            pieces = products(y[:, cut], money)
            pieces.append(jnp.zeros((8, 128), f32))
            for q in range(0, 30, 2):
                rows = jnp.concatenate(pieces[q : q + 2], axis=0)
                for i, piece in enumerate(three_parts(rows)):
                    parts[c, 256 * i + 8 * q : 256 * i + 8 * q + 16, :] = piece

    def compute(d, parts):
        lanes = (((1,), (1,)), ((), ()))
        total = paths // 128
        step = max(total // CHUNKS, 1)
        main = jnp.zeros((256, 256), f32)
        side = jnp.zeros((256, 256), f32)
        for start in range(0, total, step):
            slabs = range(start, start + step)
            split(d, parts, slabs)
            whole = [
                jnp.concatenate(
                    [parts[c, 256 * i : 256 * i + 256, :] for c in slabs], axis=1
                )
                for i in range(3)
            ]
            for i, k in ((0, 0), (1, 1)):
                main = main + lax.dot_general(
                    whole[i], whole[k], lanes, preferred_element_type=f32
                )
            for i, k in ((0, 1), (0, 2)):
                side = side + lax.dot_general(
                    whole[i], whole[k], lanes, preferred_element_type=f32
                )
        low, high = slice(0, 128), slice(128, 256)
        gram[d, 0:128, :] = main[low, high] + (side[low, high] + side[high, low].T)
        mixed, diagonal = pack(
            main[low, low] + (side[low, low] + side[low, low].T),
            main[high, high] + (side[high, high] + side[high, high].T),
        )
        gram[d, 128:256, :] = mixed
        gram[d, 256:264, :] = diagonal

    def send(d):
        k_x = lax.rem(my_x - owner_x(d) + SIDE, SIDE)
        k_z = lax.rem(my_z - owner_z(d) + SIDE, SIDE)

        @pl.when(k_x != 0)
        def _():
            copy_a(d, k_x).start()

        @pl.when(k_z != 0)
        def _():
            copy_b(d, k_z).start()

    def collect(d):
        q = d // SIDE
        k_x = lax.rem(my_x - owner_x(d) + SIDE, SIDE)
        k_z = lax.rem(my_z - owner_z(d) + SIDE, SIDE)

        @pl.when(k_x == 0)
        def _():
            for k in range(1, SIDE):
                copy_a(d, k).wait_recv()
            sum_a[q] = (gram[d, 0:HALF] + slot_a[q, 1]) + (slot_a[q, 2] + slot_a[q, 3])

            @pl.when(k_z != 0)
            def _():
                last_copy_a(d, k_z).start()

        @pl.when(k_z == 0)
        def _():
            for k in range(1, SIDE):
                copy_b(d, k).wait_recv()
            sum_b[q] = (gram[d, HALF:PACKED] + slot_b[q, 1]) + (slot_b[q, 2] + slot_b[q, 3])

            @pl.when(k_x != 0)
            def _():
                last_copy_b(d, k_x).start()

    def gram_step(i, carry):
        d = DATES - 1 - i
        compute(d, parts)
        send(d)

        @pl.when(i >= LAG)
        def _():
            collect(d + LAG)

        return carry

    for i in range(3):
        parts[:, 256 * i + 240 : 256 * i + 256, :] = jnp.zeros((paths // 128, 16, 128), bf16)
    lax.fori_loop(0, DATES, gram_step, 0)
    meanwhile()
    for d in range(LAG - 1, -1, -1):
        collect(d)

    own_q = lax.rem(my_z - my_x + SIDE, SIDE)
    own = own_q * SIDE + my_x
    system_out[...] = jnp.zeros_like(system_out)

    @pl.when(own < DATES)
    def _():
        for k in range(1, SIDE):
            last_copy_a(own, k).wait_recv()
            last_copy_b(own, k).wait_recv()
        scale = 1.0 / count_out[own, 0:1, :]
        system_out[0:HALF] = ((sum_a[own_q] + last_a[1]) + (last_a[2] + last_a[3])) * scale
        system_out[HALF:PACKED] = ((sum_b[own_q] + last_b[1]) + (last_b[2] + last_b[3])) * scale

    def finish(d, carry):
        k_x = lax.rem(my_x - owner_x(d) + SIDE, SIDE)
        k_z = lax.rem(my_z - owner_z(d) + SIDE, SIDE)

        @pl.when(k_x != 0)
        def _():
            copy_a(d, k_x).wait_send()

        @pl.when(k_z != 0)
        def _():
            copy_b(d, k_z).wait_send()

        @pl.when((k_x == 0) & (k_z != 0))
        def _():
            last_copy_a(d, k_z).wait_send()

        @pl.when((k_z == 0) & (k_x != 0))
        def _():
            last_copy_b(d, k_x).wait_send()

        return carry

    lax.fori_loop(0, DATES, finish, 0)
    for copy in copies:
        copy.wait_send()


def sweep_block(panel, b, start):
    height = panel.shape[0]
    columns = [
        jnp.broadcast_to(panel[:, start + c : start + c + 1], (height, 128)) for c in range(8)
    ]
    pivot = [column[8 * b : 8 * b + 8, :] for column in columns]
    row_of = lax.broadcasted_iota(jnp.int32, (8, 128), 0)
    for p in range(8):
        across = [jnp.broadcast_to(column[p : p + 1, :], (8, 128)) for column in pivot]
        inverse = 1.0 / across[p]
        own = pivot[p]
        here = row_of == p
        for c in range(8):
            if c == p:
                continue
            ratio = across[c] * inverse
            pivot[c] = jnp.where(here, ratio, pivot[c] - own * ratio)
        pivot[p] = jnp.where(here, -inverse, own * inverse)
    rows = panel[8 * b : 8 * b + 8, :]
    lane = lax.broadcasted_iota(jnp.int32, (8, 256), 1)
    swept = jnp.zeros((8, 256), f32)
    wide = [jnp.concatenate([column, column], axis=1) for column in pivot]
    for c in range(8):
        swept = swept - wide[c] * jnp.broadcast_to(rows[c : c + 1, :], (8, 256))
    for c in range(8):
        swept = jnp.where(lane == start + c, wide[c], swept)
    lane = lax.broadcasted_iota(jnp.int32, (height, 256), 1)
    rest = jnp.where((lane >= start) & (lane < start + 8), 0.0, panel)
    for c in range(8):
        wide_c = jnp.concatenate([columns[c], columns[c]], axis=1)
        rest = rest - wide_c * jnp.broadcast_to(swept[c : c + 1, :], (height, 256))
    pieces = [rest[8 * q : 8 * q + 8, :] for q in range(height // 8)]
    pieces[b] = swept
    return jnp.concatenate(pieces, axis=0)


def stacked(before, panel):
    one, two, three = three_parts(before)
    uno, due, tre = three_parts(panel)
    left = jnp.concatenate([three, two, one, two, one, one], axis=0)
    right = jnp.concatenate([uno, due, tre, uno, due, uno], axis=0)
    return left, right


def transposed_product(left, right):
    return lax.dot_general(
        left, right, (((0,), (0,)), ((), ())), preferred_element_type=f32
    )


def invert(gram, out, work):
    rows, lanes = triangle()
    ridge = jnp.where(rows == lanes, RIDGE, 0.0).astype(f32)
    first, cross, turned, last = unpack(gram[0:128, :], gram[128:256, :], gram[256:257, :])
    work[0:128, 0:128] = first + ridge
    work[0:128, 128:256] = cross
    work[128:256, 0:128] = turned
    work[128:256, 128:256] = last + ridge
    lane = lax.broadcasted_iota(jnp.int32, (256, 256), 1)
    current = work[0:32, :]
    for top in range(0, ROWS, 32):
        before = current
        panel = before
        for b in range(4):
            if top + 8 * b < ROWS:
                panel = sweep_block(panel, b, top + 8 * b)
        deep = min(32, ROWS - top)
        if deep < 32:
            row = lax.broadcasted_iota(jnp.int32, (32, 256), 0)
            before = jnp.where(row < deep, before, 0.0)
        kept = (lane < top) | (lane >= top + deep)
        after = top + 32
        left, right = stacked(before, panel)
        if after < ROWS:
            change = transposed_product(left[:, after : after + 32], right)
            current = jnp.where(kept[0:32, :], work[after : after + 32, :], 0.0) - change
        work[...] = jnp.where(kept, work[...], 0.0) - transposed_product(left, right)
        work[top : top + deep, :] = panel[0:deep, :]
    mixed, diagonal = pack(-work[0:128, 0:128], -work[128:256, 128:256])
    out[0:128, :] = -work[0:128, 128:256]
    out[128:256, :] = mixed
    out[256:264, :] = diagonal


def chain(
    middle, states, money_of, terminal, strike, date_index, mean, inv, count, mine,
    cash_out, price_out, coef_out,
    y, phi, exercise, discount, value, packed, solve, slots, slots_price, coefs, first_coef,
    spread_send, spread_recv, send_sem, recv_sem, price_send, price_recv, first_send, first_recv,
):
    me = lax.axis_index("path")
    paths = states.shape[2]
    chunks = paths // 128

    def prepare(d, par):
        mean_d = mean[d]
        inv_d = inv[d]
        for c in range(chunks):
            cut = slice(128 * c, 128 * c + 128)
            z = states[d, :, cut]
            y[0:FACTORS, cut] = (z - mean_d[0:FACTORS]) * inv_d[0:FACTORS]
            step = 1.0 / (1.0 + 0.25 * (0.03 * jnp.exp(0.25 * z)))
            running = step[0:1, :]
            discount[par, :, cut] = running
            total = running
            for j in range(1, FACTORS):
                running = running * step[j : j + 1, :]
                total = total + running
            annuity = 0.25 * total
            rate = (1.0 - running) / annuity
            exercise[par, :, cut] = 100.0 * annuity * (rate - strike[0])
        fill_basis(phi.at[par], y)

    my_z, my_x = me // SIDE, lax.rem(me, SIDE)
    spans = (slice(0, HALF), slice(HALF, PACKED))

    def along(axis, k):
        if axis == 0:
            return {"path": my_z * SIDE + lax.rem(my_x + k, SIDE)}
        return {"path": lax.rem(my_z + k, SIDE) * SIDE + my_x}

    def spread(source, d, half, axis, k, stage):
        return pltpu.make_async_remote_copy(
            src_ref=source,
            dst_ref=packed.at[d, spans[half]],
            send_sem=spread_send.at[stage, half, d // SIDE, k],
            recv_sem=spread_recv.at[half, d],
            device_id=along(axis, k),
            device_id_type=MESH_ID,
        )

    def relay(d, half):
        apart = my_z != owner_z(d) if half == 0 else my_x != owner_x(d)
        return jnp.logical_not(apart)

    def is_owner(d):
        return (my_x == owner_x(d)) & (my_z == owner_z(d))

    def rhs_copy(par, k):
        return pltpu.make_async_remote_copy(
            src_ref=slots.at[par, me],
            dst_ref=slots.at[par, me],
            send_sem=send_sem.at[par, k],
            recv_sem=recv_sem.at[par, k],
            device_id={"path": lax.rem(me + k, GROUP)},
            device_id_type=MESH_ID,
        )

    def price_copy(k):
        return pltpu.make_async_remote_copy(
            src_ref=slots_price.at[me],
            dst_ref=slots_price.at[me],
            send_sem=price_send.at[k],
            recv_sem=price_recv.at[k],
            device_id={"path": lax.rem(me + k, GROUP)},
            device_id_type=MESH_ID,
        )

    own = lax.rem(my_z - my_x + SIDE, SIDE) * SIDE + my_x
    last = DATES - 1
    last_owner = owner_z(last) * SIDE + owner_x(last)

    def first_copy(k):
        return pltpu.make_async_remote_copy(
            src_ref=first_coef,
            dst_ref=first_coef,
            send_sem=first_send.at[k],
            recv_sem=first_recv,
            device_id={"path": lax.rem(me + k, GROUP)},
            device_id_type=MESH_ID,
        )

    def send_rhs(t):
        par = lax.rem(t, 2)
        held = value[...] * discount[par]
        value[...] = held
        weighted = money_of[last - t] * held
        sums = jnp.zeros((ROWS, 128), f32)
        for c in range(chunks):
            cut = slice(128 * c, 128 * c + 128)
            sums = sums + phi[par, :, cut] * weighted[:, cut]
        low = jnp.sum(sums[0:128, :].T, axis=0, keepdims=True)
        high = jnp.concatenate([sums[128:ROWS, :], jnp.zeros((256 - ROWS, 128), f32)], axis=0)
        high = jnp.sum(high.T, axis=0, keepdims=True)
        slots[par, me] = jnp.concatenate([low, high], axis=0)
        for k in range(1, GROUP):
            rhs_copy(par, k).start()

    def unpack_into_solve(source):
        first, cross, turned, end = unpack(source[0:128, :], source[128:256, :], source[256:257, :])
        solve[0:128, 0:128] = first
        solve[0:128, 128:256] = cross
        solve[128:256, 0:128] = turned
        solve[128:256, 128:256] = end

    def solved(t):
        par = lax.rem(t, 2)
        rhs = slots[par, 0]
        for k in range(1, GROUP):
            rhs = rhs + slots[par, k]
        rhs = rhs / count[last - t, 0:2, :]
        product = solve[0:ROWS, 0:128] * rhs[0:1, :] + solve[0:ROWS, 128:256] * rhs[1:2, :]
        return jnp.broadcast_to(jnp.sum(product, axis=1, keepdims=True), (ROWS, 128))

    def finish_date(t, coef):
        d = last - t
        par = lax.rem(t, 2)
        lane = lax.broadcasted_iota(jnp.int32, (ROWS, 128), 1)
        coefs[0:ROWS, :] = jnp.where(lane == d, coef, coefs[0:ROWS, :])
        for c in range(chunks):
            cut = slice(128 * c, 128 * c + 128)
            continuation = jnp.sum(coef * phi[par, :, cut], axis=0, keepdims=True)
            gain = exercise[par, :, cut]
            open_date = (date_index[:, cut] <= d).astype(f32)
            money = money_of[d, :, cut]
            weight = jax.nn.sigmoid((gain - continuation) / TEMPER) * money * open_date
            old = value[:, cut]
            value[:, cut] = old + weight * (gain - old)

    def before_collecting():
        prepare(last, 0)
        value[...] = terminal[...]
        coefs[...] = jnp.zeros_like(coefs)
        send_rhs(0)

    middle(before_collecting)

    @pl.when(own < last)
    def _():
        for k in range(1, SIDE):
            for half in range(2):
                spread(mine.at[spans[half]], own, half, half, k, 0).start()
        for k in range(1, SIDE):
            for half in range(2):
                spread(mine.at[spans[half]], own, half, 1 - half, k, 1).start()
        packed[own] = mine[...]

    for k in range(1, GROUP):
        rhs_copy(0, k).wait_recv()

    @pl.when(me == last_owner)
    def _():
        unpack_into_solve(mine)
        coef = solved(0)
        high = jnp.concatenate([coef[128:ROWS, :], jnp.zeros((256 - ROWS, 128), f32)], axis=0)
        first_coef[...] = jnp.concatenate([coef[0:128, :].T[0:1, :], high.T[0:1, :]], axis=0)
        for k in range(1, GROUP):
            first_copy(k).start()

    prepare(last - 1, 1)

    def relay_step(t, carry):
        d = last - t
        for half in range(2):

            @pl.when(relay(d, half) & jnp.logical_not(is_owner(d)))
            def _(half=half):
                source = packed.at[d, spans[half]]
                spread(source, d, half, half, 1, 0).wait_recv()
                for k in range(1, SIDE):
                    spread(source, d, half, 1 - half, k, 1).start()

        return carry

    lax.fori_loop(1, DATES, relay_step, 0)

    @pl.when(me != last_owner)
    def _():
        first_copy(1).wait_recv()

    pad = jnp.zeros((127, 128), f32)
    halves = [
        jnp.concatenate([first_coef[i : i + 1, :], pad], axis=0).T[:, 0:1] for i in range(2)
    ]
    column = jnp.concatenate(halves, axis=0)[0:ROWS]
    finish_date(0, jnp.broadcast_to(column, (ROWS, 128)))
    for k in range(1, GROUP):
        rhs_copy(0, k).wait_send()
    send_rhs(1)

    def date_step(t, carry):
        d = last - t
        par = lax.rem(t, 2)
        for half in range(2):

            @pl.when(jnp.logical_not(relay(d, half)))
            def _(half=half):
                spread(packed.at[d, spans[half]], d, half, half, 1, 0).wait_recv()

        unpack_into_solve(packed.at[d])
        prepare(jnp.maximum(d - 1, 0), 1 - par)
        for k in range(1, GROUP):
            rhs_copy(par, k).wait_recv()
        finish_date(t, solved(t))
        for k in range(1, GROUP):
            rhs_copy(par, k).wait_send()

        @pl.when(t < last)
        def _():
            send_rhs(t + 1)

        return carry

    lax.fori_loop(1, DATES, date_step, 0)

    total = jnp.zeros((1, 128), f32)
    for c in range(chunks):
        total = total + value[:, 128 * c : 128 * c + 128]
    slots_price[me] = total
    for k in range(1, GROUP):
        price_copy(k).start()
    cash_out[...] = value[...]
    coef_out[...] = jnp.concatenate(
        [coefs[0:128, :].T[0:16, :], coefs[128:256, :].T[0:16, :]], axis=1
    )
    for k in range(1, GROUP):
        price_copy(k).wait_recv()
    total = slots_price[0]
    for k in range(1, GROUP):
        total = total + slots_price[k]
    price = jnp.sum(total, axis=1, keepdims=True) / (paths * GROUP)
    price_out[...] = jnp.broadcast_to(price, (1, 128))
    for k in range(1, GROUP):
        price_copy(k).wait_send()

    @pl.when(me == last_owner)
    def _():
        for k in range(1, GROUP):
            first_copy(k).wait_send()

    @pl.when(own < last)
    def _():
        for k in range(1, SIDE):
            for half in range(2):
                spread(mine.at[spans[half]], own, half, half, k, 0).wait_send()
                spread(mine.at[spans[half]], own, half, 1 - half, k, 1).wait_send()

    def relay_done(d, carry):
        for half in range(2):

            @pl.when(relay(d, half) & jnp.logical_not(is_owner(d)))
            def _(half=half):
                for k in range(1, SIDE):
                    spread(packed.at[d, spans[half]], d, half, 1 - half, k, 1).wait_send()

        return carry

    lax.fori_loop(0, last, relay_done, 0)


FRONT_SCRATCH = 22


def whole_kernel(states, flags, terminal, strike, date_index, cash, price, coefs, *scratch):
    mean, inv, count, system, mine, work = scratch[:6]
    front_scratch = scratch[6 : 6 + FRONT_SCRATCH]
    money_of, y = front_scratch[2:4]
    me = lax.axis_index("path")
    own = lax.rem(me // SIDE - lax.rem(me, SIDE) + SIDE, SIDE) * SIDE + lax.rem(me, SIDE)

    def middle(meanwhile):
        front(meanwhile, states, flags, mean, inv, count, system, *front_scratch)

        @pl.when(own < DATES)
        def _():
            invert(system, mine, work)

    chain(
        middle, states, money_of, terminal, strike, date_index, mean, inv, count, mine,
        cash, price, coefs, y, *scratch[6 + FRONT_SCRATCH :],
    )


def whole_call(states, flags, terminal, strike, date_index):
    paths = states.shape[2]
    columns = DATES // SIDE + 1
    dma = pltpu.SemaphoreType.DMA

    def space(*shape):
        return pltpu.VMEM(shape, f32)

    front_scratch = [
        space(640, 128),
        space(GROUP, 8, 128),
        space(DATES, 1, paths),
        space(24, paths),
        pltpu.VMEM((paths // 128, 768, 128), bf16),
        space(DATES, PACKED, 128),
        space(columns, SIDE, HALF, 128),
        space(columns, SIDE, PACKED - HALF, 128),
        space(columns, HALF, 128),
        space(columns, PACKED - HALF, 128),
        space(SIDE, HALF, 128),
        space(SIDE, PACKED - HALF, 128),
        dma((GROUP,)),
        dma((GROUP,)),
        dma((DATES,)),
        dma((DATES,)),
        dma((columns, SIDE)),
        dma((columns, SIDE)),
        dma((columns,)),
        dma((columns,)),
        dma((SIDE,)),
        dma((SIDE,)),
    ]
    assert len(front_scratch) == FRONT_SCRATCH
    return pl.pallas_call(
        whole_kernel,
        name="whole",
        out_shape=(
            jax.ShapeDtypeStruct((1, paths), f32),
            jax.ShapeDtypeStruct((1, 128), f32),
            jax.ShapeDtypeStruct((16, 256), f32),
        ),
        in_specs=[vmem()] * 3 + [pl.BlockSpec(memory_space=pltpu.SMEM)] + [vmem()],
        out_specs=(vmem(),) * 3,
        scratch_shapes=[
            space(DATES, 24, 128),
            space(DATES, 24, 128),
            space(DATES, 8, 128),
            space(PACKED, 128),
            space(PACKED, 128),
            space(256, 256),
            *front_scratch,
            space(2, ROWS, paths),
            space(2, 1, paths),
            space(2, 1, paths),
            space(1, paths),
            space(DATES, PACKED, 128),
            space(256, 256),
            space(2, GROUP, 2, 128),
            space(GROUP, 1, 128),
            space(256, 128),
            space(2, 128),
            dma((2, 2, columns, SIDE)),
            dma((2, DATES)),
            dma((2, GROUP)),
            dma((2, GROUP)),
            dma((GROUP,)),
            dma((GROUP,)),
            dma((GROUP,)),
            dma,
        ],
        compiler_params=pltpu.CompilerParams(collective_id=0, has_side_effects=True),
    )(states, flags, terminal, strike, date_index)


def result_kernel(cash, price, coefs, move, cash_out, price_out, coef_out):
    cash_out[...] = cash[...]
    price_out[...] = price[...]
    ordered = jnp.zeros((16, 256), f32)
    for piece in three_parts(coefs[...])[::-1]:
        ordered = ordered + jnp.dot(piece, move[...], preferred_element_type=f32)
    coef_out[...] = ordered[0:DATES, 0:BASIS]


def result_call(cash, price, coefs):
    return pl.pallas_call(
        result_kernel,
        name="result",
        out_shape=(
            jax.ShapeDtypeStruct(cash.shape, f32),
            jax.ShapeDtypeStruct((1, 128), f32),
            jax.ShapeDtypeStruct((DATES, BASIS), f32),
        ),
        in_specs=[vmem()] * 4,
        out_specs=(vmem(),) * 3,
    )(cash, price, coefs, reference_order())


def shards(states, flags, terminal, strike, date_index):
    paths = states.shape[2]
    whole = whole_call(
        states, flags, terminal.reshape(1, paths), strike, date_index.reshape(1, paths)
    )
    cash, price, coefs = result_call(*whole)
    return cash.reshape(paths), price[0, 0:1], coefs


def solution(mesh):
    both = ("book", "path")
    return jax.shard_map(
        shards,
        mesh=mesh,
        in_specs=(P(None, None, both), P(None, both), P(both), P("book"), P(both)),
        out_specs=(P(both), P("book"), P("book", None)),
        check_vma=False,
    )
```

```python
import functools

import jax
import jax.numpy as jnp
import numpy as np
from jax import lax
from jax.experimental import pallas as pl
from jax.experimental.pallas import tpu as pltpu
from jax.sharding import PartitionSpec as P

RIDGE = 0.05
TEMPER = 0.5
HIGHEST = lax.Precision.HIGHEST
f32 = jnp.float32
bf16 = jnp.bfloat16
GROUP = 16
DATES = 10
FACTORS = 20
BASIS = 231
ROWS = 232
PACKED = 264
HALF = 136
SIDE = 4
LAG = 4
CHUNKS = 8
MESH_ID = pl.DeviceIdType.MESH
FAR_FIRST = sorted(range(1, GROUP), key=lambda k: -(min(k // 4, 4 - k // 4) + min(k % 4, 4 - k % 4)))


def basis_pairs():
    pairs = []
    for base in (0, 8):
        for s in range(4):
            pairs += [(base + i, base + (i + s) % 8) for i in range(8)]
    pairs += [(i, i + 4) for i in range(4)] + [(8 + i, 8 + (i + 4) % 8) for i in range(4, 8)]
    for s in range(8):
        pairs += [(i, 8 + (i + s) % 8) for i in range(8)]
    for base in (0, 8):
        for k in range(5):
            pairs += [(base + i, 16 + k) for i in range(8)]
    pairs += [(16 + i, 16 + i) for i in range(5)] + [(16 + i, 18 + i) for i in range(3)]
    pairs += [(16 + i, 17 + i) for i in range(4)] + [(16, 19), (17, 20), (16, 20)]
    return [tuple(sorted(pair)) for pair in pairs]


def reference_order():
    left, right = np.triu_indices(FACTORS)
    wanted = [(FACTORS, FACTORS)] + [(j, FACTORS) for j in range(FACTORS)]
    wanted += list(zip(left.tolist(), right.tolist()))
    held = basis_pairs()
    move = np.zeros((256, 256), np.float32)
    for column, pair in enumerate(wanted):
        move[held.index(pair), column] = 1.0
    return jnp.asarray(move, bf16)


def owner_x(d):
    return d % SIDE


def owner_z(d):
    return (d % SIDE + d // SIDE) % SIDE


def greet(me):
    barrier = pltpu.get_barrier_semaphore()
    for k in range(1, GROUP):
        pl.semaphore_signal(
            barrier, inc=1, device_id={"path": lax.rem(me + k, GROUP)}, device_id_type=MESH_ID
        )
    return barrier


def vmem():
    return pl.BlockSpec(memory_space=pltpu.VMEM)


def three_parts(a):
    one = a.astype(bf16)
    rest = a - one.astype(f32)
    two = rest.astype(bf16)
    three = (rest - two.astype(f32)).astype(bf16)
    return one, two, three


def fill_factors(y, states_d, mean, inv):
    paths = y.shape[1]
    for c in range(paths // 128):
        cut = slice(128 * c, 128 * c + 128)
        y[0:FACTORS, cut] = (states_d(cut) - mean[0:FACTORS]) * inv[0:FACTORS]


def fill_rest(y):
    paths = y.shape[1]
    y[FACTORS : FACTORS + 1, :] = jnp.ones((1, paths), f32)
    y[FACTORS + 1 : 24, :] = jnp.zeros((23 - FACTORS, paths), f32)


def turn(rows, s):
    return rows if s == 0 else pltpu.roll(rows, 8 - s, 0)


def products(y_chunk, money=None):
    groups = [y_chunk[8 * g : 8 * g + 8, :] for g in range(3)]
    scaled = groups if money is None else [group * money for group in groups]
    turned = [turn(groups[1], s) for s in range(8)]
    pieces = [scaled[0] * turn(groups[0], s) for s in range(4)]
    pieces += [scaled[1] * turned[s] for s in range(4)]
    row = lax.broadcasted_iota(jnp.int32, groups[0].shape, 0)
    left = jnp.where(row < 4, scaled[0], scaled[1])
    pieces.append(left * jnp.where(row < 4, turn(groups[0], 4), turned[4]))
    pieces += [scaled[0] * turned[s] for s in range(8)]
    single = [jnp.broadcast_to(groups[2][k : k + 1, :], groups[0].shape) for k in range(5)]
    for g in range(2):
        pieces += [scaled[g] * single[k] for k in range(5)]
    apart = [scaled[2] * turn(groups[2], s) for s in range(5)]
    pieces.append(apart[0] + pltpu.roll(apart[2], 5, 0))
    ends = jnp.where(row < 4, apart[4], 0.0)
    pieces.append(apart[1] + pltpu.roll(apart[3], 4, 0) + pltpu.roll(ends, 6, 0))
    return pieces


def fill_basis(phi, y):
    paths = y.shape[1]

    def step(i, carry):
        cut = pl.ds(pl.multiple_of(i * 128, 128), 128)
        for q, piece in enumerate(products(y[:, cut])):
            phi[8 * q : 8 * q + 8, cut] = piece
        return carry

    lax.fori_loop(0, paths // 128, step, 0)


def triangle():
    rows = lax.broadcasted_iota(jnp.int32, (128, 128), 0)
    lanes = lax.broadcasted_iota(jnp.int32, (128, 128), 1)
    return rows, lanes


def pack(first, last):
    rows, lanes = triangle()
    mixed = jnp.where(rows > lanes, first, last)
    diagonal = jnp.sum(jnp.where(rows == lanes, first, 0.0), axis=0, keepdims=True)
    return mixed, jnp.broadcast_to(diagonal, (8, 128))


def unpack(cross, mixed, diagonal):
    rows, lanes = triangle()
    turned = mixed.T
    diagonal = jnp.broadcast_to(diagonal, (128, 128))
    first = jnp.where(rows > lanes, mixed, jnp.where(rows < lanes, turned, diagonal))
    last = jnp.where(rows <= lanes, mixed, turned)
    return first, cross, cross.T, last


def wait_all(copies):
    for copy in copies:
        copy.wait_recv()


def front(
    meanwhile, states, flags, mean_out, inv_out, count_out, system_out,
    part, slots, money_of, y, parts, gram, slot_a, slot_b, sum_a, sum_b, last_a, last_b,
    send_sem, recv_sem, send_a, send_b, recv_a, recv_b,
    send_last_a, send_last_b, recv_last_a, recv_last_b,
):
    me = lax.axis_index("path")
    barrier = greet(me)
    paths = states.shape[2]
    zero = jnp.zeros((24, 128), f32)
    for d in range(DATES):
        first = jnp.zeros((FACTORS, 128), f32)
        second = jnp.zeros((FACTORS, 128), f32)
        count = jnp.zeros((1, 128), f32)
        for c in range(paths // 128):
            z = states[d, :, 128 * c : 128 * c + 128]
            m = flags[d : d + 1, 128 * c : 128 * c + 128].astype(f32)
            money_of[d, :, 128 * c : 128 * c + 128] = m
            mz = m * z
            first = first + mz
            second = second + mz * z
            count = count + m
        base = 64 * d
        part[base : base + 24, :] = zero
        part[base : base + FACTORS, :] = first
        part[base + 24 : base + 48, :] = zero
        part[base + 24 : base + 24 + FACTORS, :] = second
        part[base + 48 : base + 64, :] = jnp.zeros((16, 128), f32)
        part[base + 48 : base + 49, :] = count
    mine = [
        jnp.sum(part[128 * t : 128 * t + 128, :].T, axis=0, keepdims=True) for t in range(5)
    ]
    slots[me] = jnp.concatenate(mine + [jnp.zeros((3, 128), f32)], axis=0)
    pl.semaphore_wait(barrier, GROUP - 1)
    copies = []
    for k in range(1, GROUP):
        copies.append(
            pltpu.make_async_remote_copy(
                src_ref=slots.at[me],
                dst_ref=slots.at[me],
                send_sem=send_sem.at[k],
                recv_sem=recv_sem.at[k],
                device_id={"path": lax.rem(me + k, GROUP)},
                device_id_type=MESH_ID,
            )
        )
        copies[-1].start()
    fill_rest(y)
    wait_all(copies)
    total = slots[0]
    for k in range(1, GROUP):
        total = total + slots[k]
    columns = jnp.concatenate([total, jnp.zeros((120, 128), f32)], axis=0).T
    for d in range(DATES):
        base = 64 * (d % 2)
        column = jnp.broadcast_to(columns[base : base + 64, d // 2 : d // 2 + 1], (64, 128))
        count = jnp.broadcast_to(column[48:49, :], (24, 128))
        mean = column[0:24, :] / count
        variance = column[24:48, :] / count - mean * mean
        mean_out[d] = mean
        inv_out[d] = 1.0 / jnp.sqrt(variance + 1e-05)
        count_out[d] = count[0:8, :]

    my_z, my_x = me // SIDE, lax.rem(me, SIDE)

    def copy_a(d, k):
        return pltpu.make_async_remote_copy(
            src_ref=gram.at[d, 0:HALF],
            dst_ref=slot_a.at[d // SIDE, k],
            send_sem=send_a.at[d],
            recv_sem=recv_a.at[d // SIDE, k],
            device_id={"path": my_z * SIDE + owner_x(d)},
            device_id_type=MESH_ID,
        )

    def copy_b(d, k):
        return pltpu.make_async_remote_copy(
            src_ref=gram.at[d, HALF:PACKED],
            dst_ref=slot_b.at[d // SIDE, k],
            send_sem=send_b.at[d],
            recv_sem=recv_b.at[d // SIDE, k],
            device_id={"path": owner_z(d) * SIDE + my_x},
            device_id_type=MESH_ID,
        )

    def last_copy_a(d, k):
        return pltpu.make_async_remote_copy(
            src_ref=sum_a.at[d // SIDE],
            dst_ref=last_a.at[k],
            send_sem=send_last_a.at[d // SIDE],
            recv_sem=recv_last_a.at[k],
            device_id={"path": owner_z(d) * SIDE + my_x},
            device_id_type=MESH_ID,
        )

    def last_copy_b(d, k):
        return pltpu.make_async_remote_copy(
            src_ref=sum_b.at[d // SIDE],
            dst_ref=last_b.at[k],
            send_sem=send_last_b.at[d // SIDE],
            recv_sem=recv_last_b.at[k],
            device_id={"path": my_z * SIDE + owner_x(d)},
            device_id_type=MESH_ID,
        )

    def split(d, parts, slabs):
        for c in slabs:
            cut = slice(128 * c, 128 * c + 128)
            y[0:FACTORS, cut] = (states[d, :, cut] - mean_out[d, 0:FACTORS]) * inv_out[d, 0:FACTORS]
            money = money_of[d, :, cut]
            pieces = products(y[:, cut], money)
            pieces.append(jnp.zeros((8, 128), f32))
            for q in range(0, 30, 2):
                rows = jnp.concatenate(pieces[q : q + 2], axis=0)
                for i, piece in enumerate(three_parts(rows)):
                    parts[c, 256 * i + 8 * q : 256 * i + 8 * q + 16, :] = piece

    def compute(d, parts):
        lanes = (((1,), (1,)), ((), ()))
        total = paths // 128
        step = max(total // CHUNKS, 1)
        main = jnp.zeros((256, 256), f32)
        side = jnp.zeros((256, 256), f32)
        for start in range(0, total, step):
            slabs = range(start, start + step)
            split(d, parts, slabs)
            whole = [
                jnp.concatenate(
                    [parts[c, 256 * i : 256 * i + 256, :] for c in slabs], axis=1
                )
                for i in range(3)
            ]
            for i, k in ((0, 0), (1, 1)):
                main = main + lax.dot_general(
                    whole[i], whole[k], lanes, preferred_element_type=f32
                )
            for i, k in ((0, 1), (0, 2)):
                side = side + lax.dot_general(
                    whole[i], whole[k], lanes, preferred_element_type=f32
                )
        low, high = slice(0, 128), slice(128, 256)
        gram[d, 0:128, :] = main[low, high] + (side[low, high] + side[high, low].T)
        mixed, diagonal = pack(
            main[low, low] + (side[low, low] + side[low, low].T),
            main[high, high] + (side[high, high] + side[high, high].T),
        )
        gram[d, 128:256, :] = mixed
        gram[d, 256:264, :] = diagonal

    def send(d):
        k_x = lax.rem(my_x - owner_x(d) + SIDE, SIDE)
        k_z = lax.rem(my_z - owner_z(d) + SIDE, SIDE)

        @pl.when(k_x != 0)
        def _():
            copy_a(d, k_x).start()

        @pl.when(k_z != 0)
        def _():
            copy_b(d, k_z).start()

    def collect(d):
        q = d // SIDE
        k_x = lax.rem(my_x - owner_x(d) + SIDE, SIDE)
        k_z = lax.rem(my_z - owner_z(d) + SIDE, SIDE)

        @pl.when(k_x == 0)
        def _():
            for k in range(1, SIDE):
                copy_a(d, k).wait_recv()
            sum_a[q] = (gram[d, 0:HALF] + slot_a[q, 1]) + (slot_a[q, 2] + slot_a[q, 3])

            @pl.when(k_z != 0)
            def _():
                last_copy_a(d, k_z).start()

        @pl.when(k_z == 0)
        def _():
            for k in range(1, SIDE):
                copy_b(d, k).wait_recv()
            sum_b[q] = (gram[d, HALF:PACKED] + slot_b[q, 1]) + (slot_b[q, 2] + slot_b[q, 3])

            @pl.when(k_x != 0)
            def _():
                last_copy_b(d, k_x).start()

    def gram_step(i, carry):
        d = DATES - 1 - i
        compute(d, parts)
        send(d)

        @pl.when(i >= LAG)
        def _():
            collect(d + LAG)

        return carry

    for i in range(3):
        parts[:, 256 * i + 240 : 256 * i + 256, :] = jnp.zeros((paths // 128, 16, 128), bf16)
    lax.fori_loop(0, DATES, gram_step, 0)
    meanwhile()
    for d in range(LAG - 1, -1, -1):
        collect(d)

    own_q = lax.rem(my_z - my_x + SIDE, SIDE)
    own = own_q * SIDE + my_x
    system_out[...] = jnp.zeros_like(system_out)

    @pl.when(own < DATES)
    def _():
        for k in range(1, SIDE):
            last_copy_a(own, k).wait_recv()
            last_copy_b(own, k).wait_recv()
        scale = 1.0 / count_out[own, 0:1, :]
        system_out[0:HALF] = ((sum_a[own_q] + last_a[1]) + (last_a[2] + last_a[3])) * scale
        system_out[HALF:PACKED] = ((sum_b[own_q] + last_b[1]) + (last_b[2] + last_b[3])) * scale

    def finish(d, carry):
        k_x = lax.rem(my_x - owner_x(d) + SIDE, SIDE)
        k_z = lax.rem(my_z - owner_z(d) + SIDE, SIDE)

        @pl.when(k_x != 0)
        def _():
            copy_a(d, k_x).wait_send()

        @pl.when(k_z != 0)
        def _():
            copy_b(d, k_z).wait_send()

        @pl.when((k_x == 0) & (k_z != 0))
        def _():
            last_copy_a(d, k_z).wait_send()

        @pl.when((k_z == 0) & (k_x != 0))
        def _():
            last_copy_b(d, k_x).wait_send()

        return carry

    lax.fori_loop(0, DATES, finish, 0)
    for copy in copies:
        copy.wait_send()


def sweep_block(panel, b, start):
    height = panel.shape[0]
    columns = [
        jnp.broadcast_to(panel[:, start + c : start + c + 1], (height, 128)) for c in range(8)
    ]
    pivot = [column[8 * b : 8 * b + 8, :] for column in columns]
    row_of = lax.broadcasted_iota(jnp.int32, (8, 128), 0)
    for p in range(8):
        across = [jnp.broadcast_to(column[p : p + 1, :], (8, 128)) for column in pivot]
        inverse = 1.0 / across[p]
        own = pivot[p]
        here = row_of == p
        for c in range(8):
            if c == p:
                continue
            ratio = across[c] * inverse
            pivot[c] = jnp.where(here, ratio, pivot[c] - own * ratio)
        pivot[p] = jnp.where(here, -inverse, own * inverse)
    rows = panel[8 * b : 8 * b + 8, :]
    lane = lax.broadcasted_iota(jnp.int32, (8, 256), 1)
    swept = jnp.zeros((8, 256), f32)
    wide = [jnp.concatenate([column, column], axis=1) for column in pivot]
    for c in range(8):
        swept = swept - wide[c] * jnp.broadcast_to(rows[c : c + 1, :], (8, 256))
    for c in range(8):
        swept = jnp.where(lane == start + c, wide[c], swept)
    lane = lax.broadcasted_iota(jnp.int32, (height, 256), 1)
    rest = jnp.where((lane >= start) & (lane < start + 8), 0.0, panel)
    for c in range(8):
        wide_c = jnp.concatenate([columns[c], columns[c]], axis=1)
        rest = rest - wide_c * jnp.broadcast_to(swept[c : c + 1, :], (height, 256))
    pieces = [rest[8 * q : 8 * q + 8, :] for q in range(height // 8)]
    pieces[b] = swept
    return jnp.concatenate(pieces, axis=0)


def stacked(before, panel):
    one, two, three = three_parts(before)
    uno, due, tre = three_parts(panel)
    left = jnp.concatenate([three, two, one, two, one, one], axis=0)
    right = jnp.concatenate([uno, due, tre, uno, due, uno], axis=0)
    return left, right


def transposed_product(left, right):
    return lax.dot_general(
        left, right, (((0,), (0,)), ((), ())), preferred_element_type=f32
    )


def invert(packing, gram, out, work):
    rows, lanes = triangle()
    ridge = jnp.where(rows == lanes, RIDGE, 0.0).astype(f32)
    first, cross, turned, last = unpack(gram[0:128, :], gram[128:256, :], gram[256:257, :])
    work[0:128, 0:128] = first + ridge
    work[0:128, 128:256] = cross
    work[128:256, 0:128] = turned
    work[128:256, 128:256] = last + ridge
    lane = lax.broadcasted_iota(jnp.int32, (256, 256), 1)
    current = work[0:32, :]
    for top in range(0, ROWS, 32):
        before = current
        panel = before
        for b in range(4):
            if top + 8 * b < ROWS:
                panel = sweep_block(panel, b, top + 8 * b)
        deep = min(32, ROWS - top)
        if deep < 32:
            row = lax.broadcasted_iota(jnp.int32, (32, 256), 0)
            before = jnp.where(row < deep, before, 0.0)
        kept = (lane < top) | (lane >= top + deep)
        after = top + 32
        left, right = stacked(before, panel)
        if after < ROWS:
            change = transposed_product(left[:, after : after + 32], right)
            current = jnp.where(kept[0:32, :], work[after : after + 32, :], 0.0) - change
        work[...] = jnp.where(kept, work[...], 0.0) - transposed_product(left, right)
        work[top : top + deep, :] = panel[0:deep, :]

    @pl.when(packing)
    def _():
        mixed, diagonal = pack(-work[0:128, 0:128], -work[128:256, 128:256])
        out[0:128, :] = -work[0:128, 128:256]
        out[128:256, :] = mixed
        out[256:264, :] = diagonal


def chain(
    middle, states, money_of, terminal, strike, date_index, mean, inv, count, mine, work,
    cash_out, price_out, coef_out,
    y, phi, exercise, discount, value, packed, solve, slots, slots_price, coefs, first_coef,
    spread_send, spread_recv, send_sem, recv_sem, price_send, price_recv, first_send, first_recv,
):
    me = lax.axis_index("path")
    paths = states.shape[2]
    chunks = paths // 128

    def prepare(d, par):
        mean_d = mean[d]
        inv_d = inv[d]
        for c in range(chunks):
            cut = slice(128 * c, 128 * c + 128)
            z = states[d, :, cut]
            y[0:FACTORS, cut] = (z - mean_d[0:FACTORS]) * inv_d[0:FACTORS]
            step = 1.0 / (1.0 + 0.25 * (0.03 * jnp.exp(0.25 * z)))
            running = step[0:1, :]
            discount[par, :, cut] = running
            total = running
            for j in range(1, FACTORS):
                running = running * step[j : j + 1, :]
                total = total + running
            annuity = 0.25 * total
            rate = (1.0 - running) / annuity
            exercise[par, :, cut] = 100.0 * annuity * (rate - strike[0])
        fill_basis(phi.at[par], y)

    my_z, my_x = me // SIDE, lax.rem(me, SIDE)
    spans = (slice(0, HALF), slice(HALF, PACKED))

    def along(axis, k):
        if axis == 0:
            return {"path": my_z * SIDE + lax.rem(my_x + k, SIDE)}
        return {"path": lax.rem(my_z + k, SIDE) * SIDE + my_x}

    def spread(source, d, half, axis, k, stage):
        return pltpu.make_async_remote_copy(
            src_ref=source,
            dst_ref=packed.at[d, spans[half]],
            send_sem=spread_send.at[stage, half, d // SIDE, k],
            recv_sem=spread_recv.at[half, d],
            device_id=along(axis, k),
            device_id_type=MESH_ID,
        )

    def relay(d, half):
        apart = my_z != owner_z(d) if half == 0 else my_x != owner_x(d)
        return jnp.logical_not(apart)

    def is_owner(d):
        return (my_x == owner_x(d)) & (my_z == owner_z(d))

    def rhs_copy(par, k):
        return pltpu.make_async_remote_copy(
            src_ref=slots.at[par, me],
            dst_ref=slots.at[par, me],
            send_sem=send_sem.at[par, k],
            recv_sem=recv_sem.at[par, k],
            device_id={"path": lax.rem(me + k, GROUP)},
            device_id_type=MESH_ID,
        )

    def price_copy(k):
        return pltpu.make_async_remote_copy(
            src_ref=slots_price.at[me],
            dst_ref=slots_price.at[me],
            send_sem=price_send.at[k],
            recv_sem=price_recv.at[k],
            device_id={"path": lax.rem(me + k, GROUP)},
            device_id_type=MESH_ID,
        )

    own = lax.rem(my_z - my_x + SIDE, SIDE) * SIDE + my_x
    last = DATES - 1
    last_owner = owner_z(last) * SIDE + owner_x(last)

    def first_copy(k):
        return pltpu.make_async_remote_copy(
            src_ref=first_coef,
            dst_ref=first_coef,
            send_sem=first_send.at[k],
            recv_sem=first_recv,
            device_id={"path": lax.rem(me + k, GROUP)},
            device_id_type=MESH_ID,
        )

    def send_rhs(t):
        par = lax.rem(t, 2)
        held = value[...] * discount[par]
        value[...] = held
        weighted = money_of[last - t] * held
        sums = jnp.zeros((ROWS, 128), f32)
        for c in range(chunks):
            cut = slice(128 * c, 128 * c + 128)
            sums = sums + phi[par, :, cut] * weighted[:, cut]
        low = jnp.sum(sums[0:128, :].T, axis=0, keepdims=True)
        high = jnp.concatenate([sums[128:ROWS, :], jnp.zeros((256 - ROWS, 128), f32)], axis=0)
        high = jnp.sum(high.T, axis=0, keepdims=True)
        slots[par, me] = jnp.concatenate([low, high], axis=0)
        for k in FAR_FIRST:
            rhs_copy(par, k).start()

    def unpack_into_solve(source):
        first, cross, turned, end = unpack(source[0:128, :], source[128:256, :], source[256:257, :])
        solve[0:128, 0:128] = first
        solve[0:128, 128:256] = cross
        solve[128:256, 0:128] = turned
        solve[128:256, 128:256] = end

    def solved(t):
        par = lax.rem(t, 2)
        rhs = slots[par, 0]
        for k in range(1, GROUP):
            rhs = rhs + slots[par, k]
        rhs = rhs / count[last - t, 0:2, :]
        product = solve[0:ROWS, 0:128] * rhs[0:1, :] + solve[0:ROWS, 128:256] * rhs[1:2, :]
        return jnp.broadcast_to(jnp.sum(product, axis=1, keepdims=True), (ROWS, 128))

    def finish_date(t, coef):
        d = last - t
        par = lax.rem(t, 2)
        lane = lax.broadcasted_iota(jnp.int32, (ROWS, 128), 1)
        coefs[0:ROWS, :] = jnp.where(lane == d, coef, coefs[0:ROWS, :])
        for c in range(chunks):
            cut = slice(128 * c, 128 * c + 128)
            continuation = jnp.sum(coef * phi[par, :, cut], axis=0, keepdims=True)
            gain = exercise[par, :, cut]
            open_date = (date_index[:, cut] <= d).astype(f32)
            money = money_of[d, :, cut]
            weight = jax.nn.sigmoid((gain - continuation) / TEMPER) * money * open_date
            old = value[:, cut]
            value[:, cut] = old + weight * (gain - old)

    def before_collecting():
        prepare(last, 0)
        value[...] = terminal[...]
        coefs[...] = jnp.zeros_like(coefs)
        send_rhs(0)

    middle(before_collecting)

    @pl.when(own < last)
    def _():
        for k in range(1, SIDE):
            for half in range(2):
                spread(mine.at[spans[half]], own, half, half, k, 0).start()
        for k in range(1, SIDE):
            for half in range(2):
                spread(mine.at[spans[half]], own, half, 1 - half, k, 1).start()
        packed[own] = mine[...]

    for k in range(1, GROUP):
        rhs_copy(0, k).wait_recv()

    @pl.when(me == last_owner)
    def _():
        solve[...] = -work[...]
        coef = solved(0)
        high = jnp.concatenate([coef[128:ROWS, :], jnp.zeros((256 - ROWS, 128), f32)], axis=0)
        first_coef[...] = jnp.concatenate([coef[0:128, :].T[0:1, :], high.T[0:1, :]], axis=0)
        for k in FAR_FIRST:
            first_copy(k).start()

    prepare(last - 1, 1)

    def relay_step(t, carry):
        d = last - t
        for half in range(2):

            @pl.when(relay(d, half) & jnp.logical_not(is_owner(d)))
            def _(half=half):
                source = packed.at[d, spans[half]]
                spread(source, d, half, half, 1, 0).wait_recv()
                for k in range(1, SIDE):
                    spread(source, d, half, 1 - half, k, 1).start()

        return carry

    lax.fori_loop(1, DATES, relay_step, 0)

    @pl.when(me != last_owner)
    def _():
        first_copy(1).wait_recv()

    pad = jnp.zeros((127, 128), f32)
    halves = [
        jnp.concatenate([first_coef[i : i + 1, :], pad], axis=0).T[:, 0:1] for i in range(2)
    ]
    column = jnp.concatenate(halves, axis=0)[0:ROWS]
    finish_date(0, jnp.broadcast_to(column, (ROWS, 128)))
    send_rhs(1)

    def date_step(t, carry):
        d = last - t
        par = lax.rem(t, 2)
        for half in range(2):

            @pl.when(jnp.logical_not(relay(d, half)))
            def _(half=half):
                spread(packed.at[d, spans[half]], d, half, half, 1, 0).wait_recv()

        unpack_into_solve(packed.at[d])
        prepare(jnp.maximum(d - 1, 0), 1 - par)
        for k in range(1, GROUP):
            rhs_copy(1 - par, k).wait_send()
        for k in range(1, GROUP):
            rhs_copy(par, k).wait_recv()
        finish_date(t, solved(t))

        @pl.when(t < last)
        def _():
            send_rhs(t + 1)

        return carry

    lax.fori_loop(1, DATES, date_step, 0)

    total = jnp.zeros((1, 128), f32)
    for c in range(chunks):
        total = total + value[:, 128 * c : 128 * c + 128]
    slots_price[me] = total
    for k in FAR_FIRST:
        price_copy(k).start()
    cash_out[...] = value[...]
    coef_out[...] = jnp.concatenate(
        [coefs[0:128, :].T[0:16, :], coefs[128:256, :].T[0:16, :]], axis=1
    )
    for k in range(1, GROUP):
        price_copy(k).wait_recv()
    total = slots_price[0]
    for k in range(1, GROUP):
        total = total + slots_price[k]
    price = jnp.sum(total, axis=1, keepdims=True) / (paths * GROUP)
    price_out[...] = jnp.broadcast_to(price, (1, 128))
    for k in range(1, GROUP):
        price_copy(k).wait_send()
        rhs_copy(last % 2, k).wait_send()

    @pl.when(me == last_owner)
    def _():
        for k in range(1, GROUP):
            first_copy(k).wait_send()

    @pl.when(own < last)
    def _():
        for k in range(1, SIDE):
            for half in range(2):
                spread(mine.at[spans[half]], own, half, half, k, 0).wait_send()
                spread(mine.at[spans[half]], own, half, 1 - half, k, 1).wait_send()

    def relay_done(d, carry):
        for half in range(2):

            @pl.when(relay(d, half) & jnp.logical_not(is_owner(d)))
            def _(half=half):
                for k in range(1, SIDE):
                    spread(packed.at[d, spans[half]], d, half, 1 - half, k, 1).wait_send()

        return carry

    lax.fori_loop(0, last, relay_done, 0)


FRONT_SCRATCH = 22


def whole_kernel(states, flags, terminal, strike, date_index, cash, price, coefs, *scratch):
    mean, inv, count, system, mine, work = scratch[:6]
    front_scratch = scratch[6 : 6 + FRONT_SCRATCH]
    money_of, y = front_scratch[2:4]
    me = lax.axis_index("path")
    own = lax.rem(me // SIDE - lax.rem(me, SIDE) + SIDE, SIDE) * SIDE + lax.rem(me, SIDE)

    def middle(meanwhile):
        front(meanwhile, states, flags, mean, inv, count, system, *front_scratch)

        @pl.when(own < DATES)
        def _():
            invert(own != DATES - 1, system, mine, work)

    chain(
        middle, states, money_of, terminal, strike, date_index, mean, inv, count, mine, work,
        cash, price, coefs, y, *scratch[6 + FRONT_SCRATCH :],
    )


def whole_call(states, flags, terminal, strike, date_index):
    paths = states.shape[2]
    columns = DATES // SIDE + 1
    dma = pltpu.SemaphoreType.DMA

    def space(*shape):
        return pltpu.VMEM(shape, f32)

    front_scratch = [
        space(640, 128),
        space(GROUP, 8, 128),
        space(DATES, 1, paths),
        space(24, paths),
        pltpu.VMEM((paths // 128, 768, 128), bf16),
        space(DATES, PACKED, 128),
        space(columns, SIDE, HALF, 128),
        space(columns, SIDE, PACKED - HALF, 128),
        space(columns, HALF, 128),
        space(columns, PACKED - HALF, 128),
        space(SIDE, HALF, 128),
        space(SIDE, PACKED - HALF, 128),
        dma((GROUP,)),
        dma((GROUP,)),
        dma((DATES,)),
        dma((DATES,)),
        dma((columns, SIDE)),
        dma((columns, SIDE)),
        dma((columns,)),
        dma((columns,)),
        dma((SIDE,)),
        dma((SIDE,)),
    ]
    assert len(front_scratch) == FRONT_SCRATCH
    return pl.pallas_call(
        whole_kernel,
        name="whole",
        out_shape=(
            jax.ShapeDtypeStruct((1, paths), f32),
            jax.ShapeDtypeStruct((1, 128), f32),
            jax.ShapeDtypeStruct((16, 256), f32),
        ),
        in_specs=[vmem()] * 3 + [pl.BlockSpec(memory_space=pltpu.SMEM)] + [vmem()],
        out_specs=(vmem(),) * 3,
        scratch_shapes=[
            space(DATES, 24, 128),
            space(DATES, 24, 128),
            space(DATES, 8, 128),
            space(PACKED, 128),
            space(PACKED, 128),
            space(256, 256),
            *front_scratch,
            space(2, ROWS, paths),
            space(2, 1, paths),
            space(2, 1, paths),
            space(1, paths),
            space(DATES, PACKED, 128),
            space(256, 256),
            space(2, GROUP, 2, 128),
            space(GROUP, 1, 128),
            space(256, 128),
            space(2, 128),
            dma((2, 2, columns, SIDE)),
            dma((2, DATES)),
            dma((2, GROUP)),
            dma((2, GROUP)),
            dma((GROUP,)),
            dma((GROUP,)),
            dma((GROUP,)),
            dma,
        ],
        compiler_params=pltpu.CompilerParams(collective_id=0, has_side_effects=True),
    )(states, flags, terminal, strike, date_index)


def result_kernel(cash, price, coefs, move, cash_out, price_out, coef_out):
    cash_out[...] = cash[...]
    price_out[...] = price[...]
    ordered = jnp.zeros((16, 256), f32)
    for piece in three_parts(coefs[...])[::-1]:
        ordered = ordered + jnp.dot(piece, move[...], preferred_element_type=f32)
    coef_out[...] = ordered[0:DATES, 0:BASIS]


def result_call(cash, price, coefs):
    return pl.pallas_call(
        result_kernel,
        name="result",
        out_shape=(
            jax.ShapeDtypeStruct(cash.shape, f32),
            jax.ShapeDtypeStruct((1, 128), f32),
            jax.ShapeDtypeStruct((DATES, BASIS), f32),
        ),
        in_specs=[vmem()] * 4,
        out_specs=(vmem(),) * 3,
    )(cash, price, coefs, reference_order())


def shards(states, flags, terminal, strike, date_index):
    paths = states.shape[2]
    whole = whole_call(
        states, flags, terminal.reshape(1, paths), strike, date_index.reshape(1, paths)
    )
    cash, price, coefs = result_call(*whole)
    return cash.reshape(paths), price[0, 0:1], coefs


def solution(mesh):
    both = ("book", "path")
    return jax.shard_map(
        shards,
        mesh=mesh,
        in_specs=(P(None, None, both), P(None, both), P(both), P("book"), P(both)),
        out_specs=(P(both), P("book"), P("book", None)),
        check_vma=False,
    )
```

```python
import functools

import jax
import jax.numpy as jnp
import numpy as np
from jax import lax
from jax.experimental import pallas as pl
from jax.experimental.pallas import tpu as pltpu
from jax.sharding import PartitionSpec as P

RIDGE = 0.05
TEMPER = 0.5
HIGHEST = lax.Precision.HIGHEST
f32 = jnp.float32
bf16 = jnp.bfloat16
GROUP = 16
DATES = 10
FACTORS = 20
BASIS = 231
ROWS = 232
PACKED = 264
HALF = 136
SIDE = 4
LAG = 4
AHEAD = 3
CHUNKS = 8
MESH_ID = pl.DeviceIdType.MESH
FAR_FIRST = sorted(range(1, GROUP), key=lambda k: -(min(k // 4, 4 - k // 4) + min(k % 4, 4 - k % 4)))


def basis_pairs():
    pairs = []
    for base in (0, 8):
        for s in range(4):
            pairs += [(base + i, base + (i + s) % 8) for i in range(8)]
    pairs += [(i, i + 4) for i in range(4)] + [(8 + i, 8 + (i + 4) % 8) for i in range(4, 8)]
    for s in range(8):
        pairs += [(i, 8 + (i + s) % 8) for i in range(8)]
    for base in (0, 8):
        for k in range(5):
            pairs += [(base + i, 16 + k) for i in range(8)]
    pairs += [(16 + i, 16 + i) for i in range(5)] + [(16 + i, 18 + i) for i in range(3)]
    pairs += [(16 + i, 17 + i) for i in range(4)] + [(16, 19), (17, 20), (16, 20)]
    return [tuple(sorted(pair)) for pair in pairs]


def reference_order():
    left, right = np.triu_indices(FACTORS)
    wanted = [(FACTORS, FACTORS)] + [(j, FACTORS) for j in range(FACTORS)]
    wanted += list(zip(left.tolist(), right.tolist()))
    held = basis_pairs()
    move = np.zeros((256, 256), np.float32)
    for column, pair in enumerate(wanted):
        move[held.index(pair), column] = 1.0
    return jnp.asarray(move, bf16)


def owner_x(d):
    return d % SIDE


def owner_z(d):
    return (d % SIDE + d // SIDE) % SIDE


def greet(me):
    barrier = pltpu.get_barrier_semaphore()
    for k in range(1, GROUP):
        pl.semaphore_signal(
            barrier, inc=1, device_id={"path": lax.rem(me + k, GROUP)}, device_id_type=MESH_ID
        )
    return barrier


def vmem():
    return pl.BlockSpec(memory_space=pltpu.VMEM)


def three_parts(a):
    one = a.astype(bf16)
    rest = a - one.astype(f32)
    two = rest.astype(bf16)
    three = (rest - two.astype(f32)).astype(bf16)
    return one, two, three


def fill_factors(y, states_d, mean, inv):
    paths = y.shape[1]
    for c in range(paths // 128):
        cut = slice(128 * c, 128 * c + 128)
        y[0:FACTORS, cut] = (states_d(cut) - mean[0:FACTORS]) * inv[0:FACTORS]


def fill_rest(y):
    paths = y.shape[1]
    y[FACTORS : FACTORS + 1, :] = jnp.ones((1, paths), f32)
    y[FACTORS + 1 : 24, :] = jnp.zeros((23 - FACTORS, paths), f32)


def turn(rows, s):
    return rows if s == 0 else pltpu.roll(rows, 8 - s, 0)


def products(y_chunk, money=None):
    groups = [y_chunk[8 * g : 8 * g + 8, :] for g in range(3)]
    scaled = groups if money is None else [group * money for group in groups]
    turned = [turn(groups[1], s) for s in range(8)]
    pieces = [scaled[0] * turn(groups[0], s) for s in range(4)]
    pieces += [scaled[1] * turned[s] for s in range(4)]
    row = lax.broadcasted_iota(jnp.int32, groups[0].shape, 0)
    left = jnp.where(row < 4, scaled[0], scaled[1])
    pieces.append(left * jnp.where(row < 4, turn(groups[0], 4), turned[4]))
    pieces += [scaled[0] * turned[s] for s in range(8)]
    single = [jnp.broadcast_to(groups[2][k : k + 1, :], groups[0].shape) for k in range(5)]
    for g in range(2):
        pieces += [scaled[g] * single[k] for k in range(5)]
    apart = [scaled[2] * turn(groups[2], s) for s in range(5)]
    pieces.append(apart[0] + pltpu.roll(apart[2], 5, 0))
    ends = jnp.where(row < 4, apart[4], 0.0)
    pieces.append(apart[1] + pltpu.roll(apart[3], 4, 0) + pltpu.roll(ends, 6, 0))
    return pieces


def fill_basis(phi, y):
    paths = y.shape[1]

    def step(i, carry):
        cut = pl.ds(pl.multiple_of(i * 128, 128), 128)
        for q, piece in enumerate(products(y[:, cut])):
            phi[8 * q : 8 * q + 8, cut] = piece
        return carry

    lax.fori_loop(0, paths // 128, step, 0)


def triangle():
    rows = lax.broadcasted_iota(jnp.int32, (128, 128), 0)
    lanes = lax.broadcasted_iota(jnp.int32, (128, 128), 1)
    return rows, lanes


def pack(first, last):
    rows, lanes = triangle()
    mixed = jnp.where(rows > lanes, first, last)
    diagonal = jnp.sum(jnp.where(rows == lanes, first, 0.0), axis=0, keepdims=True)
    return mixed, jnp.broadcast_to(diagonal, (8, 128))


def unpack(cross, mixed, diagonal):
    rows, lanes = triangle()
    turned = mixed.T
    diagonal = jnp.broadcast_to(diagonal, (128, 128))
    first = jnp.where(rows > lanes, mixed, jnp.where(rows < lanes, turned, diagonal))
    last = jnp.where(rows <= lanes, mixed, turned)
    return first, cross, cross.T, last


def wait_all(copies):
    for copy in copies:
        copy.wait_recv()


def front(
    meanwhile, states, flags, mean_out, inv_out, count_out, system_out,
    part, slots, money_of, y, parts, gram, slot_a, slot_b, sum_a, sum_b, last_a, last_b,
    send_sem, recv_sem, send_a, send_b, recv_a, recv_b,
    send_last_a, send_last_b, recv_last_a, recv_last_b,
):
    me = lax.axis_index("path")
    barrier = greet(me)
    paths = states.shape[2]
    zero = jnp.zeros((24, 128), f32)
    for d in range(DATES):
        first = jnp.zeros((FACTORS, 128), f32)
        second = jnp.zeros((FACTORS, 128), f32)
        count = jnp.zeros((1, 128), f32)
        for c in range(paths // 128):
            z = states[d, :, 128 * c : 128 * c + 128]
            m = flags[d : d + 1, 128 * c : 128 * c + 128].astype(f32)
            money_of[d, :, 128 * c : 128 * c + 128] = m
            mz = m * z
            first = first + mz
            second = second + mz * z
            count = count + m
        base = 64 * d
        part[base : base + 24, :] = zero
        part[base : base + FACTORS, :] = first
        part[base + 24 : base + 48, :] = zero
        part[base + 24 : base + 24 + FACTORS, :] = second
        part[base + 48 : base + 64, :] = jnp.zeros((16, 128), f32)
        part[base + 48 : base + 49, :] = count
    mine = [
        jnp.sum(part[128 * t : 128 * t + 128, :].T, axis=0, keepdims=True) for t in range(5)
    ]
    slots[me] = jnp.concatenate(mine + [jnp.zeros((3, 128), f32)], axis=0)
    pl.semaphore_wait(barrier, GROUP - 1)
    copies = []
    for k in range(1, GROUP):
        copies.append(
            pltpu.make_async_remote_copy(
                src_ref=slots.at[me],
                dst_ref=slots.at[me],
                send_sem=send_sem.at[k],
                recv_sem=recv_sem.at[k],
                device_id={"path": lax.rem(me + k, GROUP)},
                device_id_type=MESH_ID,
            )
        )
        copies[-1].start()
    fill_rest(y)
    wait_all(copies)
    total = slots[0]
    for k in range(1, GROUP):
        total = total + slots[k]
    columns = jnp.concatenate([total, jnp.zeros((120, 128), f32)], axis=0).T
    for d in range(DATES):
        base = 64 * (d % 2)
        column = jnp.broadcast_to(columns[base : base + 64, d // 2 : d // 2 + 1], (64, 128))
        count = jnp.broadcast_to(column[48:49, :], (24, 128))
        mean = column[0:24, :] / count
        variance = column[24:48, :] / count - mean * mean
        mean_out[d] = mean
        inv_out[d] = 1.0 / jnp.sqrt(variance + 1e-05)
        count_out[d] = count[0:8, :]

    my_z, my_x = me // SIDE, lax.rem(me, SIDE)

    def copy_a(d, k):
        return pltpu.make_async_remote_copy(
            src_ref=gram.at[d, 0:HALF],
            dst_ref=slot_a.at[d // SIDE, k],
            send_sem=send_a.at[d],
            recv_sem=recv_a.at[d // SIDE, k],
            device_id={"path": my_z * SIDE + owner_x(d)},
            device_id_type=MESH_ID,
        )

    def copy_b(d, k):
        return pltpu.make_async_remote_copy(
            src_ref=gram.at[d, HALF:PACKED],
            dst_ref=slot_b.at[d // SIDE, k],
            send_sem=send_b.at[d],
            recv_sem=recv_b.at[d // SIDE, k],
            device_id={"path": owner_z(d) * SIDE + my_x},
            device_id_type=MESH_ID,
        )

    def last_copy_a(d, k):
        return pltpu.make_async_remote_copy(
            src_ref=sum_a.at[d // SIDE],
            dst_ref=last_a.at[k],
            send_sem=send_last_a.at[d // SIDE],
            recv_sem=recv_last_a.at[k],
            device_id={"path": owner_z(d) * SIDE + my_x},
            device_id_type=MESH_ID,
        )

    def last_copy_b(d, k):
        return pltpu.make_async_remote_copy(
            src_ref=sum_b.at[d // SIDE],
            dst_ref=last_b.at[k],
            send_sem=send_last_b.at[d // SIDE],
            recv_sem=recv_last_b.at[k],
            device_id={"path": my_z * SIDE + owner_x(d)},
            device_id_type=MESH_ID,
        )

    def split(d, parts, slabs):
        for c in slabs:
            cut = slice(128 * c, 128 * c + 128)
            y[0:FACTORS, cut] = (states[d, :, cut] - mean_out[d, 0:FACTORS]) * inv_out[d, 0:FACTORS]
            money = money_of[d, :, cut]
            pieces = products(y[:, cut], money)
            pieces.append(jnp.zeros((8, 128), f32))
            for q in range(0, 30, 2):
                rows = jnp.concatenate(pieces[q : q + 2], axis=0)
                for i, piece in enumerate(three_parts(rows)):
                    parts[c, 256 * i + 8 * q : 256 * i + 8 * q + 16, :] = piece

    def compute(d, parts):
        lanes = (((1,), (1,)), ((), ()))
        total = paths // 128
        step = max(total // CHUNKS, 1)
        main = jnp.zeros((256, 256), f32)
        side = jnp.zeros((256, 256), f32)
        for start in range(0, total, step):
            slabs = range(start, start + step)
            split(d, parts, slabs)
            whole = [
                jnp.concatenate(
                    [parts[c, 256 * i : 256 * i + 256, :] for c in slabs], axis=1
                )
                for i in range(3)
            ]
            for i, k in ((0, 0), (1, 1)):
                main = main + lax.dot_general(
                    whole[i], whole[k], lanes, preferred_element_type=f32
                )
            for i, k in ((0, 1), (0, 2)):
                side = side + lax.dot_general(
                    whole[i], whole[k], lanes, preferred_element_type=f32
                )
        low, high = slice(0, 128), slice(128, 256)
        gram[d, 0:128, :] = main[low, high] + (side[low, high] + side[high, low].T)
        mixed, diagonal = pack(
            main[low, low] + (side[low, low] + side[low, low].T),
            main[high, high] + (side[high, high] + side[high, high].T),
        )
        gram[d, 128:256, :] = mixed
        gram[d, 256:264, :] = diagonal

    def send(d):
        k_x = lax.rem(my_x - owner_x(d) + SIDE, SIDE)
        k_z = lax.rem(my_z - owner_z(d) + SIDE, SIDE)

        @pl.when(k_x != 0)
        def _():
            copy_a(d, k_x).start()

        @pl.when(k_z != 0)
        def _():
            copy_b(d, k_z).start()

    def collect(d):
        q = d // SIDE
        k_x = lax.rem(my_x - owner_x(d) + SIDE, SIDE)
        k_z = lax.rem(my_z - owner_z(d) + SIDE, SIDE)

        @pl.when(k_x == 0)
        def _():
            for k in range(1, SIDE):
                copy_a(d, k).wait_recv()
            sum_a[q] = (gram[d, 0:HALF] + slot_a[q, 1]) + (slot_a[q, 2] + slot_a[q, 3])

            @pl.when(k_z != 0)
            def _():
                last_copy_a(d, k_z).start()

        @pl.when(k_z == 0)
        def _():
            for k in range(1, SIDE):
                copy_b(d, k).wait_recv()
            sum_b[q] = (gram[d, HALF:PACKED] + slot_b[q, 1]) + (slot_b[q, 2] + slot_b[q, 3])

            @pl.when(k_x != 0)
            def _():
                last_copy_b(d, k_x).start()

    def gram_step(i, carry):
        d = DATES - 1 - i
        compute(d, parts)
        send(d)

        @pl.when(i >= LAG)
        def _():
            collect(d + LAG)

        return carry

    for i in range(3):
        parts[:, 256 * i + 240 : 256 * i + 256, :] = jnp.zeros((paths // 128, 16, 128), bf16)
    lax.fori_loop(0, DATES, gram_step, 0)
    meanwhile()
    for d in range(LAG - 1, -1, -1):
        collect(d)

    own_q = lax.rem(my_z - my_x + SIDE, SIDE)
    own = own_q * SIDE + my_x
    system_out[...] = jnp.zeros_like(system_out)

    @pl.when(own < DATES)
    def _():
        for k in range(1, SIDE):
            last_copy_a(own, k).wait_recv()
            last_copy_b(own, k).wait_recv()
        scale = 1.0 / count_out[own, 0:1, :]
        system_out[0:HALF] = ((sum_a[own_q] + last_a[1]) + (last_a[2] + last_a[3])) * scale
        system_out[HALF:PACKED] = ((sum_b[own_q] + last_b[1]) + (last_b[2] + last_b[3])) * scale

    def finish(d, carry):
        k_x = lax.rem(my_x - owner_x(d) + SIDE, SIDE)
        k_z = lax.rem(my_z - owner_z(d) + SIDE, SIDE)

        @pl.when(k_x != 0)
        def _():
            copy_a(d, k_x).wait_send()

        @pl.when(k_z != 0)
        def _():
            copy_b(d, k_z).wait_send()

        @pl.when((k_x == 0) & (k_z != 0))
        def _():
            last_copy_a(d, k_z).wait_send()

        @pl.when((k_z == 0) & (k_x != 0))
        def _():
            last_copy_b(d, k_x).wait_send()

        return carry

    lax.fori_loop(0, DATES, finish, 0)
    for copy in copies:
        copy.wait_send()


def sweep_block(panel, b, start):
    height = panel.shape[0]
    columns = [
        jnp.broadcast_to(panel[:, start + c : start + c + 1], (height, 128)) for c in range(8)
    ]
    pivot = [column[8 * b : 8 * b + 8, :] for column in columns]
    row_of = lax.broadcasted_iota(jnp.int32, (8, 128), 0)
    for p in range(8):
        across = [jnp.broadcast_to(column[p : p + 1, :], (8, 128)) for column in pivot]
        inverse = 1.0 / across[p]
        own = pivot[p]
        here = row_of == p
        for c in range(8):
            if c == p:
                continue
            ratio = across[c] * inverse
            pivot[c] = jnp.where(here, ratio, pivot[c] - own * ratio)
        pivot[p] = jnp.where(here, -inverse, own * inverse)
    rows = panel[8 * b : 8 * b + 8, :]
    lane = lax.broadcasted_iota(jnp.int32, (8, 256), 1)
    swept = jnp.zeros((8, 256), f32)
    wide = [jnp.concatenate([column, column], axis=1) for column in pivot]
    for c in range(8):
        swept = swept - wide[c] * jnp.broadcast_to(rows[c : c + 1, :], (8, 256))
    for c in range(8):
        swept = jnp.where(lane == start + c, wide[c], swept)
    lane = lax.broadcasted_iota(jnp.int32, (height, 256), 1)
    rest = jnp.where((lane >= start) & (lane < start + 8), 0.0, panel)
    for c in range(8):
        wide_c = jnp.concatenate([columns[c], columns[c]], axis=1)
        rest = rest - wide_c * jnp.broadcast_to(swept[c : c + 1, :], (height, 256))
    pieces = [rest[8 * q : 8 * q + 8, :] for q in range(height // 8)]
    pieces[b] = swept
    return jnp.concatenate(pieces, axis=0)


def stacked(before, panel):
    one, two, three = three_parts(before)
    uno, due, tre = three_parts(panel)
    left = jnp.concatenate([three, two, one, two, one, one], axis=0)
    right = jnp.concatenate([uno, due, tre, uno, due, uno], axis=0)
    return left, right


def transposed_product(left, right):
    return lax.dot_general(
        left, right, (((0,), (0,)), ((), ())), preferred_element_type=f32
    )


def invert(packing, gram, out, work):
    rows, lanes = triangle()
    ridge = jnp.where(rows == lanes, RIDGE, 0.0).astype(f32)
    first, cross, turned, last = unpack(gram[0:128, :], gram[128:256, :], gram[256:257, :])
    work[0:128, 0:128] = first + ridge
    work[0:128, 128:256] = cross
    work[128:256, 0:128] = turned
    work[128:256, 128:256] = last + ridge
    lane = lax.broadcasted_iota(jnp.int32, (256, 256), 1)
    current = work[0:32, :]
    for top in range(0, ROWS, 32):
        before = current
        panel = before
        for b in range(4):
            if top + 8 * b < ROWS:
                panel = sweep_block(panel, b, top + 8 * b)
        deep = min(32, ROWS - top)
        if deep < 32:
            row = lax.broadcasted_iota(jnp.int32, (32, 256), 0)
            before = jnp.where(row < deep, before, 0.0)
        kept = (lane < top) | (lane >= top + deep)
        after = top + 32
        left, right = stacked(before, panel)
        if after < ROWS:
            change = transposed_product(left[:, after : after + 32], right)
            current = jnp.where(kept[0:32, :], work[after : after + 32, :], 0.0) - change
        work[...] = jnp.where(kept, work[...], 0.0) - transposed_product(left, right)
        work[top : top + deep, :] = panel[0:deep, :]

    @pl.when(packing)
    def _():
        mixed, diagonal = pack(-work[0:128, 0:128], -work[128:256, 128:256])
        out[0:128, :] = -work[0:128, 128:256]
        out[128:256, :] = mixed
        out[256:264, :] = diagonal


def chain(
    middle, states, money_of, terminal, strike, date_index, mean, inv, count, mine, work, move,
    cash_out, price_out, coef_out,
    y, phi, exercise, discount, value, packed, solve, slots, slots_price, coefs, first_coef,
    spread_send, spread_recv, send_sem, recv_sem, price_send, price_recv, first_send, first_recv,
):
    me = lax.axis_index("path")
    paths = states.shape[2]
    chunks = paths // 128

    def prepare(d, par):
        mean_d = mean[d]
        inv_d = inv[d]
        for c in range(chunks):
            cut = slice(128 * c, 128 * c + 128)
            z = states[d, :, cut]
            y[0:FACTORS, cut] = (z - mean_d[0:FACTORS]) * inv_d[0:FACTORS]
            step = 1.0 / (1.0 + 0.25 * (0.03 * jnp.exp(0.25 * z)))
            running = step[0:1, :]
            discount[par, :, cut] = running
            total = running
            for j in range(1, FACTORS):
                running = running * step[j : j + 1, :]
                total = total + running
            annuity = 0.25 * total
            rate = (1.0 - running) / annuity
            exercise[par, :, cut] = 100.0 * annuity * (rate - strike[0])
        fill_basis(phi.at[par], y)

    my_z, my_x = me // SIDE, lax.rem(me, SIDE)
    spans = (slice(0, HALF), slice(HALF, PACKED))

    def along(axis, k):
        if axis == 0:
            return {"path": my_z * SIDE + lax.rem(my_x + k, SIDE)}
        return {"path": lax.rem(my_z + k, SIDE) * SIDE + my_x}

    def spread(source, d, half, axis, k, stage):
        return pltpu.make_async_remote_copy(
            src_ref=source,
            dst_ref=packed.at[d, spans[half]],
            send_sem=spread_send.at[stage, half, d // SIDE, k],
            recv_sem=spread_recv.at[half, d],
            device_id=along(axis, k),
            device_id_type=MESH_ID,
        )

    def relay(d, half):
        apart = my_z != owner_z(d) if half == 0 else my_x != owner_x(d)
        return jnp.logical_not(apart)

    def is_owner(d):
        return (my_x == owner_x(d)) & (my_z == owner_z(d))

    def rhs_copy(par, k):
        return pltpu.make_async_remote_copy(
            src_ref=slots.at[par, me],
            dst_ref=slots.at[par, me],
            send_sem=send_sem.at[par, k],
            recv_sem=recv_sem.at[par, k],
            device_id={"path": lax.rem(me + k, GROUP)},
            device_id_type=MESH_ID,
        )

    def price_copy(k):
        return pltpu.make_async_remote_copy(
            src_ref=slots_price.at[me],
            dst_ref=slots_price.at[me],
            send_sem=price_send.at[k],
            recv_sem=price_recv.at[k],
            device_id={"path": lax.rem(me + k, GROUP)},
            device_id_type=MESH_ID,
        )

    own = lax.rem(my_z - my_x + SIDE, SIDE) * SIDE + my_x
    last = DATES - 1
    last_owner = owner_z(last) * SIDE + owner_x(last)

    def first_copy(k):
        return pltpu.make_async_remote_copy(
            src_ref=first_coef,
            dst_ref=first_coef,
            send_sem=first_send.at[k],
            recv_sem=first_recv,
            device_id={"path": lax.rem(me + k, GROUP)},
            device_id_type=MESH_ID,
        )

    def send_rhs(t):
        par = lax.rem(t, 2)
        held = value[...] * discount[par]
        value[...] = held
        weighted = money_of[last - t] * held
        sums = jnp.zeros((ROWS, 128), f32)
        for c in range(chunks):
            cut = slice(128 * c, 128 * c + 128)
            sums = sums + phi[par, :, cut] * weighted[:, cut]
        low = jnp.sum(sums[0:128, :].T, axis=0, keepdims=True)
        high = jnp.concatenate([sums[128:ROWS, :], jnp.zeros((256 - ROWS, 128), f32)], axis=0)
        high = jnp.sum(high.T, axis=0, keepdims=True)
        slots[par, me] = jnp.concatenate([low, high], axis=0)
        for k in FAR_FIRST:
            rhs_copy(par, k).start()

    def unpack_into_solve(source):
        first, cross, turned, end = unpack(source[0:128, :], source[128:256, :], source[256:257, :])
        solve[0:128, 0:128] = first
        solve[0:128, 128:256] = cross
        solve[128:256, 0:128] = turned
        solve[128:256, 128:256] = end

    def solved(t):
        par = lax.rem(t, 2)
        rhs = slots[par, 0]
        for k in range(1, GROUP):
            rhs = rhs + slots[par, k]
        rhs = rhs / count[last - t, 0:2, :]
        product = solve[0:ROWS, 0:128] * rhs[0:1, :] + solve[0:ROWS, 128:256] * rhs[1:2, :]
        return jnp.broadcast_to(jnp.sum(product, axis=1, keepdims=True), (ROWS, 128))

    def finish_date(t, coef):
        d = last - t
        par = lax.rem(t, 2)
        lane = lax.broadcasted_iota(jnp.int32, (ROWS, 128), 1)
        coefs[0:ROWS, :] = jnp.where(lane == d, coef, coefs[0:ROWS, :])
        for c in range(chunks):
            cut = slice(128 * c, 128 * c + 128)
            continuation = jnp.sum(coef * phi[par, :, cut], axis=0, keepdims=True)
            gain = exercise[par, :, cut]
            open_date = (date_index[:, cut] <= d).astype(f32)
            money = money_of[d, :, cut]
            weight = jax.nn.sigmoid((gain - continuation) / TEMPER) * money * open_date
            old = value[:, cut]
            value[:, cut] = old + weight * (gain - old)

    def before_collecting():
        prepare(last, 0)
        value[...] = terminal[...]
        coefs[...] = jnp.zeros_like(coefs)
        send_rhs(0)

    middle(before_collecting)

    @pl.when(own < last)
    def _():
        for k in range(1, SIDE):
            for half in range(2):
                spread(mine.at[spans[half]], own, half, half, k, 0).start()
        packed[own] = mine[...]

    for k in range(1, GROUP):
        rhs_copy(0, k).wait_recv()

    @pl.when(me == last_owner)
    def _():
        solve[...] = -work[...]
        coef = solved(0)
        high = jnp.concatenate([coef[128:ROWS, :], jnp.zeros((256 - ROWS, 128), f32)], axis=0)
        first_coef[...] = jnp.concatenate([coef[0:128, :].T[0:1, :], high.T[0:1, :]], axis=0)
        for k in FAR_FIRST:
            first_copy(k).start()

    prepare(last - 1, 1)

    def relay_date(d):
        for half in range(2):

            @pl.when(relay(d, half))
            def _(half=half):
                source = packed.at[d, spans[half]]

                @pl.when(jnp.logical_not(is_owner(d)))
                def _():
                    spread(source, d, half, half, 1, 0).wait_recv()

                for k in range(1, SIDE):
                    spread(source, d, half, 1 - half, k, 1).start()

    for t in range(1, AHEAD):
        relay_date(last - t)

    @pl.when(me != last_owner)
    def _():
        first_copy(1).wait_recv()

    pad = jnp.zeros((127, 128), f32)
    halves = [
        jnp.concatenate([first_coef[i : i + 1, :], pad], axis=0).T[:, 0:1] for i in range(2)
    ]
    column = jnp.concatenate(halves, axis=0)[0:ROWS]
    finish_date(0, jnp.broadcast_to(column, (ROWS, 128)))
    send_rhs(1)

    def date_step(t, carry):
        d = last - t
        par = lax.rem(t, 2)
        for half in range(2):

            @pl.when(jnp.logical_not(relay(d, half)))
            def _(half=half):
                spread(packed.at[d, spans[half]], d, half, half, 1, 0).wait_recv()


        @pl.when(t + AHEAD <= last + 1)
        def _():
            relay_date(last + 1 - t - AHEAD)

        unpack_into_solve(packed.at[d])
        prepare(jnp.maximum(d - 1, 0), 1 - par)
        for k in range(1, GROUP):
            rhs_copy(1 - par, k).wait_send()
        for k in range(1, GROUP):
            rhs_copy(par, k).wait_recv()
        finish_date(t, solved(t))

        @pl.when(t < last)
        def _():
            send_rhs(t + 1)

        return carry

    lax.fori_loop(1, DATES, date_step, 0)

    total = jnp.zeros((1, 128), f32)
    for c in range(chunks):
        total = total + value[:, 128 * c : 128 * c + 128]
    slots_price[me] = total
    for k in FAR_FIRST:
        price_copy(k).start()
    cash_out[...] = value[...]
    turned = jnp.concatenate([coefs[0:128, :].T[0:16, :], coefs[128:256, :].T[0:16, :]], axis=1)
    ordered = jnp.zeros((16, 256), f32)
    for piece in three_parts(turned)[::-1]:
        ordered = ordered + jnp.dot(piece, move[...], preferred_element_type=f32)
    coef_out[...] = ordered[0:DATES, 0:BASIS]
    for k in range(1, GROUP):
        price_copy(k).wait_recv()
    total = slots_price[0]
    for k in range(1, GROUP):
        total = total + slots_price[k]
    price = jnp.sum(total, axis=1, keepdims=True) / (paths * GROUP)
    price_out[...] = jnp.broadcast_to(price, (1, 128))
    for k in range(1, GROUP):
        price_copy(k).wait_send()
        rhs_copy(last % 2, k).wait_send()

    @pl.when(me == last_owner)
    def _():
        for k in range(1, GROUP):
            first_copy(k).wait_send()

    @pl.when(own < last)
    def _():
        for k in range(1, SIDE):
            for half in range(2):
                spread(mine.at[spans[half]], own, half, half, k, 0).wait_send()

    def relay_done(d, carry):
        for half in range(2):

            @pl.when(relay(d, half))
            def _(half=half):
                for k in range(1, SIDE):
                    spread(packed.at[d, spans[half]], d, half, 1 - half, k, 1).wait_send()

        return carry

    lax.fori_loop(0, last, relay_done, 0)


FRONT_SCRATCH = 22


def whole_kernel(states, flags, terminal, strike, date_index, move, cash, price, coefs, *scratch):
    mean, inv, count, system, mine, work = scratch[:6]
    front_scratch = scratch[6 : 6 + FRONT_SCRATCH]
    money_of, y = front_scratch[2:4]
    me = lax.axis_index("path")
    own = lax.rem(me // SIDE - lax.rem(me, SIDE) + SIDE, SIDE) * SIDE + lax.rem(me, SIDE)

    def middle(meanwhile):
        front(meanwhile, states, flags, mean, inv, count, system, *front_scratch)

        @pl.when(own < DATES)
        def _():
            invert(own != DATES - 1, system, mine, work)

    chain(
        middle, states, money_of, terminal, strike, date_index, mean, inv, count, mine, work, move,
        cash, price, coefs, y, *scratch[6 + FRONT_SCRATCH :],
    )


def whole_call(states, flags, terminal, strike, date_index, move):
    paths = states.shape[2]
    columns = DATES // SIDE + 1
    dma = pltpu.SemaphoreType.DMA

    def space(*shape):
        return pltpu.VMEM(shape, f32)

    front_scratch = [
        space(640, 128),
        space(GROUP, 8, 128),
        space(DATES, 1, paths),
        space(24, paths),
        pltpu.VMEM((paths // 128, 768, 128), bf16),
        space(DATES, PACKED, 128),
        space(columns, SIDE, HALF, 128),
        space(columns, SIDE, PACKED - HALF, 128),
        space(columns, HALF, 128),
        space(columns, PACKED - HALF, 128),
        space(SIDE, HALF, 128),
        space(SIDE, PACKED - HALF, 128),
        dma((GROUP,)),
        dma((GROUP,)),
        dma((DATES,)),
        dma((DATES,)),
        dma((columns, SIDE)),
        dma((columns, SIDE)),
        dma((columns,)),
        dma((columns,)),
        dma((SIDE,)),
        dma((SIDE,)),
    ]
    assert len(front_scratch) == FRONT_SCRATCH
    return pl.pallas_call(
        whole_kernel,
        name="whole",
        out_shape=(
            jax.ShapeDtypeStruct((1, paths), f32),
            jax.ShapeDtypeStruct((1, 128), f32),
            jax.ShapeDtypeStruct((DATES, BASIS), f32),
        ),
        in_specs=[vmem()] * 3 + [pl.BlockSpec(memory_space=pltpu.SMEM)] + [vmem()] * 2,
        out_specs=(vmem(),) * 3,
        scratch_shapes=[
            space(DATES, 24, 128),
            space(DATES, 24, 128),
            space(DATES, 8, 128),
            space(PACKED, 128),
            space(PACKED, 128),
            space(256, 256),
            *front_scratch,
            space(2, ROWS, paths),
            space(2, 1, paths),
            space(2, 1, paths),
            space(1, paths),
            space(DATES, PACKED, 128),
            space(256, 256),
            space(2, GROUP, 2, 128),
            space(GROUP, 1, 128),
            space(256, 128),
            space(2, 128),
            dma((2, 2, columns, SIDE)),
            dma((2, DATES)),
            dma((2, GROUP)),
            dma((2, GROUP)),
            dma((GROUP,)),
            dma((GROUP,)),
            dma((GROUP,)),
            dma,
        ],
        compiler_params=pltpu.CompilerParams(collective_id=0, has_side_effects=True),
    )(states, flags, terminal, strike, date_index, move)


def result_kernel(cash, price, coefs, cash_out, price_out, coef_out):
    cash_out[...] = cash[...]
    price_out[...] = price[...]
    coef_out[...] = coefs[...]


def result_call(cash, price, coefs):
    return pl.pallas_call(
        result_kernel,
        name="result",
        out_shape=tuple(jax.ShapeDtypeStruct(a.shape, f32) for a in (cash, price, coefs)),
        in_specs=[vmem()] * 3,
        out_specs=(vmem(),) * 3,
    )(cash, price, coefs)


def shards(states, flags, terminal, strike, date_index):
    paths = states.shape[2]
    whole = whole_call(
        states, flags, terminal.reshape(1, paths), strike, date_index.reshape(1, paths),
        reference_order(),
    )
    cash, price, coefs = result_call(*whole)
    return cash.reshape(paths), price[0, 0:1], coefs


def solution(mesh):
    both = ("book", "path")
    return jax.shard_map(
        shards,
        mesh=mesh,
        in_specs=(P(None, None, both), P(None, both), P(both), P("book"), P(both)),
        out_specs=(P(both), P("book"), P("book", None)),
        check_vma=False,
    )
```

```python
import functools

import jax
import jax.numpy as jnp
import numpy as np
from jax import lax
from jax.experimental import pallas as pl
from jax.experimental.pallas import tpu as pltpu
from jax.sharding import PartitionSpec as P

RIDGE = 0.05
TEMPER = 0.5
HIGHEST = lax.Precision.HIGHEST
f32 = jnp.float32
bf16 = jnp.bfloat16
GROUP = 16
DATES = 10
FACTORS = 20
BASIS = 231
ROWS = 232
PACKED = 264
HALF = 136
SIDE = 4
LAG = 3
AHEAD = 3
CHUNKS = 8
MESH_ID = pl.DeviceIdType.MESH
FAR_FIRST = sorted(range(1, GROUP), key=lambda k: -(min(k // 4, 4 - k // 4) + min(k % 4, 4 - k % 4)))


def basis_pairs():
    pairs = []
    for base in (0, 8):
        for s in range(4):
            pairs += [(base + i, base + (i + s) % 8) for i in range(8)]
    pairs += [(i, i + 4) for i in range(4)] + [(8 + i, 8 + (i + 4) % 8) for i in range(4, 8)]
    for s in range(8):
        pairs += [(i, 8 + (i + s) % 8) for i in range(8)]
    for base in (0, 8):
        for k in range(5):
            pairs += [(base + i, 16 + k) for i in range(8)]
    pairs += [(16 + i, 16 + i) for i in range(5)] + [(16 + i, 18 + i) for i in range(3)]
    pairs += [(16 + i, 17 + i) for i in range(4)] + [(16, 19), (17, 20), (16, 20)]
    return [tuple(sorted(pair)) for pair in pairs]


def reference_order():
    left, right = np.triu_indices(FACTORS)
    wanted = [(FACTORS, FACTORS)] + [(j, FACTORS) for j in range(FACTORS)]
    wanted += list(zip(left.tolist(), right.tolist()))
    held = basis_pairs()
    move = np.zeros((256, 256), np.float32)
    for column, pair in enumerate(wanted):
        move[held.index(pair), column] = 1.0
    return jnp.asarray(move, bf16)


def owner_x(d):
    return d % SIDE


def owner_z(d):
    return (d % SIDE + d // SIDE) % SIDE


def greet(me):
    barrier = pltpu.get_barrier_semaphore()
    for k in range(1, GROUP):
        pl.semaphore_signal(
            barrier, inc=1, device_id={"path": lax.rem(me + k, GROUP)}, device_id_type=MESH_ID
        )
    return barrier


def vmem():
    return pl.BlockSpec(memory_space=pltpu.VMEM)


def three_parts(a):
    one = a.astype(bf16)
    rest = a - one.astype(f32)
    two = rest.astype(bf16)
    three = (rest - two.astype(f32)).astype(bf16)
    return one, two, three


def fill_factors(y, states_d, mean, inv):
    paths = y.shape[1]
    for c in range(paths // 128):
        cut = slice(128 * c, 128 * c + 128)
        y[0:FACTORS, cut] = (states_d(cut) - mean[0:FACTORS]) * inv[0:FACTORS]


def fill_rest(y):
    paths = y.shape[1]
    y[FACTORS : FACTORS + 1, :] = jnp.ones((1, paths), f32)
    y[FACTORS + 1 : 24, :] = jnp.zeros((23 - FACTORS, paths), f32)


def turn(rows, s):
    return rows if s == 0 else pltpu.roll(rows, 8 - s, 0)


def products(y_chunk, money=None):
    groups = [y_chunk[8 * g : 8 * g + 8, :] for g in range(3)]
    scaled = groups if money is None else [group * money for group in groups]
    turned = [turn(groups[1], s) for s in range(8)]
    pieces = [scaled[0] * turn(groups[0], s) for s in range(4)]
    pieces += [scaled[1] * turned[s] for s in range(4)]
    row = lax.broadcasted_iota(jnp.int32, groups[0].shape, 0)
    left = jnp.where(row < 4, scaled[0], scaled[1])
    pieces.append(left * jnp.where(row < 4, turn(groups[0], 4), turned[4]))
    pieces += [scaled[0] * turned[s] for s in range(8)]
    single = [jnp.broadcast_to(groups[2][k : k + 1, :], groups[0].shape) for k in range(5)]
    for g in range(2):
        pieces += [scaled[g] * single[k] for k in range(5)]
    apart = [scaled[2] * turn(groups[2], s) for s in range(5)]
    pieces.append(apart[0] + pltpu.roll(apart[2], 5, 0))
    ends = jnp.where(row < 4, apart[4], 0.0)
    pieces.append(apart[1] + pltpu.roll(apart[3], 4, 0) + pltpu.roll(ends, 6, 0))
    return pieces


def fill_basis(phi, y):
    paths = y.shape[1]

    def step(i, carry):
        cut = pl.ds(pl.multiple_of(i * 128, 128), 128)
        for q, piece in enumerate(products(y[:, cut])):
            phi[8 * q : 8 * q + 8, cut] = piece
        return carry

    lax.fori_loop(0, paths // 128, step, 0)


def triangle():
    rows = lax.broadcasted_iota(jnp.int32, (128, 128), 0)
    lanes = lax.broadcasted_iota(jnp.int32, (128, 128), 1)
    return rows, lanes


def pack(first, last):
    rows, lanes = triangle()
    mixed = jnp.where(rows > lanes, first, last)
    diagonal = jnp.sum(jnp.where(rows == lanes, first, 0.0), axis=0, keepdims=True)
    return mixed, jnp.broadcast_to(diagonal, (8, 128))


def unpack(cross, mixed, diagonal):
    rows, lanes = triangle()
    turned = mixed.T
    diagonal = jnp.broadcast_to(diagonal, (128, 128))
    first = jnp.where(rows > lanes, mixed, jnp.where(rows < lanes, turned, diagonal))
    last = jnp.where(rows <= lanes, mixed, turned)
    return first, cross, cross.T, last


def wait_all(copies):
    for copy in copies:
        copy.wait_recv()


def front(
    meanwhile, states, flags, mean_out, inv_out, count_out, system_out,
    part, slots, money_of, y, parts, gram, slot_a, slot_b, sum_a, sum_b, last_a, last_b,
    send_sem, recv_sem, send_a, send_b, recv_a, recv_b,
    send_last_a, send_last_b, recv_last_a, recv_last_b,
):
    me = lax.axis_index("path")
    barrier = greet(me)
    paths = states.shape[2]
    zero = jnp.zeros((24, 128), f32)
    for d in range(DATES):
        first = jnp.zeros((FACTORS, 128), f32)
        second = jnp.zeros((FACTORS, 128), f32)
        count = jnp.zeros((1, 128), f32)
        for c in range(paths // 128):
            z = states[d, :, 128 * c : 128 * c + 128]
            m = flags[d : d + 1, 128 * c : 128 * c + 128].astype(f32)
            money_of[d, :, 128 * c : 128 * c + 128] = m
            mz = m * z
            first = first + mz
            second = second + mz * z
            count = count + m
        base = 64 * d
        part[base : base + 24, :] = zero
        part[base : base + FACTORS, :] = first
        part[base + 24 : base + 48, :] = zero
        part[base + 24 : base + 24 + FACTORS, :] = second
        part[base + 48 : base + 64, :] = jnp.zeros((16, 128), f32)
        part[base + 48 : base + 49, :] = count
    mine = [
        jnp.sum(part[128 * t : 128 * t + 128, :].T, axis=0, keepdims=True) for t in range(5)
    ]
    slots[me] = jnp.concatenate(mine + [jnp.zeros((3, 128), f32)], axis=0)
    pl.semaphore_wait(barrier, GROUP - 1)
    copies = []
    for k in range(1, GROUP):
        copies.append(
            pltpu.make_async_remote_copy(
                src_ref=slots.at[me],
                dst_ref=slots.at[me],
                send_sem=send_sem.at[k],
                recv_sem=recv_sem.at[k],
                device_id={"path": lax.rem(me + k, GROUP)},
                device_id_type=MESH_ID,
            )
        )
        copies[-1].start()
    fill_rest(y)
    wait_all(copies)
    total = slots[0]
    for k in range(1, GROUP):
        total = total + slots[k]
    columns = jnp.concatenate([total, jnp.zeros((120, 128), f32)], axis=0).T
    for d in range(DATES):
        base = 64 * (d % 2)
        column = jnp.broadcast_to(columns[base : base + 64, d // 2 : d // 2 + 1], (64, 128))
        count = jnp.broadcast_to(column[48:49, :], (24, 128))
        mean = column[0:24, :] / count
        variance = column[24:48, :] / count - mean * mean
        mean_out[d] = mean
        inv_out[d] = 1.0 / jnp.sqrt(variance + 1e-05)
        count_out[d] = count[0:8, :]

    my_z, my_x = me // SIDE, lax.rem(me, SIDE)

    def copy_a(d, k):
        return pltpu.make_async_remote_copy(
            src_ref=gram.at[d, 0:HALF],
            dst_ref=slot_a.at[d // SIDE, k],
            send_sem=send_a.at[d],
            recv_sem=recv_a.at[d // SIDE, k],
            device_id={"path": my_z * SIDE + owner_x(d)},
            device_id_type=MESH_ID,
        )

    def copy_b(d, k):
        return pltpu.make_async_remote_copy(
            src_ref=gram.at[d, HALF:PACKED],
            dst_ref=slot_b.at[d // SIDE, k],
            send_sem=send_b.at[d],
            recv_sem=recv_b.at[d // SIDE, k],
            device_id={"path": owner_z(d) * SIDE + my_x},
            device_id_type=MESH_ID,
        )

    def last_copy_a(d, k):
        return pltpu.make_async_remote_copy(
            src_ref=sum_a.at[d // SIDE],
            dst_ref=last_a.at[k],
            send_sem=send_last_a.at[d // SIDE],
            recv_sem=recv_last_a.at[k],
            device_id={"path": owner_z(d) * SIDE + my_x},
            device_id_type=MESH_ID,
        )

    def last_copy_b(d, k):
        return pltpu.make_async_remote_copy(
            src_ref=sum_b.at[d // SIDE],
            dst_ref=last_b.at[k],
            send_sem=send_last_b.at[d // SIDE],
            recv_sem=recv_last_b.at[k],
            device_id={"path": my_z * SIDE + owner_x(d)},
            device_id_type=MESH_ID,
        )

    def split(d, parts, slabs):
        for c in slabs:
            cut = slice(128 * c, 128 * c + 128)
            y[0:FACTORS, cut] = (states[d, :, cut] - mean_out[d, 0:FACTORS]) * inv_out[d, 0:FACTORS]
            money = money_of[d, :, cut]
            pieces = products(y[:, cut], money)
            pieces.append(jnp.zeros((8, 128), f32))
            for q in range(0, 30, 2):
                rows = jnp.concatenate(pieces[q : q + 2], axis=0)
                for i, piece in enumerate(three_parts(rows)):
                    parts[c, 256 * i + 8 * q : 256 * i + 8 * q + 16, :] = piece

    def compute(d, parts):
        lanes = (((1,), (1,)), ((), ()))
        total = paths // 128
        step = max(total // CHUNKS, 1)
        main = jnp.zeros((256, 256), f32)
        side = jnp.zeros((256, 256), f32)
        for start in range(0, total, step):
            slabs = range(start, start + step)
            split(d, parts, slabs)
            whole = [
                jnp.concatenate(
                    [parts[c, 256 * i : 256 * i + 256, :] for c in slabs], axis=1
                )
                for i in range(3)
            ]
            for i, k in ((0, 0), (1, 1)):
                main = main + lax.dot_general(
                    whole[i], whole[k], lanes, preferred_element_type=f32
                )
            for i, k in ((0, 1), (0, 2)):
                side = side + lax.dot_general(
                    whole[i], whole[k], lanes, preferred_element_type=f32
                )
        low, high = slice(0, 128), slice(128, 256)
        gram[d, 0:128, :] = main[low, high] + (side[low, high] + side[high, low].T)
        mixed, diagonal = pack(
            main[low, low] + (side[low, low] + side[low, low].T),
            main[high, high] + (side[high, high] + side[high, high].T),
        )
        gram[d, 128:256, :] = mixed
        gram[d, 256:264, :] = diagonal

    def send(d):
        k_x = lax.rem(my_x - owner_x(d) + SIDE, SIDE)
        k_z = lax.rem(my_z - owner_z(d) + SIDE, SIDE)

        @pl.when(k_x != 0)
        def _():
            copy_a(d, k_x).start()

        @pl.when(k_z != 0)
        def _():
            copy_b(d, k_z).start()

    def collect(d):
        q = d // SIDE
        k_x = lax.rem(my_x - owner_x(d) + SIDE, SIDE)
        k_z = lax.rem(my_z - owner_z(d) + SIDE, SIDE)

        @pl.when(k_x == 0)
        def _():
            for k in range(1, SIDE):
                copy_a(d, k).wait_recv()
            sum_a[q] = (gram[d, 0:HALF] + slot_a[q, 1]) + (slot_a[q, 2] + slot_a[q, 3])

            @pl.when(k_z != 0)
            def _():
                last_copy_a(d, k_z).start()

        @pl.when(k_z == 0)
        def _():
            for k in range(1, SIDE):
                copy_b(d, k).wait_recv()
            sum_b[q] = (gram[d, HALF:PACKED] + slot_b[q, 1]) + (slot_b[q, 2] + slot_b[q, 3])

            @pl.when(k_x != 0)
            def _():
                last_copy_b(d, k_x).start()

    def gram_step(i, carry):
        d = DATES - 1 - i
        compute(d, parts)
        send(d)

        @pl.when(i >= LAG)
        def _():
            collect(d + LAG)

        return carry

    for i in range(3):
        parts[:, 256 * i + 240 : 256 * i + 256, :] = jnp.zeros((paths // 128, 16, 128), bf16)
    lax.fori_loop(0, DATES, gram_step, 0)
    meanwhile()
    for d in range(LAG - 1, -1, -1):
        collect(d)

    own_q = lax.rem(my_z - my_x + SIDE, SIDE)
    own = own_q * SIDE + my_x
    system_out[...] = jnp.zeros_like(system_out)

    @pl.when(own < DATES)
    def _():
        for k in range(1, SIDE):
            last_copy_a(own, k).wait_recv()
            last_copy_b(own, k).wait_recv()
        scale = 1.0 / count_out[own, 0:1, :]
        system_out[0:HALF] = ((sum_a[own_q] + last_a[1]) + (last_a[2] + last_a[3])) * scale
        system_out[HALF:PACKED] = ((sum_b[own_q] + last_b[1]) + (last_b[2] + last_b[3])) * scale

    def finish(d, carry):
        k_x = lax.rem(my_x - owner_x(d) + SIDE, SIDE)
        k_z = lax.rem(my_z - owner_z(d) + SIDE, SIDE)

        @pl.when(k_x != 0)
        def _():
            copy_a(d, k_x).wait_send()

        @pl.when(k_z != 0)
        def _():
            copy_b(d, k_z).wait_send()

        @pl.when((k_x == 0) & (k_z != 0))
        def _():
            last_copy_a(d, k_z).wait_send()

        @pl.when((k_z == 0) & (k_x != 0))
        def _():
            last_copy_b(d, k_x).wait_send()

        return carry

    lax.fori_loop(0, DATES, finish, 0)
    for copy in copies:
        copy.wait_send()


def sweep_block(panel, b, start):
    height = panel.shape[0]
    columns = [
        jnp.broadcast_to(panel[:, start + c : start + c + 1], (height, 128)) for c in range(8)
    ]
    pivot = [column[8 * b : 8 * b + 8, :] for column in columns]
    row_of = lax.broadcasted_iota(jnp.int32, (8, 128), 0)
    for p in range(8):
        across = [jnp.broadcast_to(column[p : p + 1, :], (8, 128)) for column in pivot]
        inverse = 1.0 / across[p]
        own = pivot[p]
        here = row_of == p
        for c in range(8):
            if c == p:
                continue
            ratio = across[c] * inverse
            pivot[c] = jnp.where(here, ratio, pivot[c] - own * ratio)
        pivot[p] = jnp.where(here, -inverse, own * inverse)
    rows = panel[8 * b : 8 * b + 8, :]
    lane = lax.broadcasted_iota(jnp.int32, (8, 256), 1)
    swept = jnp.zeros((8, 256), f32)
    wide = [jnp.concatenate([column, column], axis=1) for column in pivot]
    for c in range(8):
        swept = swept - wide[c] * jnp.broadcast_to(rows[c : c + 1, :], (8, 256))
    for c in range(8):
        swept = jnp.where(lane == start + c, wide[c], swept)
    lane = lax.broadcasted_iota(jnp.int32, (height, 256), 1)
    rest = jnp.where((lane >= start) & (lane < start + 8), 0.0, panel)
    for c in range(8):
        wide_c = jnp.concatenate([columns[c], columns[c]], axis=1)
        rest = rest - wide_c * jnp.broadcast_to(swept[c : c + 1, :], (height, 256))
    pieces = [rest[8 * q : 8 * q + 8, :] for q in range(height // 8)]
    pieces[b] = swept
    return jnp.concatenate(pieces, axis=0)


def stacked(before, panel):
    one, two, three = three_parts(before)
    uno, due, tre = three_parts(panel)
    left = jnp.concatenate([three, two, one, two, one, one], axis=0)
    right = jnp.concatenate([uno, due, tre, uno, due, uno], axis=0)
    return left, right


def transposed_product(left, right):
    return lax.dot_general(
        left, right, (((0,), (0,)), ((), ())), preferred_element_type=f32
    )


def invert(packing, gram, out, work):
    rows, lanes = triangle()
    ridge = jnp.where(rows == lanes, RIDGE, 0.0).astype(f32)
    first, cross, turned, last = unpack(gram[0:128, :], gram[128:256, :], gram[256:257, :])
    work[0:128, 0:128] = first + ridge
    work[0:128, 128:256] = cross
    work[128:256, 0:128] = turned
    work[128:256, 128:256] = last + ridge
    lane = lax.broadcasted_iota(jnp.int32, (256, 256), 1)
    current = work[0:32, :]
    for top in range(0, ROWS, 32):
        before = current
        panel = before
        for b in range(4):
            if top + 8 * b < ROWS:
                panel = sweep_block(panel, b, top + 8 * b)
        deep = min(32, ROWS - top)
        if deep < 32:
            row = lax.broadcasted_iota(jnp.int32, (32, 256), 0)
            before = jnp.where(row < deep, before, 0.0)
        kept = (lane < top) | (lane >= top + deep)
        after = top + 32
        left, right = stacked(before, panel)
        if after < ROWS:
            change = transposed_product(left[:, after : after + 32], right)
            current = jnp.where(kept[0:32, :], work[after : after + 32, :], 0.0) - change
        work[...] = jnp.where(kept, work[...], 0.0) - transposed_product(left, right)
        work[top : top + deep, :] = panel[0:deep, :]

    @pl.when(packing)
    def _():
        mixed, diagonal = pack(-work[0:128, 0:128], -work[128:256, 128:256])
        out[0:128, :] = -work[0:128, 128:256]
        out[128:256, :] = mixed
        out[256:264, :] = diagonal


def chain(
    middle, states, money_of, terminal, strike, date_index, mean, inv, count, mine, work, move,
    cash_out, price_out, coef_out,
    y, phi, exercise, discount, value, packed, solve, slots, slots_price, coefs, first_coef,
    spread_send, spread_recv, send_sem, recv_sem, price_send, price_recv, first_send, first_recv,
):
    me = lax.axis_index("path")
    paths = states.shape[2]
    chunks = paths // 128

    def prepare(d, par):
        mean_d = mean[d]
        inv_d = inv[d]
        for c in range(chunks):
            cut = slice(128 * c, 128 * c + 128)
            z = states[d, :, cut]
            y[0:FACTORS, cut] = (z - mean_d[0:FACTORS]) * inv_d[0:FACTORS]
            step = 1.0 / (1.0 + 0.25 * (0.03 * jnp.exp(0.25 * z)))
            running = step[0:1, :]
            discount[par, :, cut] = running
            total = running
            for j in range(1, FACTORS):
                running = running * step[j : j + 1, :]
                total = total + running
            annuity = 0.25 * total
            rate = (1.0 - running) / annuity
            exercise[par, :, cut] = 100.0 * annuity * (rate - strike[0])
        fill_basis(phi.at[par], y)

    my_z, my_x = me // SIDE, lax.rem(me, SIDE)
    spans = (slice(0, HALF), slice(HALF, PACKED))

    def along(axis, k):
        if axis == 0:
            return {"path": my_z * SIDE + lax.rem(my_x + k, SIDE)}
        return {"path": lax.rem(my_z + k, SIDE) * SIDE + my_x}

    def spread(source, d, half, axis, k, stage):
        return pltpu.make_async_remote_copy(
            src_ref=source,
            dst_ref=packed.at[d, spans[half]],
            send_sem=spread_send.at[stage, half, d // SIDE, k],
            recv_sem=spread_recv.at[half, d],
            device_id=along(axis, k),
            device_id_type=MESH_ID,
        )

    def relay(d, half):
        apart = my_z != owner_z(d) if half == 0 else my_x != owner_x(d)
        return jnp.logical_not(apart)

    def is_owner(d):
        return (my_x == owner_x(d)) & (my_z == owner_z(d))

    def rhs_copy(par, k):
        return pltpu.make_async_remote_copy(
            src_ref=slots.at[par, me],
            dst_ref=slots.at[par, me],
            send_sem=send_sem.at[par, k],
            recv_sem=recv_sem.at[par, k],
            device_id={"path": lax.rem(me + k, GROUP)},
            device_id_type=MESH_ID,
        )

    def price_copy(k):
        return pltpu.make_async_remote_copy(
            src_ref=slots_price.at[me],
            dst_ref=slots_price.at[me],
            send_sem=price_send.at[k],
            recv_sem=price_recv.at[k],
            device_id={"path": lax.rem(me + k, GROUP)},
            device_id_type=MESH_ID,
        )

    own = lax.rem(my_z - my_x + SIDE, SIDE) * SIDE + my_x
    last = DATES - 1
    last_owner = owner_z(last) * SIDE + owner_x(last)

    def first_copy(k):
        return pltpu.make_async_remote_copy(
            src_ref=first_coef,
            dst_ref=first_coef,
            send_sem=first_send.at[k],
            recv_sem=first_recv,
            device_id={"path": lax.rem(me + k, GROUP)},
            device_id_type=MESH_ID,
        )

    def send_rhs(t):
        par = lax.rem(t, 2)
        held = value[...] * discount[par]
        value[...] = held
        weighted = money_of[last - t] * held
        sums = jnp.zeros((ROWS, 128), f32)
        for c in range(chunks):
            cut = slice(128 * c, 128 * c + 128)
            sums = sums + phi[par, :, cut] * weighted[:, cut]
        low = jnp.sum(sums[0:128, :].T, axis=0, keepdims=True)
        high = jnp.concatenate([sums[128:ROWS, :], jnp.zeros((256 - ROWS, 128), f32)], axis=0)
        high = jnp.sum(high.T, axis=0, keepdims=True)
        slots[par, me] = jnp.concatenate([low, high], axis=0)
        for k in FAR_FIRST:
            rhs_copy(par, k).start()

    def unpack_into_solve(source):
        first, cross, turned, end = unpack(source[0:128, :], source[128:256, :], source[256:257, :])
        solve[0:128, 0:128] = first
        solve[0:128, 128:256] = cross
        solve[128:256, 0:128] = turned
        solve[128:256, 128:256] = end

    def solved(t):
        par = lax.rem(t, 2)
        rhs = slots[par, 0]
        for k in range(1, GROUP):
            rhs = rhs + slots[par, k]
        rhs = rhs / count[last - t, 0:2, :]
        product = solve[0:ROWS, 0:128] * rhs[0:1, :] + solve[0:ROWS, 128:256] * rhs[1:2, :]
        return jnp.broadcast_to(jnp.sum(product, axis=1, keepdims=True), (ROWS, 128))

    def finish_date(t, coef):
        d = last - t
        par = lax.rem(t, 2)
        lane = lax.broadcasted_iota(jnp.int32, (ROWS, 128), 1)
        coefs[0:ROWS, :] = jnp.where(lane == d, coef, coefs[0:ROWS, :])
        for c in range(chunks):
            cut = slice(128 * c, 128 * c + 128)
            continuation = jnp.sum(coef * phi[par, :, cut], axis=0, keepdims=True)
            gain = exercise[par, :, cut]
            open_date = (date_index[:, cut] <= d).astype(f32)
            money = money_of[d, :, cut]
            weight = jax.nn.sigmoid((gain - continuation) / TEMPER) * money * open_date
            old = value[:, cut]
            value[:, cut] = old + weight * (gain - old)

    def before_collecting():
        prepare(last, 0)
        value[...] = terminal[...]
        coefs[...] = jnp.zeros_like(coefs)
        send_rhs(0)

    middle(before_collecting)

    @pl.when(own < last)
    def _():
        for k in range(1, SIDE):
            for half in range(2):
                spread(mine.at[spans[half]], own, half, half, k, 0).start()
        packed[own] = mine[...]

    for k in range(1, GROUP):
        rhs_copy(0, k).wait_recv()

    @pl.when(me == last_owner)
    def _():
        solve[...] = -work[...]
        coef = solved(0)
        high = jnp.concatenate([coef[128:ROWS, :], jnp.zeros((256 - ROWS, 128), f32)], axis=0)
        first_coef[...] = jnp.concatenate([coef[0:128, :].T[0:1, :], high.T[0:1, :]], axis=0)
        for k in FAR_FIRST:
            first_copy(k).start()

    prepare(last - 1, 1)

    def relay_date(d):
        for half in range(2):

            @pl.when(relay(d, half))
            def _(half=half):
                source = packed.at[d, spans[half]]

                @pl.when(jnp.logical_not(is_owner(d)))
                def _():
                    spread(source, d, half, half, 1, 0).wait_recv()

                for k in range(1, SIDE):
                    spread(source, d, half, 1 - half, k, 1).start()

    for t in range(1, AHEAD):
        relay_date(last - t)

    @pl.when(me != last_owner)
    def _():
        first_copy(1).wait_recv()

    pad = jnp.zeros((127, 128), f32)
    halves = [
        jnp.concatenate([first_coef[i : i + 1, :], pad], axis=0).T[:, 0:1] for i in range(2)
    ]
    column = jnp.concatenate(halves, axis=0)[0:ROWS]
    finish_date(0, jnp.broadcast_to(column, (ROWS, 128)))
    send_rhs(1)

    def date_step(t, carry):
        d = last - t
        par = lax.rem(t, 2)
        for half in range(2):

            @pl.when(jnp.logical_not(relay(d, half)))
            def _(half=half):
                spread(packed.at[d, spans[half]], d, half, half, 1, 0).wait_recv()


        @pl.when(t + AHEAD <= last + 1)
        def _():
            relay_date(last + 1 - t - AHEAD)

        unpack_into_solve(packed.at[d])
        prepare(jnp.maximum(d - 1, 0), 1 - par)
        for k in range(1, GROUP):
            rhs_copy(1 - par, k).wait_send()
        for k in range(1, GROUP):
            rhs_copy(par, k).wait_recv()
        finish_date(t, solved(t))

        @pl.when(t < last)
        def _():
            send_rhs(t + 1)

        return carry

    lax.fori_loop(1, DATES, date_step, 0)

    total = jnp.zeros((1, 128), f32)
    for c in range(chunks):
        total = total + value[:, 128 * c : 128 * c + 128]
    slots_price[me] = total
    for k in FAR_FIRST:
        price_copy(k).start()
    cash_out[...] = value[...]
    turned = jnp.concatenate([coefs[0:128, :].T[0:16, :], coefs[128:256, :].T[0:16, :]], axis=1)
    ordered = jnp.zeros((16, 256), f32)
    for piece in three_parts(turned)[::-1]:
        ordered = ordered + jnp.dot(piece, move[...], preferred_element_type=f32)
    coef_out[...] = ordered[0:DATES, 0:BASIS]
    for k in range(1, GROUP):
        price_copy(k).wait_recv()
    total = slots_price[0]
    for k in range(1, GROUP):
        total = total + slots_price[k]
    price = jnp.sum(total, axis=1, keepdims=True) / (paths * GROUP)
    price_out[...] = jnp.broadcast_to(price, (1, 128))
    for k in range(1, GROUP):
        price_copy(k).wait_send()
        rhs_copy(last % 2, k).wait_send()

    @pl.when(me == last_owner)
    def _():
        for k in range(1, GROUP):
            first_copy(k).wait_send()

    @pl.when(own < last)
    def _():
        for k in range(1, SIDE):
            for half in range(2):
                spread(mine.at[spans[half]], own, half, half, k, 0).wait_send()

    def relay_done(d, carry):
        for half in range(2):

            @pl.when(relay(d, half))
            def _(half=half):
                for k in range(1, SIDE):
                    spread(packed.at[d, spans[half]], d, half, 1 - half, k, 1).wait_send()

        return carry

    lax.fori_loop(0, last, relay_done, 0)


FRONT_SCRATCH = 22


def whole_kernel(states, flags, terminal, strike, date_index, move, cash, price, coefs, *scratch):
    mean, inv, count, system, mine, work = scratch[:6]
    front_scratch = scratch[6 : 6 + FRONT_SCRATCH]
    money_of, y = front_scratch[2:4]
    me = lax.axis_index("path")
    own = lax.rem(me // SIDE - lax.rem(me, SIDE) + SIDE, SIDE) * SIDE + lax.rem(me, SIDE)

    def middle(meanwhile):
        front(meanwhile, states, flags, mean, inv, count, system, *front_scratch)

        @pl.when(own < DATES)
        def _():
            invert(own != DATES - 1, system, mine, work)

    chain(
        middle, states, money_of, terminal, strike, date_index, mean, inv, count, mine, work, move,
        cash, price, coefs, y, *scratch[6 + FRONT_SCRATCH :],
    )


def whole_call(states, flags, terminal, strike, date_index, move):
    paths = states.shape[2]
    columns = DATES // SIDE + 1
    dma = pltpu.SemaphoreType.DMA

    def space(*shape):
        return pltpu.VMEM(shape, f32)

    front_scratch = [
        space(640, 128),
        space(GROUP, 8, 128),
        space(DATES, 1, paths),
        space(24, paths),
        pltpu.VMEM((paths // 128, 768, 128), bf16),
        space(DATES, PACKED, 128),
        space(columns, SIDE, HALF, 128),
        space(columns, SIDE, PACKED - HALF, 128),
        space(columns, HALF, 128),
        space(columns, PACKED - HALF, 128),
        space(SIDE, HALF, 128),
        space(SIDE, PACKED - HALF, 128),
        dma((GROUP,)),
        dma((GROUP,)),
        dma((DATES,)),
        dma((DATES,)),
        dma((columns, SIDE)),
        dma((columns, SIDE)),
        dma((columns,)),
        dma((columns,)),
        dma((SIDE,)),
        dma((SIDE,)),
    ]
    assert len(front_scratch) == FRONT_SCRATCH
    return pl.pallas_call(
        whole_kernel,
        name="whole",
        out_shape=(
            jax.ShapeDtypeStruct((1, paths), f32),
            jax.ShapeDtypeStruct((1, 128), f32),
            jax.ShapeDtypeStruct((DATES, BASIS), f32),
        ),
        in_specs=[vmem()] * 3 + [pl.BlockSpec(memory_space=pltpu.SMEM)] + [vmem()] * 2,
        out_specs=(vmem(),) * 3,
        scratch_shapes=[
            space(DATES, 24, 128),
            space(DATES, 24, 128),
            space(DATES, 8, 128),
            space(PACKED, 128),
            space(PACKED, 128),
            space(256, 256),
            *front_scratch,
            space(2, ROWS, paths),
            space(2, 1, paths),
            space(2, 1, paths),
            space(1, paths),
            space(DATES, PACKED, 128),
            space(256, 256),
            space(2, GROUP, 2, 128),
            space(GROUP, 1, 128),
            space(256, 128),
            space(2, 128),
            dma((2, 2, columns, SIDE)),
            dma((2, DATES)),
            dma((2, GROUP)),
            dma((2, GROUP)),
            dma((GROUP,)),
            dma((GROUP,)),
            dma((GROUP,)),
            dma,
        ],
        compiler_params=pltpu.CompilerParams(collective_id=0, has_side_effects=True),
    )(states, flags, terminal, strike, date_index, move)


def result_kernel(cash, price, coefs, cash_out, price_out, coef_out):
    cash_out[...] = cash[...]
    price_out[...] = price[...]
    coef_out[...] = coefs[...]


def result_call(cash, price, coefs):
    return pl.pallas_call(
        result_kernel,
        name="result",
        out_shape=tuple(jax.ShapeDtypeStruct(a.shape, f32) for a in (cash, price, coefs)),
        in_specs=[vmem()] * 3,
        out_specs=(vmem(),) * 3,
    )(cash, price, coefs)


def shards(states, flags, terminal, strike, date_index):
    paths = states.shape[2]
    whole = whole_call(
        states, flags, terminal.reshape(1, paths), strike, date_index.reshape(1, paths),
        reference_order(),
    )
    cash, price, coefs = result_call(*whole)
    return cash.reshape(paths), price[0, 0:1], coefs


def solution(mesh):
    both = ("book", "path")
    return jax.shard_map(
        shards,
        mesh=mesh,
        in_specs=(P(None, None, both), P(None, both), P(both), P("book"), P(both)),
        out_specs=(P(both), P("book"), P("book", None)),
        check_vma=False,
    )
```
